128 devices in a mesh: dp: 128 (over x, z, y, core).
Axes of the slice: x: 4, y: 4, z: 4, core: 2. Of those that a mesh axis runs over, the one named last changes fastest.
Arguments:
- captions: bfloat16 [4096, 77, 768], P('dp'), may hold values from -6 to 6
- caption_layout: int32 [2, 4096], replicated, may hold values from 0 to 77, as said below
- images: bfloat16 [4096, 768], P('dp'), may hold values from -0.24 to 0.24
- w_query: bfloat16 [768, 768], replicated, may hold values from -0.21875 to 0.21875
- w_keyval: bfloat16 [768, 1536], replicated, may hold values from -0.21875 to 0.21875
- w_out: bfloat16 [768, 768], replicated, may hold values from -0.21875 to 0.21875
- w_up: bfloat16 [768, 3072], replicated, may hold values from -0.21875 to 0.21875
- w_down: bfloat16 [3072, 768], replicated, may hold values from -0.109375 to 0.109375
- w_proj: bfloat16 [768, 768], replicated, may hold values from -0.009114583 to 0.009114583
Outputs:
- image_grad: float32 [4096, 768], P('dp')
- text_grad: float32 [4096, 768], P('dp')
The draws below stay inside these ranges and needn't reach their ends.
Inputs may be any that keep to these rules, and one draw needn't show every extreme that they name: `caption_layout`: row 0 holds each caption's token count; row 1 is 1 where the caption is encoded by the next index of dp (index 0 after the last) and 0 where by its own. Exactly 8 of each device's captions carry 1. The captions one device encodes (its own that carry 0 and those carrying 1 of the index before it) hold at most 2048 tokens together, exactly that many on some device.
All inputs are finite; a program needn't handle non-finite values.
Results may differ from the reference program's by a relative error of at most 0.018.
Values may be sent and summed in bfloat16 or wider, within the bound.
A program may use at most 128 MiB of HBM per device.

```python
import math
import jax
import jax.numpy as jnp
from jax import lax

D = 768
HEADS = 12
FF = 3072
E = 768
CTX = 77
CAP_DEV = 32
HAND = 8
TOK_CAP = 2048
PAIRS = 4096
N_DP = 128


def caption_plan(key):
    order_key = jax.random.fold_in(key, 7102)
    length_key = jax.random.fold_in(key, 7103)
    heavy_key = jax.random.fold_in(key, 7104)
    hand_counts = jnp.full((N_DP,), HAND, jnp.int32)
    permuted = jax.vmap(lambda sub_key: jax.random.permutation(sub_key, CAP_DEV))(jax.random.split(order_key, N_DP))
    position_rank = jnp.argsort(permuted, axis=1)
    handed_flags = (position_rank < hand_counts[:, None]).astype(jnp.int32)
    owner_index = jnp.broadcast_to(jnp.arange(N_DP, dtype=jnp.int32)[:, None], (N_DP, CAP_DEV))
    group_index = ((owner_index + handed_flags) % N_DP).reshape(-1)
    heaviness = jax.random.randint(heavy_key, (N_DP, 1), 2, 5)
    raw_length = (jax.random.randint(length_key, (N_DP, CAP_DEV), 0, CTX) * heaviness // 4).reshape(-1)
    raw_length = jnp.where(group_index == 0, CTX - 1, raw_length)
    onehot = (group_index[:, None] == jnp.arange(N_DP, dtype=jnp.int32)[None, :]).astype(jnp.int32)
    members = jnp.sum(onehot, axis=0)
    total_raw = jnp.sum(onehot * raw_length[:, None], axis=0)
    room_left = TOK_CAP - members
    own_room = room_left[group_index]
    own_total = jnp.maximum(total_raw[group_index], 1)
    floor_part = raw_length * own_room // own_total
    floor_total = jnp.sum(onehot * floor_part[:, None], axis=0)
    group_rank = jnp.sum((jnp.cumsum(onehot, axis=0) - onehot) * onehot, axis=1)
    extra_token = (group_rank < (room_left - floor_total)[group_index]).astype(jnp.int32)
    scaled = (total_raw > room_left)[group_index]
    lengths = jnp.where(scaled, 1 + floor_part + extra_token, 1 + raw_length)
    return jnp.stack([lengths, handed_flags.reshape(-1)]).astype(jnp.int32)


def draw_caption_layout(key, part):
    return caption_plan(key)


def draw_captions(key, part):
    noise = jax.random.normal(jax.random.fold_in(key, 7211), (PAIRS, CTX, D), jnp.float32)
    values = jnp.clip(noise, -6.0, 6.0)
    return values.astype(jnp.bfloat16)


def draw_w_proj(key, part):
    noise = jax.random.normal(jax.random.fold_in(key, 7221), (D, E), jnp.float32)
    values = jnp.clip(noise, -6.0, 6.0) / math.sqrt(D * E)
    return values.astype(jnp.bfloat16)


def draw_images(key, part):
    noise = jax.random.normal(jax.random.fold_in(key, 7231), (PAIRS, E), jnp.float32)
    values = 0.04 * jnp.clip(noise, -5.9, 5.9)
    return values.astype(jnp.bfloat16)


def bell_draw(key, dims, scale, most, held_as=jnp.bfloat16):
    values = jax.random.normal(key, dims, jnp.float32) * scale
    return jnp.minimum(jnp.maximum(values, -most), most).astype(held_as)


def setup_inputs(seed: int = 0) -> dict:
    seeds = jax.random.split(jax.random.key(seed), 10)
    captions = draw_captions(jax.random.fold_in(seeds[9], 71), 0)
    caption_layout = draw_caption_layout(jax.random.fold_in(seeds[9], 71), 0)
    images = draw_images(jax.random.fold_in(seeds[9], 71), 0)
    w_query = bell_draw(seeds[3], (D, D), D ** -0.5, 0.21875)
    w_keyval = bell_draw(seeds[4], (D, 2 * D), D ** -0.5, 0.21875)
    w_out = bell_draw(seeds[5], (D, D), D ** -0.5, 0.21875)
    w_up = bell_draw(seeds[6], (D, FF), D ** -0.5, 0.21875)
    w_down = bell_draw(seeds[7], (FF, D), FF ** -0.5, 0.109375)
    w_proj = draw_w_proj(jax.random.fold_in(seeds[9], 71), 0)
    return dict(captions=captions, caption_layout=caption_layout, images=images, w_query=w_query, w_keyval=w_keyval, w_out=w_out, w_up=w_up, w_down=w_down, w_proj=w_proj)


LOGIT_SCALE = 100.0
EPS_NORM = 1e-05
EPS_UNIT = 1e-06

def layer_norm(values):
    values = values.astype(jnp.float32)
    center = values - lax.optimization_barrier(jnp.mean(values, axis=-1, keepdims=True))
    spread = lax.optimization_barrier(jnp.mean(center * center, axis=-1, keepdims=True))
    return center * lax.rsqrt(spread + EPS_NORM)

def unit_rows(values):
    values = values.astype(jnp.float32)
    return values * lax.rsqrt(lax.optimization_barrier(jnp.sum(values * values, axis=-1, keepdims=True)) + EPS_UNIT)

def contract_first(left, right):
    return lax.dot_general(left, right, (((0,), (0,)), ((), ())), preferred_element_type=jnp.float32)

def contract_last(left, right):
    return lax.dot_general(left, right, (((1,), (1,)), ((), ())), preferred_element_type=jnp.float32)

def reference(captions, caption_layout, images, w_query, w_keyval, w_out, w_up, w_down, w_proj):
    model_width = captions.shape[2]
    head_dim = model_width // HEADS

    def encode_block(block_item):
        caption_block, block_lengths = block_item
        block_count = caption_block.shape[0]
        normed = layer_norm(caption_block).astype(jnp.bfloat16)
        keyval = jnp.dot(normed.reshape(-1, model_width), w_keyval, preferred_element_type=jnp.float32)
        keyval = keyval.astype(jnp.bfloat16).reshape(block_count, CTX, 2 * model_width)
        last_slot = (block_lengths - 1).astype(jnp.int32)[:, None, None]
        end_normed = jnp.take_along_axis(normed, last_slot, axis=1)[:, 0]
        end_tokens = jnp.take_along_axis(caption_block, last_slot, axis=1)[:, 0]
        query = jnp.dot(end_normed, w_query, preferred_element_type=jnp.float32).astype(jnp.bfloat16)
        key_heads = keyval[:, :, :model_width].reshape(block_count, CTX, HEADS, head_dim).astype(jnp.float32)
        value_heads = keyval[:, :, model_width:].reshape(block_count, CTX, HEADS, head_dim).astype(jnp.float32)
        query_heads = query.reshape(block_count, HEADS, head_dim).astype(jnp.float32)
        scores = jnp.einsum('chd,cthd->cht', query_heads, key_heads) / math.sqrt(head_dim)
        inside = jnp.arange(CTX)[None, None, :] < block_lengths[:, None, None]
        masked = jnp.where(inside, scores, -jnp.inf)
        peak = lax.optimization_barrier(jnp.max(masked, axis=-1, keepdims=True))
        exponent = jnp.exp(masked - peak)
        attention = (exponent / lax.optimization_barrier(jnp.sum(exponent, axis=-1, keepdims=True))).astype(jnp.bfloat16)
        mixed_heads = jnp.einsum('cht,cthd->chd', attention.astype(jnp.float32), value_heads)
        mixed_heads = mixed_heads.astype(jnp.bfloat16).reshape(block_count, model_width)
        residual = end_tokens.astype(jnp.float32) + jnp.dot(mixed_heads, w_out, preferred_element_type=jnp.float32)
        residual = residual.astype(jnp.bfloat16)
        inner_norm = layer_norm(residual).astype(jnp.bfloat16)
        hidden = jax.nn.gelu(jnp.dot(inner_norm, w_up, preferred_element_type=jnp.float32), approximate=False)
        hidden = hidden.astype(jnp.bfloat16)
        final_rows = residual.astype(jnp.float32) + jnp.dot(hidden, w_down, preferred_element_type=jnp.float32)
        pooled = layer_norm(final_rows).astype(jnp.bfloat16)
        return jnp.dot(pooled, w_proj, preferred_element_type=jnp.float32).astype(jnp.bfloat16)
    caption_blocks = captions.reshape(N_DP, CAP_DEV, CTX, model_width)
    length_blocks = caption_layout[0].reshape(N_DP, CAP_DEV)
    text_embed = lax.map(encode_block, (caption_blocks, length_blocks)).reshape(PAIRS, -1)
    image_unit = unit_rows(images).astype(jnp.bfloat16)
    text_unit = unit_rows(text_embed).astype(jnp.bfloat16)
    scores = LOGIT_SCALE * contract_last(image_unit, text_unit)
    row_peak = lax.optimization_barrier(jnp.max(scores, axis=1, keepdims=True))
    row_logsum = row_peak[:, 0] + jnp.log(lax.optimization_barrier(jnp.sum(jnp.exp(scores - row_peak), axis=1)))
    column_peak = lax.optimization_barrier(jnp.max(scores, axis=0, keepdims=True))
    column_logsum = column_peak[0] + jnp.log(lax.optimization_barrier(jnp.sum(jnp.exp(scores - column_peak), axis=0)))
    row_weights = jnp.exp(scores - row_logsum[:, None]).astype(jnp.bfloat16)
    column_weights = jnp.exp(scores - column_logsum[None, :]).astype(jnp.bfloat16)
    half_scale = 0.5 * LOGIT_SCALE
    image_unit_grad = half_scale * (jnp.dot(row_weights, text_unit, preferred_element_type=jnp.float32) + jnp.dot(column_weights, text_unit, preferred_element_type=jnp.float32))
    image_unit_grad = image_unit_grad - LOGIT_SCALE * text_unit.astype(jnp.float32)
    text_unit_grad = half_scale * (contract_first(row_weights, image_unit) + contract_first(column_weights, image_unit))
    text_unit_grad = text_unit_grad - LOGIT_SCALE * image_unit.astype(jnp.float32)
    image_value, image_back = jax.vjp(unit_rows, images.astype(jnp.float32))
    text_value, text_back = jax.vjp(unit_rows, text_embed.astype(jnp.float32))
    return (image_back(image_unit_grad)[0], text_back(text_unit_grad)[0])
```

```python
import math

import jax
import jax.numpy as jnp
from jax import lax
from jax.experimental import pallas as pl
from jax.experimental.pallas import tpu as pltpu
from jax.sharding import PartitionSpec as P

HEADS = 12
HEAD_DIM = 64
WIDTH = 768
CTX = 77
CAPS = 32
FF = 3072
GROUP = 16
GROUPS = CAPS // GROUP
COLS = HEADS * GROUP
TOKENS = CTX * GROUP
LOAD_STEPS = 7
STEP_T = CTX // LOAD_STEPS
CHIPS = 8
ROWS = CHIPS * 2 * CAPS
CHUNK = 128
CHUNKS = ROWS // CHUNK

LOGIT_SCALE = 100.0
EPS_NORM = 1e-05
EPS_UNIT = 1e-06

MESH = pl.DeviceIdType.MESH
F32 = jnp.float32
BF16 = jnp.bfloat16


def norm_rows(values):
    center = values - jnp.mean(values, axis=-1, keepdims=True)
    spread = jnp.mean(center * center, axis=-1, keepdims=True)
    return center * lax.rsqrt(spread + EPS_NORM)


def unit_scale(values):
    return lax.rsqrt(jnp.sum(values * values, axis=-1, keepdims=True) + EPS_UNIT)


def unit_back(values, grad):
    scale = unit_scale(values)
    along = jnp.sum(values * grad, axis=-1, keepdims=True)
    return grad * scale - values * (along * (scale * scale * scale))


def dot(left, right):
    return jnp.dot(left, right, preferred_element_type=F32)


def dot_last(left, right):
    return lax.dot_general(left, right, (((1,), (1,)), ((), ())), preferred_element_type=F32)


def dot_first(left, right):
    return lax.dot_general(left, right, (((0,), (0,)), ((), ())), preferred_element_type=F32)


def iota(shape, dim):
    return lax.broadcasted_iota(jnp.int32, shape, dim)


class Place:
    def __init__(self):
        self.me = lax.axis_index("dp")
        self.core = self.me % 2
        self.at = {"y": (self.me // 2) % 4, "z": (self.me // 8) % 4, "x": self.me // 32}
        self.partner = self.me + 1 - 2 * self.core

    def flip(self, kind, value):
        image, text = 3 - value, value + 1 - 2 * (value % 2)
        return image + kind * (text - image)

    def bit(self, kind, value):
        return value // 2 + kind * (value % 2 - value // 2)

    def coords(self, kind, offset):
        return {
            axis: self.flip(kind, self.at[axis]) if offset >> step & 1 else self.at[axis]
            for step, axis in enumerate("yzx")
        }

    def peer(self, kind, offset, core):
        where = self.coords(kind, offset)
        return ((where["x"] * 4 + where["z"]) * 4 + where["y"]) * 2 + core

    def slot(self, kind, offset):
        where = self.coords(kind, offset)
        bits = {axis: self.bit(kind, where[axis]) for axis in "yzx"}
        return bits["x"] * 4 + bits["z"] * 2 + bits["y"]


def kernel(
    captions,
    layout,
    images,
    w_query,
    w_keyval,
    w_out,
    w_up,
    w_down,
    w_proj,
    image_grad,
    text_grad,
    tokens,
    normed,
    end_rows,
    query_w,
    keyval_w,
    out_w,
    up_w,
    down_w,
    proj_w,
    attn_scores,
    attn,
    units,
    row_exp,
    col_exp,
    row_peak,
    col_peak,
    logs,
    row_log,
    blocks,
    parts,
    load_sem,
    weight_sem,
    gather_send,
    gather_recv,
    pass_send,
    pass_recv,
    log_send,
    log_recv,
    part_send,
    part_recv,
):
    place = Place()
    me, core, partner = place.me, place.core, place.partner
    other = 1 - core

    loads = []
    for step in range(LOAD_STEPS):
        span = pl.ds(step * STEP_T, STEP_T)
        copy = pltpu.make_async_copy(captions.at[span], tokens.at[span], load_sem.at[step])
        copy.start()
        loads.append(copy)
    weights = {}
    for number, (name, source, target) in enumerate(
        (
            ("query", w_query, query_w),
            ("keyval", w_keyval, keyval_w),
            ("out", w_out, out_w),
            ("up", w_up, up_w),
            ("down", w_down, down_w),
            ("proj", w_proj, proj_w),
        )
    ):
        weights[name] = pltpu.make_async_copy(source, target, weight_sem.at[number])
        weights[name].start()

    barrier = pltpu.get_barrier_semaphore()
    friends = [partner]
    for offset in range(1, CHIPS):
        for kind in range(2):
            friends += [place.peer(kind, offset, 0), place.peer(kind, offset, 1)]
    for friend in friends:
        pl.semaphore_signal(barrier, inc=1, device_id=(friend,), device_id_type=MESH)

    image_values = images[...].astype(F32)
    image_unit = (image_values * unit_scale(image_values)).astype(BF16)
    image_slot, text_slot = place.slot(0, 0), place.slot(1, 0)
    units[core, image_slot, 0] = image_unit

    span = pl.ds(pl.multiple_of(me // 4 * 128, 128), 128)
    counts = layout[0:1, span].astype(F32)
    picked = iota((CAPS, 128), 1) == iota((CAPS, 128), 0) + me % 4 * CAPS
    lengths = jnp.sum(jnp.where(picked, counts, 0.0), axis=1, keepdims=True)
    lengths = jnp.maximum(lengths, 1.0)

    end_rows[...] = jnp.zeros_like(end_rows)
    for step in range(LOAD_STEPS):
        loads[step].wait()

    def norm_step(step, _):
        for group in range(GROUPS):
            rows = slice(group * GROUP, (group + 1) * GROUP)
            ends = end_rows[rows, :]
            for inner in range(STEP_T):
                t = step * STEP_T + inner
                values = tokens[t, rows, :].astype(F32)
                at = pl.ds(pl.multiple_of(t * GROUP, GROUP), GROUP)
                normed[group, at, :] = norm_rows(values).astype(BF16)
                ends = jnp.where(lengths[rows] - 1.0 == t.astype(F32), values, ends)
            end_rows[rows, :] = ends
        return 0

    lax.fori_loop(0, LOAD_STEPS, norm_step, 0)

    end_values = end_rows[...]
    end_normed = norm_rows(end_values).astype(BF16)
    weights["query"].wait()
    query = dot(end_normed, query_w[...]).astype(BF16).astype(F32) * (1.0 / math.sqrt(HEAD_DIM))
    head_of = iota((GROUP, WIDTH), 1) // HEAD_DIM
    spread = jnp.concatenate(
        [
            jnp.where(head_of == head, query[group * GROUP : (group + 1) * GROUP], 0.0)
            for group in range(GROUPS)
            for head in range(HEADS)
        ],
        axis=0,
    ).astype(BF16)
    weights["keyval"].wait()
    key_query = dot_last(spread, keyval_w[:, :WIDTH]).astype(BF16)

    contexts = []
    same = iota((GROUP, COLS), 0) == iota((GROUP, COLS), 1) % GROUP
    for group in range(GROUPS):
        attn_scores[...] = dot_last(normed[group], key_query[group * COLS : (group + 1) * COLS])
        belongs = iota((CAPS, COLS), 0) == iota((CAPS, COLS), 1) % GROUP + group * GROUP
        limit = jnp.sum(jnp.where(belongs, lengths, 0.0), axis=0, keepdims=True)

        def at_token(t):
            return pl.ds(pl.multiple_of(t * GROUP, GROUP), GROUP)

        def peak_step(t, peak):
            inside = t.astype(F32) < limit
            return jnp.maximum(peak, jnp.where(inside, attn_scores[at_token(t), :], -jnp.inf))

        peak = lax.fori_loop(
            0, CTX, peak_step, jnp.full((GROUP, COLS), -jnp.inf, F32), unroll=STEP_T
        )

        def exp_step(t, total):
            inside = same & (t.astype(F32) < limit)
            value = jnp.where(inside, jnp.exp(attn_scores[at_token(t), :] - peak), 0.0)
            attn_scores[at_token(t), :] = value
            return total + value

        total = lax.fori_loop(0, CTX, exp_step, jnp.zeros((GROUP, COLS), F32), unroll=STEP_T)
        scale = jnp.where(same, 1.0 / jnp.where(same, total, 1.0), 0.0)

        def attn_step(t, _):
            attn[at_token(t), :] = (attn_scores[at_token(t), :] * scale).astype(BF16)
            return 0

        lax.fori_loop(0, CTX, attn_step, 0, unroll=STEP_T)
        contexts.append(dot_first(attn[...], normed[group]).astype(BF16))

    pl.semaphore_wait(barrier, len(friends))
    image_sends, text_sends = [], []
    for offset in range(CHIPS - 1, 0, -1):
        copy = pltpu.make_async_remote_copy(
            src_ref=units.at[core, image_slot, 0],
            dst_ref=units.at[core, image_slot, 0],
            send_sem=gather_send.at[0, offset],
            recv_sem=gather_recv.at[0, offset],
            device_id=(place.peer(0, offset, core),),
            device_id_type=MESH,
        )
        copy.start()
        image_sends.append((offset, copy))

    by_head = dot(jnp.concatenate(contexts, axis=0), keyval_w[:, WIDTH:])
    mixed = []
    for group in range(GROUPS):
        total = jnp.zeros((GROUP, WIDTH), F32)
        for head in range(HEADS):
            first = group * COLS + head * GROUP
            total = total + jnp.where(head_of == head, by_head[first : first + GROUP], 0.0)
        mixed.append(total)
    mixed = jnp.concatenate(mixed, axis=0).astype(BF16)

    weights["out"].wait()
    residual = (end_values + dot(mixed, out_w[...])).astype(BF16)
    residual = residual.astype(F32)
    inner = norm_rows(residual).astype(BF16)
    weights["up"].wait()
    weights["down"].wait()
    final = residual
    for part in range(FF // WIDTH):
        span = slice(part * WIDTH, (part + 1) * WIDTH)
        hidden = dot(inner, up_w[:, span])
        hidden = 0.5 * hidden * (1.0 + lax.erf(hidden * (1.0 / math.sqrt(2.0))))
        final = final + dot(hidden.astype(BF16), down_w[span, :])
    pooled = norm_rows(final).astype(BF16)
    weights["proj"].wait()
    text_values = dot(pooled, proj_w[...]).astype(BF16).astype(F32)
    text_unit = (text_values * unit_scale(text_values)).astype(BF16)
    units[other, text_slot, 0] = text_unit

    for offset in range(CHIPS - 1, 0, -1):
        copy = pltpu.make_async_remote_copy(
            src_ref=units.at[other, text_slot, 0],
            dst_ref=units.at[other, text_slot, 0],
            send_sem=gather_send.at[1, offset],
            recv_sem=gather_recv.at[1, offset],
            device_id=(place.peer(1, offset, core),),
            device_id_type=MESH,
        )
        copy.start()
        text_sends.append((offset, copy))

    def hand_on(kind, offset):
        mine, theirs = (core, other) if kind == 0 else (other, core)
        slot = place.slot(kind, offset)
        copy = pltpu.make_async_remote_copy(
            src_ref=units.at[mine, slot, 0],
            dst_ref=units.at[theirs, slot, 1],
            send_sem=pass_send.at[kind, offset],
            recv_sem=pass_recv.at[kind, offset],
            device_id=(partner,),
            device_id_type=MESH,
        )
        copy.start()
        return copy

    passed = [hand_on(1, 0), hand_on(0, 0)]
    for offset, copy in image_sends[::-1]:
        copy.wait_recv()
        passed.append(hand_on(0, offset))
    for offset, copy in text_sends[::-1]:
        copy.wait_recv()
        passed.append(hand_on(1, offset))
    for copy in passed:
        copy.wait_recv()

    others = units[1].reshape(ROWS, WIDTH)
    eye = iota((CHUNK, CHUNK), 0) == iota((CHUNK, CHUNK), 1)
    col_sums, col_peaks = [], []
    for chunk in range(CHUNKS):
        mine = units[0, 2 * chunk : 2 * chunk + 2].reshape(CHUNK, WIDTH)
        scores = LOGIT_SCALE * dot_last(mine, others)
        peak = jnp.max(scores, axis=1, keepdims=True)
        value = jnp.exp(scores - peak)
        row_exp[chunk] = value
        row_peak[chunk] = peak
        log = peak + jnp.log(jnp.sum(value, axis=1, keepdims=True))
        logs[0, 0, chunk : chunk + 1, :] = jnp.sum(
            jnp.where(eye, log, 0.0), axis=0, keepdims=True
        )
        peak = jnp.max(scores, axis=0, keepdims=True)
        value = jnp.exp(scores - peak)
        col_exp[chunk] = value
        col_peak[chunk] = peak
        col_peaks.append(peak)
        col_sums.append(jnp.sum(value, axis=0, keepdims=True))
    top = col_peaks[0]
    for peak in col_peaks[1:]:
        top = jnp.maximum(top, peak)
    total = sum(part * jnp.exp(peak - top) for part, peak in zip(col_sums, col_peaks))
    log = top + jnp.log(total)
    for chunk in range(CHUNKS):
        logs[1, 0, chunk : chunk + 1, :] = log[:, chunk * CHUNK : (chunk + 1) * CHUNK]

    log_sends = []
    for offset in range(CHIPS - 1, 0, -1):
        for side, kind in ((0, core), (1, other)):
            copy = pltpu.make_async_remote_copy(
                src_ref=logs.at[side, 0],
                dst_ref=logs.at[side, offset],
                send_sem=log_send.at[side, offset],
                recv_sem=log_recv.at[side, offset],
                device_id=(place.peer(kind, offset, core),),
                device_id_type=MESH,
            )
            copy.start()
            log_sends.append(copy)
    for copy in log_sends:
        copy.wait_recv()

    def whole_log(side):
        top = logs[side, 0]
        for offset in range(1, CHIPS):
            top = jnp.maximum(top, logs[side, offset])
        total = jnp.zeros_like(top)
        for offset in range(CHIPS):
            total = total + jnp.exp(logs[side, offset] - top)
        return top + jnp.log(total)

    row_logs, col_logs = whole_log(0), whole_log(1)
    for chunk in range(CHUNKS):
        row_log[chunk] = row_logs[chunk : chunk + 1, :]
    col_logs = jnp.concatenate([col_logs[chunk : chunk + 1, :] for chunk in range(CHUNKS)], axis=1)

    part_sends = []
    for pair in range(CHUNKS - 1, -1, -1):
        chunk = place.slot(core, 2 * pair) // 2
        log = jnp.sum(jnp.where(eye, row_log[chunk], 0.0), axis=1, keepdims=True)
        row_scale = jnp.exp(row_peak[chunk] - log)
        col_scale = jnp.exp(col_peak[chunk] - col_logs)
        weight = (row_exp[chunk] * row_scale + col_exp[chunk] * col_scale).astype(BF16)
        grad = dot(weight, others).astype(BF16).reshape(2, 2, CAPS, WIDTH)
        blocks[pl.ds(chunk * 2, 2)] = grad
        for offset in (2 * pair + 1, 2 * pair):
            slot = place.slot(core, offset)
            for side in range(2):
                if offset == 0 and side == 0:
                    parts[core, 0] = blocks[slot, 0]
                    continue
                copy = pltpu.make_async_remote_copy(
                    src_ref=blocks.at[slot, side],
                    dst_ref=parts.at[core, offset],
                    send_sem=part_send.at[offset, side],
                    recv_sem=part_recv.at[core, offset],
                    device_id=(place.peer(core, offset, core + side - 2 * side * core),),
                    device_id_type=MESH,
                )
                copy.start()
                part_sends.append(copy)

    def arrived(kind, offset):
        pltpu.make_async_remote_copy(
            src_ref=parts.at[kind, offset],
            dst_ref=parts.at[kind, offset],
            send_sem=part_send.at[0, 0],
            recv_sem=part_recv.at[kind, offset],
            device_id=(partner,),
            device_id_type=MESH,
        ).wait_recv()

    arrived(other, 0)
    for offset in range(1, CHIPS):
        for kind in range(2):
            arrived(kind, offset)

    half = 0.5 * LOGIT_SCALE
    sums = []
    for kind in range(2):
        total = parts[kind, 0].astype(F32)
        for offset in range(1, CHIPS):
            total = total + parts[kind, offset].astype(F32)
        sums.append(total)
    image_unit_grad = half * sums[0] - LOGIT_SCALE * text_unit.astype(F32)
    text_unit_grad = half * sums[1] - LOGIT_SCALE * image_unit.astype(F32)
    image_grad[...] = unit_back(image_values, image_unit_grad)
    text_grad[...] = unit_back(text_values, text_unit_grad)

    for _, copy in image_sends + text_sends:
        copy.wait_send()
    for copy in passed + log_sends + part_sends:
        copy.wait_send()


def body(captions, caption_layout, images, w_query, w_keyval, w_out, w_up, w_down, w_proj):
    hbm = pl.BlockSpec(memory_space=pl.ANY)
    vmem = pl.BlockSpec(memory_space=pltpu.VMEM)
    dma = pltpu.SemaphoreType.DMA
    return pl.pallas_call(
        kernel,
        out_shape=(
            jax.ShapeDtypeStruct((CAPS, WIDTH), F32),
            jax.ShapeDtypeStruct((CAPS, WIDTH), F32),
        ),
        in_specs=[hbm, vmem, vmem] + [hbm] * 6,
        out_specs=(vmem, vmem),
        scratch_shapes=[
            pltpu.VMEM((CTX, CAPS, WIDTH), BF16),
            pltpu.VMEM((GROUPS, TOKENS, WIDTH), BF16),
            pltpu.VMEM((CAPS, WIDTH), F32),
            pltpu.VMEM((WIDTH, WIDTH), BF16),
            pltpu.VMEM((WIDTH, 2 * WIDTH), BF16),
            pltpu.VMEM((WIDTH, WIDTH), BF16),
            pltpu.VMEM((WIDTH, FF), BF16),
            pltpu.VMEM((FF, WIDTH), BF16),
            pltpu.VMEM((WIDTH, WIDTH), BF16),
            pltpu.VMEM((TOKENS, COLS), F32),
            pltpu.VMEM((TOKENS, COLS), BF16),
            pltpu.VMEM((2, CHIPS, 2, CAPS, WIDTH), BF16),
            pltpu.VMEM((CHUNKS, CHUNK, ROWS), F32),
            pltpu.VMEM((CHUNKS, CHUNK, ROWS), F32),
            pltpu.VMEM((CHUNKS, CHUNK, 1), F32),
            pltpu.VMEM((CHUNKS, 1, ROWS), F32),
            pltpu.VMEM((2, CHIPS, CHUNKS, CHUNK), F32),
            pltpu.VMEM((CHUNKS, 1, CHUNK), F32),
            pltpu.VMEM((CHIPS, 2, CAPS, WIDTH), BF16),
            pltpu.VMEM((2, CHIPS, CAPS, WIDTH), BF16),
            dma((LOAD_STEPS,)),
            dma((6,)),
            dma((2, CHIPS)),
            dma((2, CHIPS)),
            dma((2, CHIPS)),
            dma((2, CHIPS)),
            dma((2, CHIPS)),
            dma((2, CHIPS)),
            dma((CHIPS, 2)),
            dma((2, CHIPS)),
        ],
        compiler_params=pltpu.CompilerParams(
            collective_id=0, has_side_effects=True, vmem_limit_bytes=60 * 1024 * 1024
        ),
    )(
        captions.transpose(1, 0, 2),
        caption_layout,
        images,
        w_query,
        w_keyval,
        w_out,
        w_up,
        w_down,
        w_proj,
    )


def solution(mesh):
    return jax.shard_map(
        body,
        mesh=mesh,
        in_specs=(P("dp", None, None), P(), P("dp", None), P(), P(), P(), P(), P(), P()),
        out_specs=(P("dp", None), P("dp", None)),
        check_vma=False,
    )
```

```python
import math

import jax
import jax.numpy as jnp
from jax import lax
from jax.experimental import pallas as pl
from jax.experimental.pallas import tpu as pltpu
from jax.sharding import PartitionSpec as P

HEADS = 12
HEAD_DIM = 64
WIDTH = 768
CTX = 77
CAPS = 32
FF = 3072
GROUP = 16
GROUPS = CAPS // GROUP
COLS = HEADS * GROUP
TOKENS = CTX * GROUP
LOAD_STEPS = 7
STEP_T = CTX // LOAD_STEPS
CHIPS = 8
ROWS = CHIPS * 2 * CAPS
CHUNK = 128
CHUNKS = ROWS // CHUNK

LOGIT_SCALE = 100.0
EPS_NORM = 1e-05
EPS_UNIT = 1e-06
LOG2_E = math.log2(math.e)

MESH = pl.DeviceIdType.MESH
F32 = jnp.float32
BF16 = jnp.bfloat16


def norm_rows(values):
    center = values - jnp.mean(values, axis=-1, keepdims=True)
    spread = jnp.mean(center * center, axis=-1, keepdims=True)
    return center * lax.rsqrt(spread + EPS_NORM)


def unit_scale(values):
    return lax.rsqrt(jnp.sum(values * values, axis=-1, keepdims=True) + EPS_UNIT)


def unit_back(values, grad):
    scale = unit_scale(values)
    along = jnp.sum(values * grad, axis=-1, keepdims=True)
    return grad * scale - values * (along * (scale * scale * scale))


def dot(left, right):
    return jnp.dot(left, right, preferred_element_type=F32)


def dot_last(left, right):
    return lax.dot_general(left, right, (((1,), (1,)), ((), ())), preferred_element_type=F32)


def dot_first(left, right):
    return lax.dot_general(left, right, (((0,), (0,)), ((), ())), preferred_element_type=F32)


def iota(shape, dim):
    return lax.broadcasted_iota(jnp.int32, shape, dim)


class Place:
    def __init__(self):
        self.me = lax.axis_index("dp")
        self.core = self.me % 2
        self.at = {"y": (self.me // 2) % 4, "z": (self.me // 8) % 4, "x": self.me // 32}
        self.partner = self.me + 1 - 2 * self.core

    def flip(self, kind, value):
        image, text = 3 - value, value + 1 - 2 * (value % 2)
        return image + kind * (text - image)

    def bit(self, kind, value):
        return value // 2 + kind * (value % 2 - value // 2)

    def coords(self, kind, offset):
        return {
            axis: self.flip(kind, self.at[axis]) if offset >> step & 1 else self.at[axis]
            for step, axis in enumerate("yzx")
        }

    def peer(self, kind, offset, core):
        where = self.coords(kind, offset)
        return ((where["x"] * 4 + where["z"]) * 4 + where["y"]) * 2 + core

    def slot(self, kind, offset):
        where = self.coords(kind, offset)
        bits = {axis: self.bit(kind, where[axis]) for axis in "yzx"}
        return bits["x"] * 4 + bits["z"] * 2 + bits["y"]


def kernel(
    captions,
    layout,
    images,
    w_query,
    w_keyval,
    w_out,
    w_up,
    w_down,
    w_proj,
    image_grad,
    text_grad,
    tokens,
    normed,
    end_rows,
    query_w,
    keyval_w,
    out_w,
    up_w,
    down_w,
    proj_w,
    attn_scores,
    attn,
    units,
    row_exp,
    col_exp,
    row_peak,
    col_peak,
    logs,
    row_log,
    blocks,
    parts,
    load_sem,
    weight_sem,
    gather_send,
    gather_recv,
    pass_send,
    pass_recv,
    log_send,
    log_recv,
    part_send,
    part_recv,
):
    place = Place()
    me, core, partner = place.me, place.core, place.partner
    other = 1 - core

    def load(step):
        span = pl.ds(step * STEP_T, STEP_T)
        return pltpu.make_async_copy(captions.at[span], tokens.at[span], load_sem.at[step])

    for step in range(LOAD_STEPS):
        load(step).start()
    weights = {}
    for number, (name, source, target) in enumerate(
        (
            ("query", w_query, query_w),
            ("keyval", w_keyval, keyval_w),
            ("out", w_out, out_w),
            ("up", w_up, up_w),
            ("down", w_down, down_w),
            ("proj", w_proj, proj_w),
        )
    ):
        weights[name] = pltpu.make_async_copy(source, target, weight_sem.at[number])
    weights["query"].start()

    barrier = pltpu.get_barrier_semaphore()
    friends = [partner]
    for offset in range(1, CHIPS):
        for kind in range(2):
            friends += [place.peer(kind, offset, 0), place.peer(kind, offset, 1)]
    for friend in friends:
        pl.semaphore_signal(barrier, inc=1, device_id=(friend,), device_id_type=MESH)

    image_values = images[...].astype(F32)
    image_unit = (image_values * unit_scale(image_values)).astype(BF16)
    image_slot, text_slot = place.slot(0, 0), place.slot(1, 0)
    units[core, image_slot, 0] = image_unit

    span = pl.ds(pl.multiple_of(me // 4 * 128, 128), 128)
    counts = layout[0:1, span].astype(F32)
    picked = iota((CAPS, 128), 1) == iota((CAPS, 128), 0) + me % 4 * CAPS
    lengths = jnp.sum(jnp.where(picked, counts, 0.0), axis=1, keepdims=True)
    lengths = jnp.maximum(lengths, 1.0)

    end_rows[...] = jnp.zeros_like(end_rows)

    def norm_step(step, _):
        load(step).wait()

        @pl.when(step == 1)
        def _():
            weights["keyval"].start()

        @pl.when(step == 3)
        def _():
            for name in ("out", "up", "down", "proj"):
                weights[name].start()

        for group in range(GROUPS):
            rows = slice(group * GROUP, (group + 1) * GROUP)
            ends = end_rows[rows, :]
            for inner in range(STEP_T):
                t = step * STEP_T + inner
                values = tokens[t, rows, :].astype(F32)
                at = pl.ds(pl.multiple_of(t * GROUP, GROUP), GROUP)
                normed[group, at, :] = norm_rows(values).astype(BF16)
                ends = jnp.where(lengths[rows] - 1.0 == t.astype(F32), values, ends)
            end_rows[rows, :] = ends
        return 0

    lax.fori_loop(0, LOAD_STEPS, norm_step, 0)

    pl.semaphore_wait(barrier, len(friends))
    image_sends, text_sends = [], []
    for offset in range(CHIPS - 1, 0, -1):
        copy = pltpu.make_async_remote_copy(
            src_ref=units.at[core, image_slot, 0],
            dst_ref=units.at[core, image_slot, 0],
            send_sem=gather_send.at[0, offset],
            recv_sem=gather_recv.at[0, offset],
            device_id=(place.peer(0, offset, core),),
            device_id_type=MESH,
        )
        copy.start()
        image_sends.append((offset, copy))

    end_values = end_rows[...]
    end_normed = norm_rows(end_values).astype(BF16)
    weights["query"].wait()
    query = dot(end_normed, query_w[...]).astype(BF16).astype(F32) * (1.0 / math.sqrt(HEAD_DIM))
    head_of = iota((GROUP, WIDTH), 1) // HEAD_DIM
    spread = jnp.concatenate(
        [
            jnp.where(head_of == head, query[group * GROUP : (group + 1) * GROUP], 0.0)
            for group in range(GROUPS)
            for head in range(HEADS)
        ],
        axis=0,
    ).astype(BF16)
    weights["keyval"].wait()
    key_query = (dot_last(spread, keyval_w[:, :WIDTH]) * LOG2_E).astype(BF16)

    contexts = []
    turn = iota((COLS, COLS), 0) == iota((COLS, COLS), 1)
    same = iota((GROUP, COLS), 0) == iota((GROUP, COLS), 1) % GROUP
    for group in range(GROUPS):
        attn_scores[...] = dot_last(normed[group], key_query[group * COLS : (group + 1) * COLS])
        belongs = iota((CAPS, COLS), 0) == iota((CAPS, COLS), 1) % GROUP + group * GROUP
        limit = jnp.sum(jnp.where(belongs, lengths, 0.0), axis=0, keepdims=True)

        def at_token(t):
            return pl.ds(pl.multiple_of(t * GROUP, GROUP), GROUP)

        def peak_step(t, peak):
            inside = t.astype(F32) < limit
            return jnp.maximum(peak, jnp.where(inside, attn_scores[at_token(t), :], -jnp.inf))

        peak = lax.fori_loop(
            0, CTX, peak_step, jnp.full((GROUP, COLS), -jnp.inf, F32), unroll=CTX
        )

        peak = jnp.where(same, peak, jnp.inf)

        def exp_step(t, total):
            inside = t.astype(F32) < limit
            value = jnp.where(inside, attn_scores[at_token(t), :], -jnp.inf)
            value = jnp.exp2(value - peak)
            attn[at_token(t), :] = value.astype(BF16)
            return total + value

        total = lax.fori_loop(0, CTX, exp_step, jnp.zeros((GROUP, COLS), F32), unroll=CTX)
        total = jnp.sum(total, axis=0, keepdims=True)
        total = jnp.sum(jnp.where(turn, total, 0.0), axis=1, keepdims=True)
        contexts.append((dot_first(attn[...], normed[group]) / total).astype(BF16))

    by_head = dot(jnp.concatenate(contexts, axis=0), keyval_w[:, WIDTH:])
    mixed = []
    for group in range(GROUPS):
        total = jnp.zeros((GROUP, WIDTH), F32)
        for head in range(HEADS):
            first = group * COLS + head * GROUP
            total = total + jnp.where(head_of == head, by_head[first : first + GROUP], 0.0)
        mixed.append(total)
    mixed = jnp.concatenate(mixed, axis=0).astype(BF16)

    weights["out"].wait()
    residual = (end_values + dot(mixed, out_w[...])).astype(BF16)
    residual = residual.astype(F32)
    inner = norm_rows(residual).astype(BF16)
    weights["up"].wait()
    weights["down"].wait()
    final = residual
    for part in range(FF // WIDTH):
        span = slice(part * WIDTH, (part + 1) * WIDTH)
        hidden = dot(inner, up_w[:, span])
        hidden = 0.5 * hidden * (1.0 + lax.erf(hidden * (1.0 / math.sqrt(2.0))))
        final = final + dot(hidden.astype(BF16), down_w[span, :])
    pooled = norm_rows(final).astype(BF16)
    weights["proj"].wait()
    text_values = dot(pooled, proj_w[...]).astype(BF16).astype(F32)
    text_unit = (text_values * unit_scale(text_values)).astype(BF16)
    units[other, text_slot, 0] = text_unit

    for offset in range(CHIPS - 1, 0, -1):
        copy = pltpu.make_async_remote_copy(
            src_ref=units.at[other, text_slot, 0],
            dst_ref=units.at[other, text_slot, 0],
            send_sem=gather_send.at[1, offset],
            recv_sem=gather_recv.at[1, offset],
            device_id=(place.peer(1, offset, core),),
            device_id_type=MESH,
        )
        copy.start()
        text_sends.append((offset, copy))

    def hand_on(kind, offset):
        mine, theirs = (core, other) if kind == 0 else (other, core)
        slot = place.slot(kind, offset)
        copy = pltpu.make_async_remote_copy(
            src_ref=units.at[mine, slot, 0],
            dst_ref=units.at[theirs, slot, 1],
            send_sem=pass_send.at[kind, offset],
            recv_sem=pass_recv.at[kind, offset],
            device_id=(partner,),
            device_id_type=MESH,
        )
        copy.start()
        return copy

    passed = [hand_on(1, 0), hand_on(0, 0)]
    for offset, copy in image_sends[::-1]:
        copy.wait_recv()
        passed.append(hand_on(0, offset))
    for offset, copy in text_sends[::-1]:
        copy.wait_recv()
        passed.append(hand_on(1, offset))
    for copy in passed:
        copy.wait_recv()

    others = units[1].reshape(ROWS, WIDTH)
    eye = iota((CHUNK, CHUNK), 0) == iota((CHUNK, CHUNK), 1)
    col_sums, col_peaks = [], []
    for chunk in range(CHUNKS):
        mine = units[0, 2 * chunk : 2 * chunk + 2].reshape(CHUNK, WIDTH)
        scores = LOGIT_SCALE * dot_last(mine, others)
        peak = jnp.max(scores, axis=1, keepdims=True)
        value = jnp.exp(scores - peak)
        row_exp[chunk] = value
        row_peak[chunk] = peak
        log = peak + jnp.log(jnp.sum(value, axis=1, keepdims=True))
        logs[0, 0, chunk : chunk + 1, :] = jnp.sum(
            jnp.where(eye, log, 0.0), axis=0, keepdims=True
        )
        peak = jnp.max(scores, axis=0, keepdims=True)
        value = jnp.exp(scores - peak)
        col_exp[chunk] = value
        col_peak[chunk] = peak
        col_peaks.append(peak)
        col_sums.append(jnp.sum(value, axis=0, keepdims=True))
    top = col_peaks[0]
    for peak in col_peaks[1:]:
        top = jnp.maximum(top, peak)
    total = sum(part * jnp.exp(peak - top) for part, peak in zip(col_sums, col_peaks))
    log = top + jnp.log(total)
    for chunk in range(CHUNKS):
        logs[1, 0, chunk : chunk + 1, :] = log[:, chunk * CHUNK : (chunk + 1) * CHUNK]

    log_sends = []
    for offset in range(CHIPS - 1, 0, -1):
        for side, kind in ((0, core), (1, other)):
            copy = pltpu.make_async_remote_copy(
                src_ref=logs.at[side, 0],
                dst_ref=logs.at[side, offset],
                send_sem=log_send.at[side, offset],
                recv_sem=log_recv.at[side, offset],
                device_id=(place.peer(kind, offset, core),),
                device_id_type=MESH,
            )
            copy.start()
            log_sends.append(copy)
    for copy in log_sends:
        copy.wait_recv()

    def whole_log(side):
        top = logs[side, 0]
        for offset in range(1, CHIPS):
            top = jnp.maximum(top, logs[side, offset])
        total = jnp.zeros_like(top)
        for offset in range(CHIPS):
            total = total + jnp.exp(logs[side, offset] - top)
        return top + jnp.log(total)

    row_logs, col_logs = whole_log(0), whole_log(1)
    for chunk in range(CHUNKS):
        row_log[chunk] = row_logs[chunk : chunk + 1, :]
    col_logs = jnp.concatenate([col_logs[chunk : chunk + 1, :] for chunk in range(CHUNKS)], axis=1)

    part_sends = []
    for pair in range(CHUNKS - 1, -1, -1):
        chunk = place.slot(core, 2 * pair) // 2
        log = jnp.sum(jnp.where(eye, row_log[chunk], 0.0), axis=1, keepdims=True)
        row_scale = jnp.exp(row_peak[chunk] - log)
        col_scale = jnp.exp(col_peak[chunk] - col_logs)
        weight = (row_exp[chunk] * row_scale + col_exp[chunk] * col_scale).astype(BF16)
        grad = dot(weight, others).astype(BF16).reshape(2, 2, CAPS, WIDTH)
        blocks[pl.ds(chunk * 2, 2)] = grad
        for offset in (2 * pair + 1, 2 * pair):
            slot = place.slot(core, offset)
            for side in range(2):
                if offset == 0 and side == 0:
                    parts[core, 0] = blocks[slot, 0]
                    continue
                copy = pltpu.make_async_remote_copy(
                    src_ref=blocks.at[slot, side],
                    dst_ref=parts.at[core, offset],
                    send_sem=part_send.at[offset, side],
                    recv_sem=part_recv.at[core, offset],
                    device_id=(place.peer(core, offset, core + side - 2 * side * core),),
                    device_id_type=MESH,
                )
                copy.start()
                part_sends.append(copy)

    def arrived(kind, offset):
        pltpu.make_async_remote_copy(
            src_ref=parts.at[kind, offset],
            dst_ref=parts.at[kind, offset],
            send_sem=part_send.at[0, 0],
            recv_sem=part_recv.at[kind, offset],
            device_id=(partner,),
            device_id_type=MESH,
        ).wait_recv()

    arrived(other, 0)
    for offset in range(1, CHIPS):
        for kind in range(2):
            arrived(kind, offset)

    half = 0.5 * LOGIT_SCALE
    sums = []
    for kind in range(2):
        total = parts[kind, 0].astype(F32)
        for offset in range(1, CHIPS):
            total = total + parts[kind, offset].astype(F32)
        sums.append(total)
    image_unit_grad = half * sums[0] - LOGIT_SCALE * text_unit.astype(F32)
    text_unit_grad = half * sums[1] - LOGIT_SCALE * image_unit.astype(F32)
    image_grad[...] = unit_back(image_values, image_unit_grad)
    text_grad[...] = unit_back(text_values, text_unit_grad)

    for _, copy in image_sends + text_sends:
        copy.wait_send()
    for copy in passed + log_sends + part_sends:
        copy.wait_send()


def hand_out(image_from, text_from, image_to, text_to):
    image_to[...] = image_from[...]
    text_to[...] = text_from[...]


def body(captions, caption_layout, images, w_query, w_keyval, w_out, w_up, w_down, w_proj):
    hbm = pl.BlockSpec(memory_space=pl.ANY)
    vmem = pl.BlockSpec(memory_space=pltpu.VMEM)
    dma = pltpu.SemaphoreType.DMA
    grads = (jax.ShapeDtypeStruct((CAPS, WIDTH), F32),) * 2
    made = pl.pallas_call(
        kernel,
        out_shape=grads,
        in_specs=[hbm, vmem, vmem] + [hbm] * 6,
        out_specs=(vmem, vmem),
        scratch_shapes=[
            pltpu.VMEM((CTX, CAPS, WIDTH), BF16),
            pltpu.VMEM((GROUPS, TOKENS, WIDTH), BF16),
            pltpu.VMEM((CAPS, WIDTH), F32),
            pltpu.VMEM((WIDTH, WIDTH), BF16),
            pltpu.VMEM((WIDTH, 2 * WIDTH), BF16),
            pltpu.VMEM((WIDTH, WIDTH), BF16),
            pltpu.VMEM((WIDTH, FF), BF16),
            pltpu.VMEM((FF, WIDTH), BF16),
            pltpu.VMEM((WIDTH, WIDTH), BF16),
            pltpu.VMEM((TOKENS, COLS), F32),
            pltpu.VMEM((TOKENS, COLS), BF16),
            pltpu.VMEM((2, CHIPS, 2, CAPS, WIDTH), BF16),
            pltpu.VMEM((CHUNKS, CHUNK, ROWS), F32),
            pltpu.VMEM((CHUNKS, CHUNK, ROWS), F32),
            pltpu.VMEM((CHUNKS, CHUNK, 1), F32),
            pltpu.VMEM((CHUNKS, 1, ROWS), F32),
            pltpu.VMEM((2, CHIPS, CHUNKS, CHUNK), F32),
            pltpu.VMEM((CHUNKS, 1, CHUNK), F32),
            pltpu.VMEM((CHIPS, 2, CAPS, WIDTH), BF16),
            pltpu.VMEM((2, CHIPS, CAPS, WIDTH), BF16),
            dma((LOAD_STEPS,)),
            dma((6,)),
            dma((2, CHIPS)),
            dma((2, CHIPS)),
            dma((2, CHIPS)),
            dma((2, CHIPS)),
            dma((2, CHIPS)),
            dma((2, CHIPS)),
            dma((CHIPS, 2)),
            dma((2, CHIPS)),
        ],
        compiler_params=pltpu.CompilerParams(
            collective_id=0, has_side_effects=True, vmem_limit_bytes=60 * 1024 * 1024
        ),
    )(
        captions.transpose(1, 0, 2),
        caption_layout,
        images,
        w_query,
        w_keyval,
        w_out,
        w_up,
        w_down,
        w_proj,
    )
    return pl.pallas_call(hand_out, out_shape=grads, in_specs=[vmem] * 2, out_specs=(vmem, vmem))(*made)


def solution(mesh):
    return jax.shard_map(
        body,
        mesh=mesh,
        in_specs=(P("dp", None, None), P(), P("dp", None), P(), P(), P(), P(), P(), P()),
        out_specs=(P("dp", None), P("dp", None)),
        check_vma=False,
    )
```

```python
import math

import jax
import jax.numpy as jnp
from jax import lax
from jax.experimental import pallas as pl
from jax.experimental.pallas import tpu as pltpu
from jax.sharding import PartitionSpec as P

HEADS = 12
HEAD_DIM = 64
WIDTH = 768
CTX = 77
CAPS = 32
FF = 3072
GROUP = 16
GROUPS = CAPS // GROUP
SPLIT = HEADS * GROUP
TOKENS = CTX * GROUP
TOKENS_PAD = -(-TOKENS // 256) * 256
BLOCK = 256
BLOCK_HEADS = BLOCK // HEAD_DIM
LOAD_STEPS = 7
STEP_T = CTX // LOAD_STEPS
NORM_UNROLL = 11
CHIPS = 8
ROWS = CHIPS * 2 * CAPS
HALF = ROWS // 2
PIECE = 128
PIECES = ROWS // PIECE

LOGIT_SCALE = 100.0
EPS_NORM = 1e-05
EPS_UNIT = 1e-06
LOG2_E = math.log2(math.e)

MESH = pl.DeviceIdType.MESH
F32 = jnp.float32
BF16 = jnp.bfloat16


def norm_rows(values):
    center = values - jnp.mean(values, axis=-1, keepdims=True)
    spread = jnp.mean(center * center, axis=-1, keepdims=True)
    return center * lax.rsqrt(spread + EPS_NORM)


def unit_scale(values):
    return lax.rsqrt(jnp.sum(values * values, axis=-1, keepdims=True) + EPS_UNIT)


def unit_back(values, grad):
    scale = unit_scale(values)
    along = jnp.sum(values * grad, axis=-1, keepdims=True)
    return grad * scale - values * (along * (scale * scale * scale))


def dot(left, right):
    return jnp.dot(left, right, preferred_element_type=F32)


def dot_last(left, right):
    return lax.dot_general(left, right, (((1,), (1,)), ((), ())), preferred_element_type=F32)


def dot_first(left, right):
    return lax.dot_general(left, right, (((0,), (0,)), ((), ())), preferred_element_type=F32)


def iota(shape, dim):
    return lax.broadcasted_iota(jnp.int32, shape, dim)


class Place:
    def __init__(self):
        self.me = lax.axis_index("dp")
        self.core = self.me % 2
        self.at = {"y": (self.me // 2) % 4, "z": (self.me // 8) % 4, "x": self.me // 32}
        self.partner = self.me + 1 - 2 * self.core

    def flip(self, kind, value):
        image, text = 3 - value, value + 1 - 2 * (value % 2)
        return image + kind * (text - image)

    def bit(self, kind, value):
        return value // 2 + kind * (value % 2 - value // 2)

    def coords(self, kind, offset):
        return {
            axis: self.flip(kind, self.at[axis]) if offset >> step & 1 else self.at[axis]
            for step, axis in enumerate("yzx")
        }

    def peer(self, kind, offset, core):
        where = self.coords(kind, offset)
        return ((where["x"] * 4 + where["z"]) * 4 + where["y"]) * 2 + core

    def slot(self, kind, offset):
        where = self.coords(kind, offset)
        bits = {axis: self.bit(kind, where[axis]) for axis in "yzx"}
        return bits["x"] * 4 + bits["z"] * 2 + bits["y"]


def kernel(
    captions,
    layout,
    images,
    w_query,
    w_keyval,
    w_out,
    w_up,
    w_down,
    w_proj,
    image_grad,
    text_grad,
    tokens,
    normed,
    query_w,
    keyval_w,
    out_w,
    up_w,
    down_w,
    proj_w,
    counts,
    ends,
    image_rows,
    attn_scores,
    attn_bias,
    attn,
    units,
    row_exp,
    col_exp,
    row_peak,
    col_peak,
    logs,
    weight,
    blocks,
    parts,
    small_sem,
    load_sem,
    weight_sem,
    gather_send,
    gather_recv,
    pass_send,
    pass_recv,
    log_send,
    log_recv,
    part_send,
    part_recv,
):
    place = Place()
    me, core, partner = place.me, place.core, place.partner
    other = 1 - core

    def load(step):
        span = pl.ds(step * STEP_T, STEP_T)
        return pltpu.make_async_copy(captions.at[span], tokens.at[span], load_sem.at[step])

    span = pl.ds(pl.multiple_of(me // 4 * 128, 128), 128)
    load_counts = pltpu.make_async_copy(layout.at[:, span], counts, small_sem.at[0])
    load_images = pltpu.make_async_copy(images, image_rows, small_sem.at[1])
    load_ends = pltpu.make_async_copy(layout.at[:, span], ends, small_sem.at[2])
    for step in range(LOAD_STEPS):
        load(step).start()
    for copy in (load_counts, load_ends, load_images):
        copy.start()
    weights = {}
    for number, (name, source, target) in enumerate(
        (
            ("query", w_query, query_w),
            ("keyval", w_keyval, keyval_w),
            ("out", w_out, out_w),
            ("up", w_up, up_w),
            ("down", w_down, down_w),
            ("proj", w_proj, proj_w),
        )
    ):
        weights[name] = pltpu.make_async_copy(source, target, weight_sem.at[number])
    weights["query"].start()

    barrier = pltpu.get_barrier_semaphore()
    friends = [partner]
    for offset in range(1, CHIPS):
        for kind in range(2):
            friends += [place.peer(kind, offset, 0), place.peer(kind, offset, 1)]
    for friend in friends:
        pl.semaphore_signal(barrier, inc=1, device_id=(friend,), device_id_type=MESH)

    normed[:, TOKENS:, :] = jnp.zeros((GROUPS, TOKENS_PAD - TOKENS, WIDTH), BF16)

    def norm_step(step, _):
        load(step).wait()

        @pl.when(step == 1)
        def _():
            weights["keyval"].start()

        @pl.when(step == 3)
        def _():
            for name in ("out", "up", "down", "proj"):
                weights[name].start()

        def token_step(inner, _):
            t = step * STEP_T + inner
            at = pl.ds(pl.multiple_of(t * GROUP, GROUP), GROUP)
            for group in range(GROUPS):
                rows = slice(group * GROUP, (group + 1) * GROUP)
                values = tokens[t, rows, :].astype(F32)
                normed[group, at, :] = norm_rows(values).astype(BF16)
            return 0

        return lax.fori_loop(0, STEP_T, token_step, 0, unroll=NORM_UNROLL)

    lax.fori_loop(0, LOAD_STEPS, norm_step, 0)

    load_images.wait()
    image_values = image_rows[...].astype(F32)
    image_unit = (image_values * unit_scale(image_values)).astype(BF16)
    slots = (place.slot(0, 0), place.slot(1, 0))
    units[0, 0, slots[0]] = image_unit

    pl.semaphore_wait(barrier, len(friends))

    def send_units(kind):
        copies = {}
        for offset in range(CHIPS - 1, 0, -1):
            copies[offset] = pltpu.make_async_remote_copy(
                src_ref=units.at[kind, 0, slots[kind]],
                dst_ref=units.at[kind, 0, slots[kind]],
                send_sem=gather_send.at[kind, offset],
                recv_sem=gather_recv.at[kind, offset],
                device_id=(place.peer(kind, offset, core),),
                device_id_type=MESH,
            )
            copies[offset].start()
        return copies

    def hand_on(kind, offset):
        slot = place.slot(kind, offset)
        copy = pltpu.make_async_remote_copy(
            src_ref=units.at[kind, 0, slot],
            dst_ref=units.at[kind, 1, slot],
            send_sem=pass_send.at[kind, offset],
            recv_sem=pass_recv.at[kind, offset],
            device_id=(partner,),
            device_id_type=MESH,
        )
        copy.start()
        return copy

    image_sends = send_units(0)
    passed = {(0, 0): hand_on(0, 0)}

    load_counts.wait()
    picked = iota((CAPS, 128), 1) == iota((CAPS, 128), 0) + me % 4 * CAPS
    lengths = jnp.sum(jnp.where(picked, counts[0:1, :].astype(F32), 0.0), axis=1, keepdims=True)
    lengths = jnp.maximum(lengths, 1.0)

    token = iota((GROUP, TOKENS_PAD), 1)
    own = token % GROUP == iota((GROUP, TOKENS_PAD), 0)
    for group in range(GROUPS):
        count = lengths[group * GROUP : (group + 1) * GROUP]
        inside = own & ((token // GROUP).astype(F32) < count)
        attn_bias[group] = jnp.where(inside, 0.0, -jnp.inf)

    load_ends.wait()
    end_values = []
    for group in range(GROUPS):
        rows = jnp.zeros((GROUP, WIDTH), BF16)
        for inner in range(GROUP):
            caption = group * GROUP + inner
            last = jnp.clip(ends[0, me % 4 * CAPS + caption] - 1, 0, CTX - 1)
            found = tokens[last, group * GROUP : (group + 1) * GROUP, :]
            rows = jnp.where(iota((GROUP, WIDTH), 0) == inner, found, rows)
        end_values.append(rows)
    end_values = jnp.concatenate(end_values, axis=0).astype(F32)
    end_normed = norm_rows(end_values).astype(BF16)
    weights["query"].wait()
    query = dot(end_normed, query_w[...]).astype(BF16).astype(F32) * (1.0 / math.sqrt(HEAD_DIM))
    head_of = iota((GROUP, BLOCK), 1) // HEAD_DIM
    groups = [slice(group * GROUP, (group + 1) * GROUP) for group in range(GROUPS)]
    spans = [slice(at, at + BLOCK) for at in range(0, WIDTH, BLOCK)]
    weights["keyval"].wait()
    key_query = []
    for span in spans:
        spread = [
            jnp.where(head_of == head, query[rows, span], 0.0)
            for rows in groups
            for head in range(BLOCK_HEADS)
        ]
        spread = jnp.concatenate(spread, axis=0).astype(BF16)
        key_query.append((dot_last(spread, keyval_w[:, span]) * LOG2_E).astype(BF16))

    part = BLOCK_HEADS * GROUP
    contexts = []
    for group in range(GROUPS):
        rows = slice(group * part, (group + 1) * part)
        asked = jnp.concatenate([block[rows] for block in key_query], axis=0)
        attn_scores[...] = dot_last(asked, normed[group])
        totals = []
        for head in range(HEADS):
            rows = slice(head * GROUP, (head + 1) * GROUP)
            value = attn_scores[rows, :] + attn_bias[group]
            value = jnp.exp2(value - jnp.max(value, axis=1, keepdims=True))
            attn[rows, :] = value.astype(BF16)
            totals.append(jnp.sum(value, axis=1, keepdims=True))
        context = dot(attn[...], normed[group]) / jnp.concatenate(totals, axis=0)
        contexts.append(context.astype(BF16))

    mixed = []
    for number, span in enumerate(spans):
        rows = slice(number * part, (number + 1) * part)
        by_head = jnp.concatenate([context[rows] for context in contexts], axis=0)
        by_head = dot(by_head, keyval_w[:, WIDTH + span.start : WIDTH + span.stop])
        sums = []
        for group in range(GROUPS):
            total = jnp.zeros((GROUP, BLOCK), F32)
            for head in range(BLOCK_HEADS):
                first = group * part + head * GROUP
                total = total + jnp.where(head_of == head, by_head[first : first + GROUP], 0.0)
            sums.append(total)
        mixed.append(jnp.concatenate(sums, axis=0))
    mixed = jnp.concatenate(mixed, axis=1).astype(BF16)

    weights["out"].wait()
    residual = (end_values + dot(mixed, out_w[...])).astype(BF16)
    residual = residual.astype(F32)
    inner = norm_rows(residual).astype(BF16)
    weights["up"].wait()
    weights["down"].wait()
    final = residual
    for part in range(FF // WIDTH):
        span = slice(part * WIDTH, (part + 1) * WIDTH)
        hidden = dot(inner, up_w[:, span])
        hidden = 0.5 * hidden * (1.0 + lax.erf(hidden * (1.0 / math.sqrt(2.0))))
        final = final + dot(hidden.astype(BF16), down_w[span, :])
    pooled = norm_rows(final).astype(BF16)
    weights["proj"].wait()
    text_values = dot(pooled, proj_w[...]).astype(BF16).astype(F32)
    text_unit = (text_values * unit_scale(text_values)).astype(BF16)
    units[1, 0, slots[1]] = text_unit

    text_sends = send_units(1)
    passed[1, 0] = hand_on(1, 0)

    for offset in range(1, CHIPS):
        image_sends[offset].wait_recv()
        passed[0, offset] = hand_on(0, offset)

    for offset in range(CHIPS - 1, 0, -1):
        text_sends[offset].wait_recv()
        passed[1, offset] = hand_on(1, offset)
    for offset in range(CHIPS):
        passed[0, offset].wait_recv()

    eye = iota((PIECE, PIECE), 0) == iota((PIECE, PIECE), 1)
    col_sums, col_peaks = [], []
    for half in range(2):
        if half == 1:
            for offset in range(CHIPS):
                passed[1, offset].wait_recv()
        scores = dot_last(units[1, half].reshape(HALF, WIDTH), units[0].reshape(ROWS, WIDTH))
        scores = scores * (LOGIT_SCALE * LOG2_E)
        peak = jnp.max(scores, axis=1, keepdims=True)
        value = jnp.exp2(scores - peak)
        row_exp[half] = value
        row_peak[half] = peak
        log = peak + jnp.log(jnp.sum(value, axis=1, keepdims=True)) * LOG2_E
        for piece in range(HALF // PIECE):
            part = log[piece * PIECE : (piece + 1) * PIECE]
            part = jnp.sum(jnp.where(eye, part, 0.0), axis=0, keepdims=True)
            logs[1, 0, half * (HALF // PIECE) + piece] = part
        peak = jnp.max(scores, axis=0, keepdims=True)
        value = jnp.exp2(scores - peak)
        col_exp[half] = value
        col_peak[half] = peak
        col_peaks.append(peak)
        col_sums.append(jnp.sum(value, axis=0, keepdims=True))
    top = jnp.maximum(*col_peaks)
    total = sum(part * jnp.exp2(peak - top) for part, peak in zip(col_sums, col_peaks))
    log = top + jnp.log(total) * LOG2_E
    for piece in range(PIECES):
        logs[0, 0, piece] = log[:, piece * PIECE : (piece + 1) * PIECE]

    log_sends = []
    for offset in range(CHIPS - 1, 0, -1):
        for kind in range(2):
            copy = pltpu.make_async_remote_copy(
                src_ref=logs.at[kind, 0],
                dst_ref=logs.at[kind, offset],
                send_sem=log_send.at[kind, offset],
                recv_sem=log_recv.at[kind, offset],
                device_id=(place.peer(kind, offset, core),),
                device_id_type=MESH,
            )
            copy.start()
            log_sends.append(copy)
    for copy in log_sends:
        copy.wait_recv()

    def whole_log(kind):
        top = logs[kind, 0]
        for offset in range(1, CHIPS):
            top = jnp.maximum(top, logs[kind, offset])
        total = jnp.zeros_like(top)
        for offset in range(CHIPS):
            total = total + jnp.exp2(logs[kind, offset] - top)
        return top + jnp.log(total) * LOG2_E

    image_logs, text_logs = whole_log(0), whole_log(1)
    image_logs = jnp.concatenate([image_logs[piece] for piece in range(PIECES)], axis=1)
    for half in range(2):
        col_scale = jnp.exp2(col_peak[half] - image_logs)
        for piece in range(HALF // PIECE):
            rows = slice(piece * PIECE, (piece + 1) * PIECE)
            first = half * HALF + piece * PIECE
            log = text_logs[half * (HALF // PIECE) + piece]
            log = jnp.sum(jnp.where(eye, log, 0.0), axis=1, keepdims=True)
            row_scale = jnp.exp2(row_peak[half, rows] - log)
            both = row_exp[half, rows] * row_scale + col_exp[half, rows] * col_scale
            weight[first : first + PIECE, :] = both.astype(BF16)

    part_sends = []
    for far in (1, 0):
        for side in range(2):
            first = place.slot(core, 4 * far) // 4 * 4
            span = pl.ds(pl.multiple_of(side * HALF + first * CAPS, PIECE), PIECE)

            def keep(grad):
                blocks[side, pl.ds(first, 4)] = grad.astype(BF16).reshape(4, CAPS, WIDTH)

            @pl.when(core == 0)
            def _():
                keep(dot_first(weight[:, span], units[1].reshape(ROWS, WIDTH)))

            @pl.when(core == 1)
            def _():
                keep(dot(weight[span, :], units[0].reshape(ROWS, WIDTH)))

            for offset in range(4 * far + 3, 4 * far - 1, -1):
                slot = place.slot(core, offset)
                if offset == 0 and side == 0:
                    parts[core, 0] = blocks[0, slot]
                    continue
                copy = pltpu.make_async_remote_copy(
                    src_ref=blocks.at[side, slot],
                    dst_ref=parts.at[core, offset],
                    send_sem=part_send.at[offset, side],
                    recv_sem=part_recv.at[core, offset],
                    device_id=(place.peer(core, offset, core + side - 2 * side * core),),
                    device_id_type=MESH,
                )
                copy.start()
                part_sends.append(copy)

    def arrived(kind, offset):
        pltpu.make_async_remote_copy(
            src_ref=parts.at[kind, offset],
            dst_ref=parts.at[kind, offset],
            send_sem=part_send.at[0, 0],
            recv_sem=part_recv.at[kind, offset],
            device_id=(partner,),
            device_id_type=MESH,
        ).wait_recv()

    arrived(other, 0)
    for offset in range(1, CHIPS):
        for kind in range(2):
            arrived(kind, offset)

    half = 0.5 * LOGIT_SCALE
    sums = []
    for kind in range(2):
        total = parts[kind, 0].astype(F32)
        for offset in range(1, CHIPS):
            total = total + parts[kind, offset].astype(F32)
        sums.append(total)
    image_unit_grad = half * sums[0] - LOGIT_SCALE * text_unit.astype(F32)
    text_unit_grad = half * sums[1] - LOGIT_SCALE * image_unit.astype(F32)
    image_grad[...] = unit_back(image_values, image_unit_grad)
    text_grad[...] = unit_back(text_values, text_unit_grad)

    for copy in [*image_sends.values(), *text_sends.values(), *passed.values()]:
        copy.wait_send()
    for copy in log_sends + part_sends:
        copy.wait_send()


def hand_out(image_from, text_from, image_to, text_to):
    image_to[...] = image_from[...]
    text_to[...] = text_from[...]


def body(captions, caption_layout, images, w_query, w_keyval, w_out, w_up, w_down, w_proj):
    hbm = pl.BlockSpec(memory_space=pl.ANY)
    vmem = pl.BlockSpec(memory_space=pltpu.VMEM)
    dma = pltpu.SemaphoreType.DMA
    grads = (jax.ShapeDtypeStruct((CAPS, WIDTH), F32),) * 2
    made = pl.pallas_call(
        kernel,
        out_shape=grads,
        in_specs=[hbm] * 9,
        out_specs=(vmem, vmem),
        scratch_shapes=[
            pltpu.VMEM((CTX, CAPS, WIDTH), BF16),
            pltpu.VMEM((GROUPS, TOKENS_PAD, WIDTH), BF16),
            pltpu.VMEM((WIDTH, WIDTH), BF16),
            pltpu.VMEM((WIDTH, 2 * WIDTH), BF16),
            pltpu.VMEM((WIDTH, WIDTH), BF16),
            pltpu.VMEM((WIDTH, FF), BF16),
            pltpu.VMEM((FF, WIDTH), BF16),
            pltpu.VMEM((WIDTH, WIDTH), BF16),
            pltpu.VMEM((2, 128), jnp.int32),
            pltpu.SMEM((2, 128), jnp.int32),
            pltpu.VMEM((CAPS, WIDTH), BF16),
            pltpu.VMEM((SPLIT, TOKENS_PAD), F32),
            pltpu.VMEM((GROUPS, GROUP, TOKENS_PAD), F32),
            pltpu.VMEM((SPLIT, TOKENS_PAD), BF16),
            pltpu.VMEM((2, 2, CHIPS, CAPS, WIDTH), BF16),
            pltpu.VMEM((2, HALF, ROWS), F32),
            pltpu.VMEM((2, HALF, ROWS), F32),
            pltpu.VMEM((2, HALF, 1), F32),
            pltpu.VMEM((2, 1, ROWS), F32),
            pltpu.VMEM((2, CHIPS, PIECES, 1, PIECE), F32),
            pltpu.VMEM((ROWS, ROWS), BF16),
            pltpu.VMEM((2, CHIPS, CAPS, WIDTH), BF16),
            pltpu.VMEM((2, CHIPS, CAPS, WIDTH), BF16),
            dma((3,)),
            dma((LOAD_STEPS,)),
            dma((6,)),
            dma((2, CHIPS)),
            dma((2, CHIPS)),
            dma((2, CHIPS)),
            dma((2, CHIPS)),
            dma((2, CHIPS)),
            dma((2, CHIPS)),
            dma((CHIPS, 2)),
            dma((2, CHIPS)),
        ],
        compiler_params=pltpu.CompilerParams(
            collective_id=0, has_side_effects=True, vmem_limit_bytes=60 * 1024 * 1024
        ),
    )(
        captions.transpose(1, 0, 2),
        caption_layout,
        images,
        w_query,
        w_keyval,
        w_out,
        w_up,
        w_down,
        w_proj,
    )
    return pl.pallas_call(hand_out, out_shape=grads, in_specs=[vmem] * 2, out_specs=(vmem, vmem))(*made)


def solution(mesh):
    return jax.shard_map(
        body,
        mesh=mesh,
        in_specs=(P("dp", None, None), P(), P("dp", None), P(), P(), P(), P(), P(), P()),
        out_specs=(P("dp", None), P("dp", None)),
        check_vma=False,
    )
```

```python
import math

import jax
import jax.numpy as jnp
from jax import lax
from jax.experimental import pallas as pl
from jax.experimental.pallas import tpu as pltpu
from jax.sharding import PartitionSpec as P

HEADS = 12
HEAD_DIM = 64
WIDTH = 768
CTX = 77
CAPS = 32
FF = 3072
GROUP = 16
GROUPS = CAPS // GROUP
SPLIT = HEADS * GROUP
TOKENS = CTX * GROUP
TOKENS_PAD = -(-TOKENS // 256) * 256
BLOCK = 256
BLOCK_HEADS = BLOCK // HEAD_DIM
LOAD_STEPS = 7
STEP_T = CTX // LOAD_STEPS
LOOP_STEPS = 7
CHIPS = 8
ROWS = CHIPS * 2 * CAPS
HALF = ROWS // 2
PIECE = 128
PIECES = ROWS // PIECE

VMEM_LIMIT = 60 * 1024 * 1024
LOGIT_SCALE = 100.0
EPS_NORM = 1e-05
EPS_UNIT = 1e-06
LOG2_E = math.log2(math.e)

MESH = pl.DeviceIdType.MESH
F32 = jnp.float32
BF16 = jnp.bfloat16


def norm_rows(values):
    center = values - jnp.mean(values, axis=-1, keepdims=True)
    spread = jnp.mean(center * center, axis=-1, keepdims=True)
    return center * lax.rsqrt(spread + EPS_NORM)


def unit_scale(values):
    return lax.rsqrt(jnp.sum(values * values, axis=-1, keepdims=True) + EPS_UNIT)


def unit_back(values, grad):
    scale = unit_scale(values)
    along = jnp.sum(values * grad, axis=-1, keepdims=True)
    return grad * scale - values * (along * (scale * scale * scale))


def dot(left, right):
    return jnp.dot(left, right, preferred_element_type=F32)


def dot_last(left, right):
    return lax.dot_general(left, right, (((1,), (1,)), ((), ())), preferred_element_type=F32)


def dot_first(left, right):
    return lax.dot_general(left, right, (((0,), (0,)), ((), ())), preferred_element_type=F32)


def iota(shape, dim):
    return lax.broadcasted_iota(jnp.int32, shape, dim)


class Place:
    def __init__(self):
        self.me = lax.axis_index("dp")
        self.core = self.me % 2
        self.at = {"y": (self.me // 2) % 4, "z": (self.me // 8) % 4, "x": self.me // 32}
        self.partner = self.me + 1 - 2 * self.core

    def flip(self, kind, value):
        image, text = 3 - value, value + 1 - 2 * (value % 2)
        return image + kind * (text - image)

    def bit(self, kind, value):
        return value // 2 + kind * (value % 2 - value // 2)

    def coords(self, kind, offset):
        return {
            axis: self.flip(kind, self.at[axis]) if offset >> step & 1 else self.at[axis]
            for step, axis in enumerate("yzx")
        }

    def peer(self, kind, offset, core):
        where = self.coords(kind, offset)
        return ((where["x"] * 4 + where["z"]) * 4 + where["y"]) * 2 + core

    def slot(self, kind, offset):
        where = self.coords(kind, offset)
        bits = {axis: self.bit(kind, where[axis]) for axis in "yzx"}
        return bits["x"] * 4 + bits["z"] * 2 + bits["y"]


def kernel(
    captions,
    layout,
    images,
    w_query,
    w_keyval,
    w_out,
    w_up,
    w_down,
    w_proj,
    image_grad,
    text_grad,
    tokens,
    normed,
    query_w,
    key_w,
    value_w,
    out_w,
    up_w,
    down_w,
    proj_w,
    counts,
    ends,
    image_rows,
    attn_scores,
    attn_bias,
    attn,
    units,
    row_exp,
    col_exp,
    row_peak,
    col_peak,
    logs,
    weight,
    blocks,
    parts,
    small_sem,
    load_sem,
    weight_sem,
    gather_send,
    gather_recv,
    pass_send,
    pass_recv,
    log_send,
    log_recv,
    part_send,
    part_recv,
):
    place = Place()
    me, core, partner = place.me, place.core, place.partner
    other = 1 - core

    def load(step):
        span = pl.ds(step * STEP_T, STEP_T)
        return pltpu.make_async_copy(captions.at[span], tokens.at[span], load_sem.at[step])

    span = pl.ds(pl.multiple_of(me // 4 * 128, 128), 128)
    load_counts = pltpu.make_async_copy(layout.at[:, span], counts, small_sem.at[0])
    load_images = pltpu.make_async_copy(images, image_rows, small_sem.at[1])
    load_ends = pltpu.make_async_copy(layout.at[:, span], ends, small_sem.at[2])
    weights = {}
    for number, (name, source, target) in enumerate(
        (
            ("query", w_query, query_w),
            ("key", w_keyval.at[:, :WIDTH], key_w),
            ("value", w_keyval.at[:, WIDTH:], value_w),
            ("out", w_out, out_w),
            ("up", w_up, up_w),
            ("down", w_down, down_w),
            ("proj", w_proj, proj_w),
        )
    ):
        weights[name] = pltpu.make_async_copy(source, target, weight_sem.at[number])
    for step in range(LOAD_STEPS):
        load(step).start()
    for copy in (load_counts, load_ends, load_images):
        copy.start()
    for copy in weights.values():
        copy.start(priority=1)

    barrier = pltpu.get_barrier_semaphore()
    friends = [partner]
    for offset in range(1, CHIPS):
        for kind in range(2):
            friends += [place.peer(kind, offset, 0), place.peer(kind, offset, 1)]
    for friend in friends:
        pl.semaphore_signal(barrier, inc=1, device_id=(friend,), device_id_type=MESH)

    normed[:, TOKENS:, :] = jnp.zeros((GROUPS, TOKENS_PAD - TOKENS, WIDTH), BF16)


    def norm_token(t):
        at = t * GROUP if isinstance(t, int) else pl.multiple_of(t * GROUP, GROUP)
        for group in range(GROUPS):
            values = tokens[t, group * GROUP : (group + 1) * GROUP, :].astype(F32)
            normed[group, pl.ds(at, GROUP), :] = norm_rows(values).astype(BF16)

    def norm_step(step, _):
        load(step).wait()
        for inner in range(STEP_T):
            norm_token(step * STEP_T + inner)
        return 0

    lax.fori_loop(0, LOOP_STEPS, norm_step, 0)
    for step in range(LOOP_STEPS, LOAD_STEPS):
        load(step).wait()

    load_ends.wait()
    load_counts.wait()
    weights["query"].wait()
    weights["key"].wait()
    end_values = []
    for group in range(GROUPS):
        rows = jnp.zeros((GROUP, WIDTH), BF16)
        for inner in range(GROUP):
            caption = group * GROUP + inner
            last = jnp.clip(ends[0, me % 4 * CAPS + caption] - 1, 0, CTX - 1)
            found = tokens[last, group * GROUP : (group + 1) * GROUP, :]
            rows = jnp.where(iota((GROUP, WIDTH), 0) == inner, found, rows)
        end_values.append(rows)
    end_values = jnp.concatenate(end_values, axis=0).astype(F32)
    end_normed = norm_rows(end_values).astype(BF16)
    head_of = iota((GROUP, BLOCK), 1) // HEAD_DIM
    groups = [slice(group * GROUP, (group + 1) * GROUP) for group in range(GROUPS)]
    spans = [slice(at, at + BLOCK) for at in range(0, WIDTH, BLOCK)]
    key_query = []
    for span in spans:
        query = dot(end_normed, query_w[:, span]).astype(BF16).astype(F32)
        query = query * (1.0 / math.sqrt(HEAD_DIM))
        spread = [
            jnp.where(head_of == head, query[rows], 0.0)
            for rows in groups
            for head in range(BLOCK_HEADS)
        ]
        spread = jnp.concatenate(spread, axis=0).astype(BF16)
        key_query.append((dot_last(spread, key_w[:, span]) * LOG2_E).astype(BF16))
    for t in range(LOOP_STEPS * STEP_T, CTX):
        norm_token(t)

    picked = iota((CAPS, 128), 1) == iota((CAPS, 128), 0) + me % 4 * CAPS
    lengths = jnp.sum(jnp.where(picked, counts[0:1, :].astype(F32), 0.0), axis=1, keepdims=True)
    lengths = jnp.maximum(lengths, 1.0)

    token = iota((GROUP, TOKENS_PAD), 1)
    own = token % GROUP == iota((GROUP, TOKENS_PAD), 0)
    for group in range(GROUPS):
        count = lengths[group * GROUP : (group + 1) * GROUP]
        inside = own & ((token // GROUP).astype(F32) < count)
        attn_bias[group] = jnp.where(inside, 0.0, -jnp.inf)

    part = BLOCK_HEADS * GROUP
    contexts = []
    for group in range(GROUPS):
        rows = slice(group * part, (group + 1) * part)
        asked = jnp.concatenate([block[rows] for block in key_query], axis=0)
        attn_scores[...] = dot_last(asked, normed[group])
        totals = []
        for head in range(HEADS):
            rows = slice(head * GROUP, (head + 1) * GROUP)
            value = attn_scores[rows, :] + attn_bias[group]
            value = jnp.exp2(value - jnp.max(value, axis=1, keepdims=True))
            attn[rows, :] = value.astype(BF16)
            totals.append(jnp.sum(value, axis=1, keepdims=True))
        context = dot(attn[...], normed[group]) / jnp.concatenate(totals, axis=0)
        contexts.append(context.astype(BF16))

    load_images.wait()
    image_values = image_rows[...].astype(F32)
    image_unit = (image_values * unit_scale(image_values)).astype(BF16)
    slots = (place.slot(0, 0), place.slot(1, 0))
    units[0, 0, slots[0]] = image_unit

    pl.semaphore_wait(barrier, len(friends))

    def send_units(kind):
        copies = {}
        for offset in range(CHIPS - 1, 0, -1):
            copies[offset] = pltpu.make_async_remote_copy(
                src_ref=units.at[kind, 0, slots[kind]],
                dst_ref=units.at[kind, 0, slots[kind]],
                send_sem=gather_send.at[kind, offset],
                recv_sem=gather_recv.at[kind, offset],
                device_id=(place.peer(kind, offset, core),),
                device_id_type=MESH,
            )
            copies[offset].start()
        return copies

    def hand_on(kind, offset):
        slot = place.slot(kind, offset)
        copy = pltpu.make_async_remote_copy(
            src_ref=units.at[kind, 0, slot],
            dst_ref=units.at[kind, 1, slot],
            send_sem=pass_send.at[kind, offset],
            recv_sem=pass_recv.at[kind, offset],
            device_id=(partner,),
            device_id_type=MESH,
        )
        copy.start()
        return copy

    image_sends = send_units(0)
    passed = {(0, 0): hand_on(0, 0)}

    for name in ("value", "out", "up", "down", "proj"):
        weights[name].wait()
    mixed = []
    for number, span in enumerate(spans):
        rows = slice(number * part, (number + 1) * part)
        by_head = jnp.concatenate([context[rows] for context in contexts], axis=0)
        by_head = dot(by_head, value_w[:, span])
        sums = []
        for group in range(GROUPS):
            total = jnp.zeros((GROUP, BLOCK), F32)
            for head in range(BLOCK_HEADS):
                first = group * part + head * GROUP
                total = total + jnp.where(head_of == head, by_head[first : first + GROUP], 0.0)
            sums.append(total)
        mixed.append(jnp.concatenate(sums, axis=0))
    mixed = jnp.concatenate(mixed, axis=1).astype(BF16)

    residual = (end_values + dot(mixed, out_w[...])).astype(BF16)
    residual = residual.astype(F32)
    inner = norm_rows(residual).astype(BF16)
    final = residual
    for part in range(FF // WIDTH):
        span = slice(part * WIDTH, (part + 1) * WIDTH)
        hidden = dot(inner, up_w[:, span])
        hidden = 0.5 * hidden * (1.0 + lax.erf(hidden * (1.0 / math.sqrt(2.0))))
        final = final + dot(hidden.astype(BF16), down_w[span, :])
    pooled = norm_rows(final).astype(BF16)
    text_values = dot(pooled, proj_w[...]).astype(BF16).astype(F32)
    text_unit = (text_values * unit_scale(text_values)).astype(BF16)
    units[1, 0, slots[1]] = text_unit

    text_sends = send_units(1)
    passed[1, 0] = hand_on(1, 0)

    for offset in range(1, CHIPS):
        image_sends[offset].wait_recv()
        passed[0, offset] = hand_on(0, offset)

    for offset in range(CHIPS - 1, 0, -1):
        text_sends[offset].wait_recv()
        passed[1, offset] = hand_on(1, offset)
    for offset in range(CHIPS):
        passed[0, offset].wait_recv()

    eye = iota((PIECE, PIECE), 0) == iota((PIECE, PIECE), 1)
    col_sums, col_peaks = [], []
    for half in range(2):
        if half == 1:
            for offset in range(CHIPS):
                passed[1, offset].wait_recv()
        scores = dot_last(units[1, half].reshape(HALF, WIDTH), units[0].reshape(ROWS, WIDTH))
        scores = scores * (LOGIT_SCALE * LOG2_E)
        peak = jnp.max(scores, axis=1, keepdims=True)
        value = jnp.exp2(scores - peak)
        row_exp[half] = value
        row_peak[half] = peak
        log = peak + jnp.log(jnp.sum(value, axis=1, keepdims=True)) * LOG2_E
        for piece in range(HALF // PIECE):
            part = log[piece * PIECE : (piece + 1) * PIECE]
            part = jnp.sum(jnp.where(eye, part, 0.0), axis=0, keepdims=True)
            logs[1, 0, half * (HALF // PIECE) + piece] = part
        peak = jnp.max(scores, axis=0, keepdims=True)
        value = jnp.exp2(scores - peak)
        col_exp[half] = value
        col_peak[half] = peak
        col_peaks.append(peak)
        col_sums.append(jnp.sum(value, axis=0, keepdims=True))
    top = jnp.maximum(*col_peaks)
    total = sum(part * jnp.exp2(peak - top) for part, peak in zip(col_sums, col_peaks))
    log = top + jnp.log(total) * LOG2_E
    for piece in range(PIECES):
        logs[0, 0, piece] = log[:, piece * PIECE : (piece + 1) * PIECE]

    log_sends = []
    for offset in range(CHIPS - 1, 0, -1):
        for kind in range(2):
            copy = pltpu.make_async_remote_copy(
                src_ref=logs.at[kind, 0],
                dst_ref=logs.at[kind, offset],
                send_sem=log_send.at[kind, offset],
                recv_sem=log_recv.at[kind, offset],
                device_id=(place.peer(kind, offset, core),),
                device_id_type=MESH,
            )
            copy.start()
            log_sends.append(copy)
    for copy in log_sends:
        copy.wait_recv()

    def whole_log(kind):
        top = logs[kind, 0]
        for offset in range(1, CHIPS):
            top = jnp.maximum(top, logs[kind, offset])
        total = jnp.zeros_like(top)
        for offset in range(CHIPS):
            total = total + jnp.exp2(logs[kind, offset] - top)
        return top + jnp.log(total) * LOG2_E

    image_logs, text_logs = whole_log(0), whole_log(1)
    image_logs = jnp.concatenate([image_logs[piece] for piece in range(PIECES)], axis=1)
    for half in range(2):
        col_scale = jnp.exp2(col_peak[half] - image_logs)
        for piece in range(HALF // PIECE):
            rows = slice(piece * PIECE, (piece + 1) * PIECE)
            first = half * HALF + piece * PIECE
            log = text_logs[half * (HALF // PIECE) + piece]
            log = jnp.sum(jnp.where(eye, log, 0.0), axis=1, keepdims=True)
            row_scale = jnp.exp2(row_peak[half, rows] - log)
            both = row_exp[half, rows] * row_scale + col_exp[half, rows] * col_scale
            weight[first : first + PIECE, :] = both.astype(BF16)

    part_sends = []
    for far in (1, 0):
        first = place.slot(core, 4 * far) // 4 * 4
        spans = [
            pl.ds(pl.multiple_of(side * HALF + first * CAPS, PIECE), PIECE) for side in range(2)
        ]

        def keep(grad):
            blocks[:, pl.ds(first, 4)] = grad.astype(BF16).reshape(2, 4, CAPS, WIDTH)

        @pl.when(core == 0)
        def _():
            columns = jnp.concatenate([weight[:, span] for span in spans], axis=1)
            keep(dot_first(columns, units[1].reshape(ROWS, WIDTH)))

        @pl.when(core == 1)
        def _():
            rows = jnp.concatenate([weight[span, :] for span in spans], axis=0)
            keep(dot(rows, units[0].reshape(ROWS, WIDTH)))

        for offset in range(4 * far + 3, 4 * far - 1, -1):
            slot = place.slot(core, offset)
            for side in range(2):
                if offset == 0 and side == 0:
                    parts[core, 0] = blocks[0, slot]
                    continue
                copy = pltpu.make_async_remote_copy(
                    src_ref=blocks.at[side, slot],
                    dst_ref=parts.at[core, offset],
                    send_sem=part_send.at[offset, side],
                    recv_sem=part_recv.at[core, offset],
                    device_id=(place.peer(core, offset, core + side - 2 * side * core),),
                    device_id_type=MESH,
                )
                copy.start()
                part_sends.append(copy)

    def arrived(kind, offset):
        pltpu.make_async_remote_copy(
            src_ref=parts.at[kind, offset],
            dst_ref=parts.at[kind, offset],
            send_sem=part_send.at[0, 0],
            recv_sem=part_recv.at[kind, offset],
            device_id=(partner,),
            device_id_type=MESH,
        ).wait_recv()

    arrived(other, 0)
    for offset in range(1, CHIPS):
        for kind in range(2):
            arrived(kind, offset)

    half = 0.5 * LOGIT_SCALE
    sums = []
    for kind in range(2):
        total = parts[kind, 0].astype(F32)
        for offset in range(1, CHIPS):
            total = total + parts[kind, offset].astype(F32)
        sums.append(total)
    image_unit_grad = half * sums[0] - LOGIT_SCALE * text_unit.astype(F32)
    text_unit_grad = half * sums[1] - LOGIT_SCALE * image_unit.astype(F32)
    image_grad[...] = unit_back(image_values, image_unit_grad)
    text_grad[...] = unit_back(text_values, text_unit_grad)

    for copy in [*image_sends.values(), *text_sends.values(), *passed.values()]:
        copy.wait_send()
    for copy in log_sends + part_sends:
        copy.wait_send()


def hand_out(image_from, text_from, image_to, text_to):
    image_to[...] = image_from[...]
    text_to[...] = text_from[...]


def body(captions, caption_layout, images, w_query, w_keyval, w_out, w_up, w_down, w_proj):
    hbm = pl.BlockSpec(memory_space=pl.ANY)
    vmem = pl.BlockSpec(memory_space=pltpu.VMEM)
    dma = pltpu.SemaphoreType.DMA
    grads = (jax.ShapeDtypeStruct((CAPS, WIDTH), F32),) * 2
    made = pl.pallas_call(
        kernel,
        out_shape=(pltpu.VMEM((CAPS, WIDTH), F32),) * 2,
        in_specs=[hbm] * 9,
        out_specs=(vmem, vmem),
        scratch_shapes=[
            pltpu.VMEM((CTX, CAPS, WIDTH), BF16),
            pltpu.VMEM((GROUPS, TOKENS_PAD, WIDTH), BF16),
            pltpu.VMEM((WIDTH, WIDTH), BF16),
            pltpu.VMEM((WIDTH, WIDTH), BF16),
            pltpu.VMEM((WIDTH, WIDTH), BF16),
            pltpu.VMEM((WIDTH, WIDTH), BF16),
            pltpu.VMEM((WIDTH, FF), BF16),
            pltpu.VMEM((FF, WIDTH), BF16),
            pltpu.VMEM((WIDTH, WIDTH), BF16),
            pltpu.VMEM((2, 128), jnp.int32),
            pltpu.SMEM((2, 128), jnp.int32),
            pltpu.VMEM((CAPS, WIDTH), BF16),
            pltpu.VMEM((SPLIT, TOKENS_PAD), F32),
            pltpu.VMEM((GROUPS, GROUP, TOKENS_PAD), F32),
            pltpu.VMEM((SPLIT, TOKENS_PAD), BF16),
            pltpu.VMEM((2, 2, CHIPS, CAPS, WIDTH), BF16),
            pltpu.VMEM((2, HALF, ROWS), F32),
            pltpu.VMEM((2, HALF, ROWS), F32),
            pltpu.VMEM((2, HALF, 1), F32),
            pltpu.VMEM((2, 1, ROWS), F32),
            pltpu.VMEM((2, CHIPS, PIECES, 1, PIECE), F32),
            pltpu.VMEM((ROWS, ROWS), BF16),
            pltpu.VMEM((2, CHIPS, CAPS, WIDTH), BF16),
            pltpu.VMEM((2, CHIPS, CAPS, WIDTH), BF16),
            dma((3,)),
            dma((LOAD_STEPS,)),
            dma((7,)),
            dma((2, CHIPS)),
            dma((2, CHIPS)),
            dma((2, CHIPS)),
            dma((2, CHIPS)),
            dma((2, CHIPS)),
            dma((2, CHIPS)),
            dma((CHIPS, 2)),
            dma((2, CHIPS)),
        ],
        compiler_params=pltpu.CompilerParams(
            collective_id=0, has_side_effects=True, vmem_limit_bytes=VMEM_LIMIT
        ),
    )(
        captions.transpose(1, 0, 2),
        caption_layout,
        images,
        w_query,
        w_keyval,
        w_out,
        w_up,
        w_down,
        w_proj,
    )
    return pl.pallas_call(
        hand_out,
        out_shape=grads,
        in_specs=[vmem] * 2,
        out_specs=(vmem, vmem),
        compiler_params=pltpu.CompilerParams(vmem_limit_bytes=4 * 1024 * 1024),
    )(*made)


def solution(mesh):
    return jax.shard_map(
        body,
        mesh=mesh,
        in_specs=(P("dp", None, None), P(), P("dp", None), P(), P(), P(), P(), P(), P()),
        out_specs=(P("dp", None), P("dp", None)),
        check_vma=False,
    )
```

```python
import math

import jax
import jax.numpy as jnp
from jax import lax
from jax.experimental import pallas as pl
from jax.experimental.pallas import tpu as pltpu
from jax.sharding import PartitionSpec as P

HEADS = 12
HEAD_DIM = 64
WIDTH = 768
CTX = 77
CAPS = 32
FF = 3072
GROUP = 16
GROUPS = CAPS // GROUP
SPLIT = HEADS * GROUP
TOKENS = CTX * GROUP
TOKENS_PAD = -(-TOKENS // 256) * 256
BLOCK = 256
BLOCK_HEADS = BLOCK // HEAD_DIM
LOAD_STEPS = 7
STEP_T = CTX // LOAD_STEPS
LOOP_STEPS = 7
CHIPS = 8
ARRIVAL = (7, 1, 6, 3, 2, 5, 4)
ROWS = CHIPS * 2 * CAPS
HALF = ROWS // 2
PIECE = 128
PIECES = ROWS // PIECE

VMEM_LIMIT = 60 * 1024 * 1024
LOGIT_SCALE = 100.0
EPS_NORM = 1e-05
EPS_UNIT = 1e-06
LOG2_E = math.log2(math.e)

MESH = pl.DeviceIdType.MESH
F32 = jnp.float32
BF16 = jnp.bfloat16


def norm_rows(values):
    center = values - jnp.mean(values, axis=-1, keepdims=True)
    spread = jnp.mean(center * center, axis=-1, keepdims=True)
    return center * lax.rsqrt(spread + EPS_NORM)


def unit_scale(values):
    return lax.rsqrt(jnp.sum(values * values, axis=-1, keepdims=True) + EPS_UNIT)


def unit_back(values, grad):
    scale = unit_scale(values)
    along = jnp.sum(values * grad, axis=-1, keepdims=True)
    return grad * scale - values * (along * (scale * scale * scale))


def dot(left, right):
    return jnp.dot(left, right, preferred_element_type=F32)


def dot_last(left, right):
    return lax.dot_general(left, right, (((1,), (1,)), ((), ())), preferred_element_type=F32)


def dot_first(left, right):
    return lax.dot_general(left, right, (((0,), (0,)), ((), ())), preferred_element_type=F32)


def iota(shape, dim):
    return lax.broadcasted_iota(jnp.int32, shape, dim)


class Place:
    def __init__(self):
        self.me = lax.axis_index("dp")
        self.core = self.me % 2
        self.at = {"y": (self.me // 2) % 4, "z": (self.me // 8) % 4, "x": self.me // 32}
        self.partner = self.me + 1 - 2 * self.core

    def flip(self, kind, value):
        image, text = 3 - value, value + 1 - 2 * (value % 2)
        return image + kind * (text - image)

    def bit(self, kind, value):
        return value // 2 + kind * (value % 2 - value // 2)

    def coords(self, kind, offset):
        return {
            axis: self.flip(kind, self.at[axis]) if offset >> step & 1 else self.at[axis]
            for step, axis in enumerate("yzx")
        }

    def peer(self, kind, offset, core):
        where = self.coords(kind, offset)
        return ((where["x"] * 4 + where["z"]) * 4 + where["y"]) * 2 + core

    def slot(self, kind, offset):
        where = self.coords(kind, offset)
        bits = {axis: self.bit(kind, where[axis]) for axis in "yzx"}
        return bits["x"] * 4 + bits["z"] * 2 + bits["y"]


def kernel(
    captions,
    layout,
    images,
    w_query,
    w_keyval,
    w_out,
    w_up,
    w_down,
    w_proj,
    image_grad,
    text_grad,
    tokens,
    normed,
    query_w,
    key_w,
    value_w,
    out_w,
    up_w,
    down_w,
    proj_w,
    counts,
    ends,
    image_rows,
    attn_scores,
    attn_bias,
    attn,
    units,
    row_exp,
    col_exp,
    row_peak,
    col_peak,
    logs,
    weight,
    blocks,
    parts,
    small_sem,
    load_sem,
    weight_sem,
    gather_send,
    gather_recv,
    pass_send,
    pass_recv,
    log_send,
    log_recv,
    part_send,
    part_recv,
):
    place = Place()
    me, core, partner = place.me, place.core, place.partner

    def load(step):
        span = pl.ds(step * STEP_T, STEP_T)
        return pltpu.make_async_copy(captions.at[span], tokens.at[span], load_sem.at[step])

    span = pl.ds(pl.multiple_of(me // 4 * 128, 128), 128)
    load_counts = pltpu.make_async_copy(layout.at[:, span], counts, small_sem.at[0])
    load_images = pltpu.make_async_copy(images, image_rows, small_sem.at[1])
    load_ends = pltpu.make_async_copy(layout.at[:, span], ends, small_sem.at[2])
    weights = {}
    for number, (name, source, target) in enumerate(
        (
            ("query", w_query, query_w),
            ("key", w_keyval.at[:, :WIDTH], key_w),
            ("value", w_keyval.at[:, WIDTH:], value_w),
            ("out", w_out, out_w),
            ("up", w_up, up_w),
            ("down", w_down, down_w),
            ("proj", w_proj, proj_w),
        )
    ):
        weights[name] = pltpu.make_async_copy(source, target, weight_sem.at[number])
    for step in range(LOAD_STEPS):
        load(step).start()
    for copy in (load_counts, load_ends, load_images):
        copy.start()
    for copy in weights.values():
        copy.start(priority=1)

    barrier = pltpu.get_barrier_semaphore()
    friends = [partner]
    for offset in range(1, CHIPS):
        for kind in range(2):
            friends += [place.peer(kind, offset, 0), place.peer(kind, offset, 1)]
    for friend in friends:
        pl.semaphore_signal(barrier, inc=1, device_id=(friend,), device_id_type=MESH)

    normed[:, TOKENS:, :] = jnp.zeros((GROUPS, TOKENS_PAD - TOKENS, WIDTH), BF16)


    def norm_token(t):
        at = t * GROUP if isinstance(t, int) else pl.multiple_of(t * GROUP, GROUP)
        for group in range(GROUPS):
            values = tokens[t, group * GROUP : (group + 1) * GROUP, :].astype(F32)
            normed[group, pl.ds(at, GROUP), :] = norm_rows(values).astype(BF16)

    def norm_step(step, _):
        load(step).wait()
        for inner in range(STEP_T):
            norm_token(step * STEP_T + inner)
        return 0

    lax.fori_loop(0, LOOP_STEPS, norm_step, 0)
    for step in range(LOOP_STEPS, LOAD_STEPS):
        load(step).wait()

    load_ends.wait()
    load_counts.wait()
    weights["query"].wait()
    weights["key"].wait()
    end_values = []
    for group in range(GROUPS):
        rows = jnp.zeros((GROUP, WIDTH), BF16)
        for inner in range(GROUP):
            caption = group * GROUP + inner
            last = jnp.clip(ends[0, me % 4 * CAPS + caption] - 1, 0, CTX - 1)
            found = tokens[last, group * GROUP : (group + 1) * GROUP, :]
            rows = jnp.where(iota((GROUP, WIDTH), 0) == inner, found, rows)
        end_values.append(rows)
    end_values = jnp.concatenate(end_values, axis=0).astype(F32)
    end_normed = norm_rows(end_values).astype(BF16)
    head_of = iota((GROUP, BLOCK), 1) // HEAD_DIM
    groups = [slice(group * GROUP, (group + 1) * GROUP) for group in range(GROUPS)]
    spans = [slice(at, at + BLOCK) for at in range(0, WIDTH, BLOCK)]
    key_query = []
    for span in spans:
        query = dot(end_normed, query_w[:, span]).astype(BF16).astype(F32)
        query = query * (1.0 / math.sqrt(HEAD_DIM))
        spread = [
            jnp.where(head_of == head, query[rows], 0.0)
            for rows in groups
            for head in range(BLOCK_HEADS)
        ]
        spread = jnp.concatenate(spread, axis=0).astype(BF16)
        key_query.append((dot_last(spread, key_w[:, span]) * LOG2_E).astype(BF16))
    for t in range(LOOP_STEPS * STEP_T, CTX):
        norm_token(t)

    picked = iota((CAPS, 128), 1) == iota((CAPS, 128), 0) + me % 4 * CAPS
    lengths = jnp.sum(jnp.where(picked, counts[0:1, :].astype(F32), 0.0), axis=1, keepdims=True)
    lengths = jnp.maximum(lengths, 1.0)

    token = iota((GROUP, TOKENS_PAD), 1)
    own = token % GROUP == iota((GROUP, TOKENS_PAD), 0)
    for group in range(GROUPS):
        count = lengths[group * GROUP : (group + 1) * GROUP]
        inside = own & ((token // GROUP).astype(F32) < count)
        attn_bias[group] = jnp.where(inside, 0.0, -jnp.inf)

    part = BLOCK_HEADS * GROUP
    contexts = []
    for group in range(GROUPS):
        rows = slice(group * part, (group + 1) * part)
        asked = jnp.concatenate([block[rows] for block in key_query], axis=0)
        attn_scores[group] = dot_last(asked, normed[group])
    for group in range(GROUPS):
        totals = []
        for head in range(HEADS):
            rows = slice(head * GROUP, (head + 1) * GROUP)
            value = attn_scores[group, rows, :] + attn_bias[group]
            value = jnp.exp2(value - jnp.max(value, axis=1, keepdims=True))
            attn[group, rows, :] = value.astype(BF16)
            totals.append(jnp.sum(value, axis=1, keepdims=True))
        context = dot(attn[group], normed[group]) / jnp.concatenate(totals, axis=0)
        contexts.append(context.astype(BF16))

    load_images.wait()
    image_values = image_rows[...].astype(F32)
    image_unit = (image_values * unit_scale(image_values)).astype(BF16)
    slots = (place.slot(0, 0), place.slot(1, 0))
    units[0, 0, slots[0]] = image_unit

    pl.semaphore_wait(barrier, len(friends))

    def send_units(kind):
        copies = {}
        for offset in range(CHIPS - 1, 0, -1):
            copies[offset] = pltpu.make_async_remote_copy(
                src_ref=units.at[kind, 0, slots[kind]],
                dst_ref=units.at[kind, 0, slots[kind]],
                send_sem=gather_send.at[kind, offset],
                recv_sem=gather_recv.at[kind, offset],
                device_id=(place.peer(kind, offset, core),),
                device_id_type=MESH,
            )
            copies[offset].start()
        return copies

    def hand_on(kind, offset):
        slot = place.slot(kind, offset)
        copy = pltpu.make_async_remote_copy(
            src_ref=units.at[kind, 0, slot],
            dst_ref=units.at[kind, 1, slot],
            send_sem=pass_send.at[kind, offset],
            recv_sem=pass_recv.at[kind, offset],
            device_id=(partner,),
            device_id_type=MESH,
        )
        copy.start()
        return copy

    image_sends = send_units(0)
    passed = {(0, 0): hand_on(0, 0)}

    for name in ("value", "out", "up", "down", "proj"):
        weights[name].wait()
    mixed = []
    for number, span in enumerate(spans):
        rows = slice(number * part, (number + 1) * part)
        by_head = jnp.concatenate([context[rows] for context in contexts], axis=0)
        by_head = dot(by_head, value_w[:, span])
        sums = []
        for group in range(GROUPS):
            total = jnp.zeros((GROUP, BLOCK), F32)
            for head in range(BLOCK_HEADS):
                first = group * part + head * GROUP
                total = total + jnp.where(head_of == head, by_head[first : first + GROUP], 0.0)
            sums.append(total)
        mixed.append(jnp.concatenate(sums, axis=0))
    mixed = jnp.concatenate(mixed, axis=1).astype(BF16)

    residual = (end_values + dot(mixed, out_w[...])).astype(BF16)
    residual = residual.astype(F32)
    inner = norm_rows(residual).astype(BF16)
    final = residual
    for part in range(FF // WIDTH):
        span = slice(part * WIDTH, (part + 1) * WIDTH)
        hidden = dot(inner, up_w[:, span])
        hidden = 0.5 * hidden * (1.0 + lax.erf(hidden * (1.0 / math.sqrt(2.0))))
        final = final + dot(hidden.astype(BF16), down_w[span, :])
    pooled = norm_rows(final).astype(BF16)
    text_values = dot(pooled, proj_w[...]).astype(BF16).astype(F32)
    text_unit = (text_values * unit_scale(text_values)).astype(BF16)
    units[1, 0, slots[1]] = text_unit

    text_sends = send_units(1)
    passed[1, 0] = hand_on(1, 0)

    for offset in range(1, CHIPS):
        image_sends[offset].wait_recv()
        passed[0, offset] = hand_on(0, offset)

    for offset in ARRIVAL:
        text_sends[offset].wait_recv()
        passed[1, offset] = hand_on(1, offset)
    for offset in range(CHIPS):
        passed[0, offset].wait_recv()

    eye = iota((PIECE, PIECE), 0) == iota((PIECE, PIECE), 1)
    col_sums, col_peaks = [], []
    for half in range(2):
        if half == 1:
            for offset in range(CHIPS):
                passed[1, offset].wait_recv()
        scores = dot_last(units[1, half].reshape(HALF, WIDTH), units[0].reshape(ROWS, WIDTH))
        scores = scores * (LOGIT_SCALE * LOG2_E)
        peak = jnp.max(scores, axis=1, keepdims=True)
        value = jnp.exp2(scores - peak)
        row_exp[half] = value
        row_peak[half] = peak
        log = peak + jnp.log(jnp.sum(value, axis=1, keepdims=True)) * LOG2_E
        for piece in range(HALF // PIECE):
            part = log[piece * PIECE : (piece + 1) * PIECE]
            part = jnp.sum(jnp.where(eye, part, 0.0), axis=0, keepdims=True)
            logs[1, 0, half * (HALF // PIECE) + piece] = part
        peak = jnp.max(scores, axis=0, keepdims=True)
        value = jnp.exp2(scores - peak)
        col_exp[half] = value
        col_peak[half] = peak
        col_peaks.append(peak)
        col_sums.append(jnp.sum(value, axis=0, keepdims=True))
    top = jnp.maximum(*col_peaks)
    total = sum(part * jnp.exp2(peak - top) for part, peak in zip(col_sums, col_peaks))
    log = top + jnp.log(total) * LOG2_E
    for piece in range(PIECES):
        logs[0, 0, piece] = log[:, piece * PIECE : (piece + 1) * PIECE]

    log_sends = []
    for offset in range(CHIPS - 1, 0, -1):
        for kind in range(2):
            copy = pltpu.make_async_remote_copy(
                src_ref=logs.at[kind, 0],
                dst_ref=logs.at[kind, offset],
                send_sem=log_send.at[kind, offset],
                recv_sem=log_recv.at[kind, offset],
                device_id=(place.peer(kind, offset, core),),
                device_id_type=MESH,
            )
            copy.start()
            log_sends.append(copy)
    for copy in log_sends:
        copy.wait_recv()

    def whole_log(kind):
        top = logs[kind, 0]
        for offset in range(1, CHIPS):
            top = jnp.maximum(top, logs[kind, offset])
        total = jnp.zeros_like(top)
        for offset in range(CHIPS):
            total = total + jnp.exp2(logs[kind, offset] - top)
        return top + jnp.log(total) * LOG2_E

    image_logs, text_logs = whole_log(0), whole_log(1)
    image_logs = jnp.concatenate([image_logs[piece] for piece in range(PIECES)], axis=1)
    for half in range(2):
        col_scale = jnp.exp2(col_peak[half] - image_logs)
        for piece in range(HALF // PIECE):
            rows = slice(piece * PIECE, (piece + 1) * PIECE)
            first = half * HALF + piece * PIECE
            log = text_logs[half * (HALF // PIECE) + piece]
            log = jnp.sum(jnp.where(eye, log, 0.0), axis=1, keepdims=True)
            row_scale = jnp.exp2(row_peak[half, rows] - log)
            both = row_exp[half, rows] * row_scale + col_exp[half, rows] * col_scale
            weight[first : first + PIECE, :] = both.astype(BF16)

    duty = 1 - core
    part_sends = []
    for far in (1, 0):
        first = place.slot(duty, 4 * far) // 4 * 4
        spans = [
            pl.ds(pl.multiple_of(side * HALF + first * CAPS, PIECE), PIECE) for side in range(2)
        ]

        def keep(grad):
            blocks[:, pl.ds(first, 4)] = grad.astype(BF16).reshape(2, 4, CAPS, WIDTH)

        @pl.when(duty == 0)
        def _():
            columns = jnp.concatenate([weight[:, span] for span in spans], axis=1)
            keep(dot_first(columns, units[1].reshape(ROWS, WIDTH)))

        @pl.when(duty == 1)
        def _():
            rows = jnp.concatenate([weight[span, :] for span in spans], axis=0)
            keep(dot(rows, units[0].reshape(ROWS, WIDTH)))

        for offset in range(4 * far + 3, 4 * far - 1, -1):
            slot = place.slot(duty, offset)
            for side in range(2):
                if offset == 0 and side == 0:
                    parts[duty, 0] = blocks[0, slot]
                    continue
                copy = pltpu.make_async_remote_copy(
                    src_ref=blocks.at[side, slot],
                    dst_ref=parts.at[duty, offset],
                    send_sem=part_send.at[offset, side],
                    recv_sem=part_recv.at[duty, offset],
                    device_id=(place.peer(duty, offset, core + side - 2 * side * core),),
                    device_id_type=MESH,
                )
                copy.start()
                part_sends.append(copy)

    def arrived(kind, offset):
        pltpu.make_async_remote_copy(
            src_ref=parts.at[kind, offset],
            dst_ref=parts.at[kind, offset],
            send_sem=part_send.at[0, 0],
            recv_sem=part_recv.at[kind, offset],
            device_id=(partner,),
            device_id_type=MESH,
        ).wait_recv()

    arrived(core, 0)
    for offset in range(1, CHIPS):
        for kind in range(2):
            arrived(kind, offset)

    half = 0.5 * LOGIT_SCALE
    sums = []
    for kind in range(2):
        total = parts[kind, 0].astype(F32)
        for offset in range(1, CHIPS):
            total = total + parts[kind, offset].astype(F32)
        sums.append(total)
    image_unit_grad = half * sums[0] - LOGIT_SCALE * text_unit.astype(F32)
    text_unit_grad = half * sums[1] - LOGIT_SCALE * image_unit.astype(F32)
    image_grad[...] = unit_back(image_values, image_unit_grad)
    text_grad[...] = unit_back(text_values, text_unit_grad)

    for copy in [*image_sends.values(), *text_sends.values(), *passed.values()]:
        copy.wait_send()
    for copy in log_sends + part_sends:
        copy.wait_send()


def hand_out(image_from, text_from, image_to, text_to):
    image_to[...] = image_from[...]
    text_to[...] = text_from[...]


def body(captions, caption_layout, images, w_query, w_keyval, w_out, w_up, w_down, w_proj):
    hbm = pl.BlockSpec(memory_space=pl.ANY)
    vmem = pl.BlockSpec(memory_space=pltpu.VMEM)
    dma = pltpu.SemaphoreType.DMA
    grads = (jax.ShapeDtypeStruct((CAPS, WIDTH), F32),) * 2
    made = pl.pallas_call(
        kernel,
        out_shape=(pltpu.VMEM((CAPS, WIDTH), F32),) * 2,
        in_specs=[hbm] * 9,
        out_specs=(vmem, vmem),
        scratch_shapes=[
            pltpu.VMEM((CTX, CAPS, WIDTH), BF16),
            pltpu.VMEM((GROUPS, TOKENS_PAD, WIDTH), BF16),
            pltpu.VMEM((WIDTH, WIDTH), BF16),
            pltpu.VMEM((WIDTH, WIDTH), BF16),
            pltpu.VMEM((WIDTH, WIDTH), BF16),
            pltpu.VMEM((WIDTH, WIDTH), BF16),
            pltpu.VMEM((WIDTH, FF), BF16),
            pltpu.VMEM((FF, WIDTH), BF16),
            pltpu.VMEM((WIDTH, WIDTH), BF16),
            pltpu.VMEM((2, 128), jnp.int32),
            pltpu.SMEM((2, 128), jnp.int32),
            pltpu.VMEM((CAPS, WIDTH), BF16),
            pltpu.VMEM((GROUPS, SPLIT, TOKENS_PAD), F32),
            pltpu.VMEM((GROUPS, GROUP, TOKENS_PAD), F32),
            pltpu.VMEM((GROUPS, SPLIT, TOKENS_PAD), BF16),
            pltpu.VMEM((2, 2, CHIPS, CAPS, WIDTH), BF16),
            pltpu.VMEM((2, HALF, ROWS), F32),
            pltpu.VMEM((2, HALF, ROWS), F32),
            pltpu.VMEM((2, HALF, 1), F32),
            pltpu.VMEM((2, 1, ROWS), F32),
            pltpu.VMEM((2, CHIPS, PIECES, 1, PIECE), F32),
            pltpu.VMEM((ROWS, ROWS), BF16),
            pltpu.VMEM((2, CHIPS, CAPS, WIDTH), BF16),
            pltpu.VMEM((2, CHIPS, CAPS, WIDTH), BF16),
            dma((3,)),
            dma((LOAD_STEPS,)),
            dma((7,)),
            dma((2, CHIPS)),
            dma((2, CHIPS)),
            dma((2, CHIPS)),
            dma((2, CHIPS)),
            dma((2, CHIPS)),
            dma((2, CHIPS)),
            dma((CHIPS, 2)),
            dma((2, CHIPS)),
        ],
        compiler_params=pltpu.CompilerParams(
            collective_id=0, has_side_effects=True, vmem_limit_bytes=VMEM_LIMIT
        ),
    )(
        captions.transpose(1, 0, 2),
        caption_layout,
        images,
        w_query,
        w_keyval,
        w_out,
        w_up,
        w_down,
        w_proj,
    )
    return pl.pallas_call(
        hand_out,
        out_shape=grads,
        in_specs=[vmem] * 2,
        out_specs=(vmem, vmem),
        compiler_params=pltpu.CompilerParams(vmem_limit_bytes=4 * 1024 * 1024),
    )(*made)


def solution(mesh):
    return jax.shard_map(
        body,
        mesh=mesh,
        in_specs=(P("dp", None, None), P(), P("dp", None), P(), P(), P(), P(), P(), P()),
        out_specs=(P("dp", None), P("dp", None)),
        check_vma=False,
    )
```

```python
import math

import jax
import jax.numpy as jnp
from jax import lax
from jax.experimental import pallas as pl
from jax.experimental.pallas import tpu as pltpu
from jax.sharding import PartitionSpec as P

HEADS = 12
HEAD_DIM = 64
WIDTH = 768
CTX = 77
CAPS = 32
FF = 3072
TILE = 16
GROUP = 8
GROUPS = CAPS // GROUP
SPLIT = HEADS * GROUP
PAIRS = (CTX + 1) // 2
TOKENS = PAIRS * 2 * GROUP
TOKENS_PAD = -(-TOKENS // 128) * 128
BLOCK = 256
BLOCK_HEADS = BLOCK // HEAD_DIM
BLOCKS = WIDTH // BLOCK
LOAD_STEPS = 6
STEP_T = 12
TAIL = CTX - LOAD_STEPS * STEP_T
CHIPS = 8
ARRIVAL = (7, 1, 6, 3, 2, 5, 4)
ROWS = CHIPS * 2 * CAPS
HALF = ROWS // 2
PIECE = 128
PIECES = ROWS // PIECE

VMEM_LIMIT = 60 * 1024 * 1024
LOGIT_SCALE = 100.0
EPS_NORM = 1e-05
EPS_UNIT = 1e-06
LOG2_E = math.log2(math.e)

MESH = pl.DeviceIdType.MESH
F32 = jnp.float32
BF16 = jnp.bfloat16


def norm_rows(values):
    center = values - jnp.mean(values, axis=-1, keepdims=True)
    spread = jnp.mean(center * center, axis=-1, keepdims=True)
    return center * lax.rsqrt(spread + EPS_NORM)


def unit_scale(values):
    return lax.rsqrt(jnp.sum(values * values, axis=-1, keepdims=True) + EPS_UNIT)


def unit_back(values, grad):
    scale = unit_scale(values)
    along = jnp.sum(values * grad, axis=-1, keepdims=True)
    return grad * scale - values * (along * (scale * scale * scale))


def dot(left, right):
    return jnp.dot(left, right, preferred_element_type=F32)


def dot_last(left, right):
    return lax.dot_general(left, right, (((1,), (1,)), ((), ())), preferred_element_type=F32)


def dot_first(left, right):
    return lax.dot_general(left, right, (((0,), (0,)), ((), ())), preferred_element_type=F32)


def iota(shape, dim):
    return lax.broadcasted_iota(jnp.int32, shape, dim)


class Place:
    def __init__(self):
        self.me = lax.axis_index("dp")
        self.core = self.me % 2
        self.at = {"y": (self.me // 2) % 4, "z": (self.me // 8) % 4, "x": self.me // 32}
        self.partner = self.me + 1 - 2 * self.core

    def flip(self, kind, value):
        image, text = 3 - value, value + 1 - 2 * (value % 2)
        return image + kind * (text - image)

    def bit(self, kind, value):
        return value // 2 + kind * (value % 2 - value // 2)

    def coords(self, kind, offset):
        return {
            axis: self.flip(kind, self.at[axis]) if offset >> step & 1 else self.at[axis]
            for step, axis in enumerate("yzx")
        }

    def peer(self, kind, offset, core):
        where = self.coords(kind, offset)
        return ((where["x"] * 4 + where["z"]) * 4 + where["y"]) * 2 + core

    def slot(self, kind, offset):
        where = self.coords(kind, offset)
        bits = {axis: self.bit(kind, where[axis]) for axis in "yzx"}
        return bits["x"] * 4 + bits["z"] * 2 + bits["y"]


def kernel(
    captions,
    layout,
    images,
    w_query,
    w_keyval,
    w_out,
    w_up,
    w_down,
    w_proj,
    image_grad,
    text_grad,
    tokens,
    normed,
    query_w,
    key_w,
    value_w,
    out_w,
    up_w,
    down_w,
    proj_w,
    counts,
    ends,
    image_rows,
    attn_scores,
    attn_bias,
    attn,
    units,
    row_exp,
    col_exp,
    row_peak,
    col_peak,
    logs,
    weight,
    blocks,
    parts,
    small_sem,
    load_sem,
    weight_sem,
    gather_send,
    gather_recv,
    pass_send,
    pass_recv,
    log_send,
    log_recv,
    part_send,
    part_recv,
):
    place = Place()
    me, core, partner = place.me, place.core, place.partner

    def load(step, size=STEP_T):
        span = pl.ds(step * STEP_T, size)
        return pltpu.make_async_copy(captions.at[span], tokens.at[span], load_sem.at[step])

    span = pl.ds(pl.multiple_of(me // 4 * 128, 128), 128)
    load_counts = pltpu.make_async_copy(layout.at[:, span], counts, small_sem.at[0])
    load_images = pltpu.make_async_copy(images, image_rows, small_sem.at[1])
    load_ends = pltpu.make_async_copy(layout.at[:, span], ends, small_sem.at[2])
    weights = {}
    for number, (name, source, target) in enumerate(
        (
            ("query", w_query, query_w),
            ("key", w_keyval.at[:, :WIDTH], key_w),
            ("value", w_keyval.at[:, WIDTH:], value_w),
            ("out", w_out, out_w),
            ("up", w_up, up_w),
            ("down", w_down, down_w),
            ("proj", w_proj, proj_w),
        )
    ):
        weights[name] = pltpu.make_async_copy(source, target, weight_sem.at[number])
    for step in range(LOAD_STEPS):
        load(step).start()
    load_tail = load(LOAD_STEPS, TAIL)
    load_tail.start()
    for copy in (load_counts, load_ends, load_images):
        copy.start()
    for copy in weights.values():
        copy.start(priority=1)

    barrier = pltpu.get_barrier_semaphore()
    friends = [partner]
    for offset in range(1, CHIPS):
        for kind in range(2):
            friends += [place.peer(kind, offset, 0), place.peer(kind, offset, 1)]
    for friend in friends:
        pl.semaphore_signal(barrier, inc=1, device_id=(friend,), device_id_type=MESH)

    normed[:, TOKENS:, :] = jnp.zeros((GROUPS, TOKENS_PAD - TOKENS, WIDTH), BF16)
    tokens[CTX] = jnp.zeros((CAPS, WIDTH), BF16)


    def norm_pair(pair):
        at = pair * TILE if isinstance(pair, int) else pl.multiple_of(pair * TILE, TILE)
        for tile in range(0, CAPS, TILE):
            halves = [
                norm_rows(tokens[2 * pair + side, tile : tile + TILE, :].astype(F32))
                for side in range(2)
            ]
            for first in range(0, TILE, GROUP):
                rows = jnp.concatenate([half[first : first + GROUP] for half in halves], axis=0)
                normed[(tile + first) // GROUP, pl.ds(at, TILE), :] = rows.astype(BF16)

    def norm_step(step, _):
        load(step).wait()
        for inner in range(STEP_T // 2):
            norm_pair(step * (STEP_T // 2) + inner)
        return 0

    lax.fori_loop(0, LOAD_STEPS, norm_step, 0)
    load_tail.wait()
    for pair in range(LOAD_STEPS * STEP_T // 2, PAIRS):
        norm_pair(pair)

    load_ends.wait()
    load_counts.wait()
    weights["query"].wait()
    weights["key"].wait()
    end_values = []
    for first in range(0, CAPS, TILE):
        rows = jnp.zeros((TILE, WIDTH), BF16)
        for inner in range(TILE):
            last = jnp.clip(ends[0, me % 4 * CAPS + first + inner] - 1, 0, CTX - 1)
            found = tokens[last, first : first + TILE, :]
            rows = jnp.where(iota((TILE, WIDTH), 0) == inner, found, rows)
        end_values.append(rows)
    end_values = jnp.concatenate(end_values, axis=0).astype(F32)
    end_normed = norm_rows(end_values).astype(BF16)
    head_of = iota((GROUP, BLOCK), 1) // HEAD_DIM
    groups = [slice(group * GROUP, (group + 1) * GROUP) for group in range(GROUPS)]
    spans = [slice(at, at + BLOCK) for at in range(0, WIDTH, BLOCK)]
    key_query = []
    for span in spans:
        query = dot(end_normed, query_w[:, span]).astype(BF16).astype(F32)
        query = query * (1.0 / math.sqrt(HEAD_DIM))
        spread = [
            jnp.where(head_of == head, query[rows], 0.0)
            for rows in groups
            for head in range(BLOCK_HEADS)
        ]
        spread = jnp.concatenate(spread, axis=0).astype(BF16)
        key_query.append((dot_last(spread, key_w[:, span]) * LOG2_E).astype(BF16))

    picked = iota((CAPS, 128), 1) == iota((CAPS, 128), 0) + me % 4 * CAPS
    lengths = jnp.sum(jnp.where(picked, counts[0:1, :].astype(F32), 0.0), axis=1, keepdims=True)
    lengths = jnp.maximum(lengths, 1.0)

    token = iota((2 * GROUP, TOKENS_PAD), 1)
    own = token % GROUP == iota((2 * GROUP, TOKENS_PAD), 0) % GROUP
    for group in range(GROUPS):
        count = lengths[group * GROUP : (group + 1) * GROUP]
        count = jnp.concatenate([count, count], axis=0)
        inside = own & ((token // GROUP).astype(F32) < count)
        attn_bias[group] = jnp.where(inside, 0.0, -jnp.inf)

    part = BLOCK_HEADS * GROUP
    contexts = []
    for group in range(GROUPS):
        rows = slice(group * part, (group + 1) * part)
        asked = jnp.concatenate([block[rows] for block in key_query], axis=0)
        attn_scores[group] = dot_last(asked, normed[group])
    for group in range(GROUPS):
        totals = []
        for head in range(0, HEADS, 2):
            rows = slice(head * GROUP, (head + 2) * GROUP)
            value = attn_scores[group, rows, :] + attn_bias[group]
            value = jnp.exp2(value - jnp.max(value, axis=1, keepdims=True))
            attn[group, rows, :] = value.astype(BF16)
            totals.append(jnp.sum(value, axis=1, keepdims=True))
        context = dot(attn[group], normed[group]) / jnp.concatenate(totals, axis=0)
        contexts.append(context.astype(BF16))

    load_images.wait()
    image_values = image_rows[...].astype(F32)
    image_unit = (image_values * unit_scale(image_values)).astype(BF16)
    slots = (place.slot(0, 0), place.slot(1, 0))
    units[0, 0, slots[0]] = image_unit

    pl.semaphore_wait(barrier, len(friends))

    def send_units(kind):
        copies = {}
        for offset in range(CHIPS - 1, 0, -1):
            copies[offset] = pltpu.make_async_remote_copy(
                src_ref=units.at[kind, 0, slots[kind]],
                dst_ref=units.at[kind, 0, slots[kind]],
                send_sem=gather_send.at[kind, offset],
                recv_sem=gather_recv.at[kind, offset],
                device_id=(place.peer(kind, offset, core),),
                device_id_type=MESH,
            )
            copies[offset].start()
        return copies

    def hand_on(kind, offset):
        slot = place.slot(kind, offset)
        copy = pltpu.make_async_remote_copy(
            src_ref=units.at[kind, 0, slot],
            dst_ref=units.at[kind, 1, slot],
            send_sem=pass_send.at[kind, offset],
            recv_sem=pass_recv.at[kind, offset],
            device_id=(partner,),
            device_id_type=MESH,
        )
        copy.start()
        return copy

    image_sends = send_units(0)
    passed = {(0, 0): hand_on(0, 0)}

    for name in ("value", "out", "up", "down", "proj"):
        weights[name].wait()
    mixed = []
    for number, span in enumerate(spans):
        rows = slice(number * part, (number + 1) * part)
        by_head = jnp.concatenate([context[rows] for context in contexts], axis=0)
        by_head = dot(by_head, value_w[:, span])
        sums = []
        for group in range(GROUPS):
            total = jnp.zeros((GROUP, BLOCK), F32)
            for head in range(BLOCK_HEADS):
                first = group * part + head * GROUP
                total = total + jnp.where(head_of == head, by_head[first : first + GROUP], 0.0)
            sums.append(total)
        mixed.append(jnp.concatenate(sums, axis=0))
    mixed = jnp.concatenate(mixed, axis=1).astype(BF16)

    residual = (end_values + dot(mixed, out_w[...])).astype(BF16)
    residual = residual.astype(F32)
    inner = norm_rows(residual).astype(BF16)
    final = residual
    for part in range(FF // WIDTH):
        span = slice(part * WIDTH, (part + 1) * WIDTH)
        hidden = dot(inner, up_w[:, span])
        hidden = 0.5 * hidden * (1.0 + lax.erf(hidden * (1.0 / math.sqrt(2.0))))
        final = final + dot(hidden.astype(BF16), down_w[span, :])
    pooled = norm_rows(final).astype(BF16)
    text_values = dot(pooled, proj_w[...]).astype(BF16).astype(F32)
    text_unit = (text_values * unit_scale(text_values)).astype(BF16)
    units[1, 0, slots[1]] = text_unit

    text_sends = send_units(1)
    passed[1, 0] = hand_on(1, 0)

    for offset in range(1, CHIPS):
        image_sends[offset].wait_recv()
        passed[0, offset] = hand_on(0, offset)

    for offset in ARRIVAL:
        text_sends[offset].wait_recv()
        passed[1, offset] = hand_on(1, offset)
    for offset in range(CHIPS):
        passed[0, offset].wait_recv()

    eye = iota((PIECE, PIECE), 0) == iota((PIECE, PIECE), 1)
    col_sums, col_peaks = [], []
    for half in range(2):
        if half == 1:
            for offset in range(CHIPS):
                passed[1, offset].wait_recv()
        scores = dot_last(units[1, half].reshape(HALF, WIDTH), units[0].reshape(ROWS, WIDTH))
        scores = scores * (LOGIT_SCALE * LOG2_E)
        peak = jnp.max(scores, axis=1, keepdims=True)
        value = jnp.exp2(scores - peak)
        row_exp[half] = value
        row_peak[half] = peak
        log = peak + jnp.log(jnp.sum(value, axis=1, keepdims=True)) * LOG2_E
        for piece in range(HALF // PIECE):
            part = log[piece * PIECE : (piece + 1) * PIECE]
            part = jnp.sum(jnp.where(eye, part, 0.0), axis=0, keepdims=True)
            logs[1, 0, half * (HALF // PIECE) + piece] = part
        peak = jnp.max(scores, axis=0, keepdims=True)
        value = jnp.exp2(scores - peak)
        col_exp[half] = value
        col_peak[half] = peak
        col_peaks.append(peak)
        col_sums.append(jnp.sum(value, axis=0, keepdims=True))
    top = jnp.maximum(*col_peaks)
    total = sum(part * jnp.exp2(peak - top) for part, peak in zip(col_sums, col_peaks))
    log = top + jnp.log(total) * LOG2_E
    for piece in range(PIECES):
        logs[0, 0, piece] = log[:, piece * PIECE : (piece + 1) * PIECE]

    log_sends = []
    for offset in range(CHIPS - 1, 0, -1):
        for kind in range(2):
            copy = pltpu.make_async_remote_copy(
                src_ref=logs.at[kind, 0],
                dst_ref=logs.at[kind, offset],
                send_sem=log_send.at[kind, offset],
                recv_sem=log_recv.at[kind, offset],
                device_id=(place.peer(kind, offset, core),),
                device_id_type=MESH,
            )
            copy.start()
            log_sends.append(copy)
    for copy in log_sends:
        copy.wait_recv()

    def whole_log(kind):
        top = logs[kind, 0]
        for offset in range(1, CHIPS):
            top = jnp.maximum(top, logs[kind, offset])
        total = jnp.zeros_like(top)
        for offset in range(CHIPS):
            total = total + jnp.exp2(logs[kind, offset] - top)
        return top + jnp.log(total) * LOG2_E

    image_logs, text_logs = whole_log(0), whole_log(1)
    image_logs = jnp.concatenate([image_logs[piece] for piece in range(PIECES)], axis=1)
    for half in range(2):
        col_scale = jnp.exp2(col_peak[half] - image_logs)
        for piece in range(HALF // PIECE):
            rows = slice(piece * PIECE, (piece + 1) * PIECE)
            first = half * HALF + piece * PIECE
            log = text_logs[half * (HALF // PIECE) + piece]
            log = jnp.sum(jnp.where(eye, log, 0.0), axis=1, keepdims=True)
            row_scale = jnp.exp2(row_peak[half, rows] - log)
            both = row_exp[half, rows] * row_scale + col_exp[half, rows] * col_scale
            weight[first : first + PIECE, :] = both.astype(BF16)

    duty = 1 - core
    part_sends = []
    for far in (1, 0):
        first = place.slot(duty, 4 * far) // 4 * 4
        spans = [
            pl.ds(pl.multiple_of(side * HALF + first * CAPS, PIECE), PIECE) for side in range(2)
        ]

        def keep(grad):
            blocks[:, pl.ds(first, 4)] = grad.astype(BF16).reshape(2, 4, CAPS, WIDTH)

        @pl.when(duty == 0)
        def _():
            columns = jnp.concatenate([weight[:, span] for span in spans], axis=1)
            keep(dot_first(columns, units[1].reshape(ROWS, WIDTH)))

        @pl.when(duty == 1)
        def _():
            rows = jnp.concatenate([weight[span, :] for span in spans], axis=0)
            keep(dot(rows, units[0].reshape(ROWS, WIDTH)))

        for offset in range(4 * far + 3, 4 * far - 1, -1):
            slot = place.slot(duty, offset)
            for side in range(2):
                if offset == 0 and side == 0:
                    parts[duty, 0] = blocks[0, slot]
                    continue
                copy = pltpu.make_async_remote_copy(
                    src_ref=blocks.at[side, slot],
                    dst_ref=parts.at[duty, offset],
                    send_sem=part_send.at[offset, side],
                    recv_sem=part_recv.at[duty, offset],
                    device_id=(place.peer(duty, offset, core + side - 2 * side * core),),
                    device_id_type=MESH,
                )
                copy.start()
                part_sends.append(copy)

    def arrived(kind, offset):
        pltpu.make_async_remote_copy(
            src_ref=parts.at[kind, offset],
            dst_ref=parts.at[kind, offset],
            send_sem=part_send.at[0, 0],
            recv_sem=part_recv.at[kind, offset],
            device_id=(partner,),
            device_id_type=MESH,
        ).wait_recv()

    arrived(core, 0)
    for offset in range(1, CHIPS):
        for kind in range(2):
            arrived(kind, offset)

    half = 0.5 * LOGIT_SCALE
    sums = []
    for kind in range(2):
        total = parts[kind, 0].astype(F32)
        for offset in range(1, CHIPS):
            total = total + parts[kind, offset].astype(F32)
        sums.append(total)
    image_unit_grad = half * sums[0] - LOGIT_SCALE * text_unit.astype(F32)
    text_unit_grad = half * sums[1] - LOGIT_SCALE * image_unit.astype(F32)
    image_grad[...] = unit_back(image_values, image_unit_grad)
    text_grad[...] = unit_back(text_values, text_unit_grad)

    for copy in [*image_sends.values(), *text_sends.values(), *passed.values()]:
        copy.wait_send()
    for copy in log_sends + part_sends:
        copy.wait_send()


def hand_out(image_from, text_from, image_to, text_to):
    image_to[...] = image_from[...]
    text_to[...] = text_from[...]


def body(captions, caption_layout, images, w_query, w_keyval, w_out, w_up, w_down, w_proj):
    hbm = pl.BlockSpec(memory_space=pl.ANY)
    vmem = pl.BlockSpec(memory_space=pltpu.VMEM)
    dma = pltpu.SemaphoreType.DMA
    grads = (jax.ShapeDtypeStruct((CAPS, WIDTH), F32),) * 2
    made = pl.pallas_call(
        kernel,
        out_shape=(pltpu.VMEM((CAPS, WIDTH), F32),) * 2,
        in_specs=[hbm] * 9,
        out_specs=(vmem, vmem),
        scratch_shapes=[
            pltpu.VMEM((CTX + 1, CAPS, WIDTH), BF16),
            pltpu.VMEM((GROUPS, TOKENS_PAD, WIDTH), BF16),
            pltpu.VMEM((WIDTH, WIDTH), BF16),
            pltpu.VMEM((WIDTH, WIDTH), BF16),
            pltpu.VMEM((WIDTH, WIDTH), BF16),
            pltpu.VMEM((WIDTH, WIDTH), BF16),
            pltpu.VMEM((WIDTH, FF), BF16),
            pltpu.VMEM((FF, WIDTH), BF16),
            pltpu.VMEM((WIDTH, WIDTH), BF16),
            pltpu.VMEM((2, 128), jnp.int32),
            pltpu.SMEM((2, 128), jnp.int32),
            pltpu.VMEM((CAPS, WIDTH), BF16),
            pltpu.VMEM((GROUPS, SPLIT, TOKENS_PAD), F32),
            pltpu.VMEM((GROUPS, 2 * GROUP, TOKENS_PAD), F32),
            pltpu.VMEM((GROUPS, SPLIT, TOKENS_PAD), BF16),
            pltpu.VMEM((2, 2, CHIPS, CAPS, WIDTH), BF16),
            pltpu.VMEM((2, HALF, ROWS), F32),
            pltpu.VMEM((2, HALF, ROWS), F32),
            pltpu.VMEM((2, HALF, 1), F32),
            pltpu.VMEM((2, 1, ROWS), F32),
            pltpu.VMEM((2, CHIPS, PIECES, 1, PIECE), F32),
            pltpu.VMEM((ROWS, ROWS), BF16),
            pltpu.VMEM((2, CHIPS, CAPS, WIDTH), BF16),
            pltpu.VMEM((2, CHIPS, CAPS, WIDTH), BF16),
            dma((3,)),
            dma((LOAD_STEPS + 1,)),
            dma((7,)),
            dma((2, CHIPS)),
            dma((2, CHIPS)),
            dma((2, CHIPS)),
            dma((2, CHIPS)),
            dma((2, CHIPS)),
            dma((2, CHIPS)),
            dma((CHIPS, 2)),
            dma((2, CHIPS)),
        ],
        compiler_params=pltpu.CompilerParams(
            collective_id=0, has_side_effects=True, vmem_limit_bytes=VMEM_LIMIT
        ),
    )(
        captions.transpose(1, 0, 2),
        caption_layout,
        images,
        w_query,
        w_keyval,
        w_out,
        w_up,
        w_down,
        w_proj,
    )
    return pl.pallas_call(
        hand_out,
        out_shape=grads,
        in_specs=[vmem] * 2,
        out_specs=(vmem, vmem),
        compiler_params=pltpu.CompilerParams(vmem_limit_bytes=4 * 1024 * 1024),
    )(*made)


def solution(mesh):
    return jax.shard_map(
        body,
        mesh=mesh,
        in_specs=(P("dp", None, None), P(), P("dp", None), P(), P(), P(), P(), P(), P()),
        out_specs=(P("dp", None), P("dp", None)),
        check_vma=False,
    )
```

```python
import math

import jax
import jax.numpy as jnp
from jax import lax
from jax.experimental import pallas as pl
from jax.experimental.pallas import tpu as pltpu
from jax.sharding import PartitionSpec as P

HEADS = 12
HEAD_DIM = 64
WIDTH = 768
CTX = 77
CAPS = 32
FF = 3072
TILE = 16
GROUP = 8
GROUPS = CAPS // GROUP
SPLIT = HEADS * GROUP
PAIRS = (CTX + 1) // 2
TOKENS = PAIRS * 2 * GROUP
TOKENS_PAD = -(-TOKENS // 128) * 128
BLOCK = 256
BLOCK_HEADS = BLOCK // HEAD_DIM
BLOCKS = WIDTH // BLOCK
LOAD_STEPS = 6
STEP_T = 12
TAIL = CTX - LOAD_STEPS * STEP_T
CHIPS = 8
ARRIVAL = (7, 1, 6, 3, 2, 5, 4)
ROWS = CHIPS * 2 * CAPS
HALF = ROWS // 2
PIECE = 128
PIECES = ROWS // PIECE

VMEM_LIMIT = 60 * 1024 * 1024
LOGIT_SCALE = 100.0
EPS_NORM = 1e-05
EPS_UNIT = 1e-06
LOG2_E = math.log2(math.e)

MESH = pl.DeviceIdType.MESH
F32 = jnp.float32
BF16 = jnp.bfloat16


def norm_rows(values):
    center = values - jnp.mean(values, axis=-1, keepdims=True)
    spread = jnp.mean(center * center, axis=-1, keepdims=True)
    return center * lax.rsqrt(spread + EPS_NORM)


def unit_scale(values):
    return lax.rsqrt(jnp.sum(values * values, axis=-1, keepdims=True) + EPS_UNIT)


def unit_back(values, grad):
    scale = unit_scale(values)
    along = jnp.sum(values * grad, axis=-1, keepdims=True)
    return grad * scale - values * (along * (scale * scale * scale))


def dot(left, right):
    return jnp.dot(left, right, preferred_element_type=F32)


def dot_last(left, right):
    return lax.dot_general(left, right, (((1,), (1,)), ((), ())), preferred_element_type=F32)


def dot_first(left, right):
    return lax.dot_general(left, right, (((0,), (0,)), ((), ())), preferred_element_type=F32)


def iota(shape, dim):
    return lax.broadcasted_iota(jnp.int32, shape, dim)


class Place:
    def __init__(self):
        self.me = lax.axis_index("dp")
        self.core = self.me % 2
        self.at = {"y": (self.me // 2) % 4, "z": (self.me // 8) % 4, "x": self.me // 32}
        self.partner = self.me + 1 - 2 * self.core

    def flip(self, kind, value):
        image, text = 3 - value, value + 1 - 2 * (value % 2)
        return image + kind * (text - image)

    def bit(self, kind, value):
        return value // 2 + kind * (value % 2 - value // 2)

    def coords(self, kind, offset):
        return {
            axis: self.flip(kind, self.at[axis]) if offset >> step & 1 else self.at[axis]
            for step, axis in enumerate("yzx")
        }

    def peer(self, kind, offset, core):
        where = self.coords(kind, offset)
        return ((where["x"] * 4 + where["z"]) * 4 + where["y"]) * 2 + core

    def slot(self, kind, offset):
        where = self.coords(kind, offset)
        bits = {axis: self.bit(kind, where[axis]) for axis in "yzx"}
        return bits["x"] * 4 + bits["z"] * 2 + bits["y"]


def kernel(
    captions,
    layout,
    images,
    w_query,
    w_keyval,
    w_out,
    w_up,
    w_down,
    w_proj,
    image_grad,
    text_grad,
    tokens,
    normed,
    query_w,
    key_w,
    value_w,
    out_w,
    up_w,
    down_w,
    proj_w,
    counts,
    ends,
    image_rows,
    attn_scores,
    attn_bias,
    attn,
    units,
    row_exp,
    col_exp,
    row_peak,
    col_peak,
    image_logs,
    text_logs,
    weight,
    blocks,
    parts,
    small_sem,
    load_sem,
    weight_sem,
    gather_send,
    gather_recv,
    pass_send,
    pass_recv,
    log_send,
    log_recv,
    part_send,
    part_recv,
):
    place = Place()
    me, core, partner = place.me, place.core, place.partner

    def load(step, size=STEP_T):
        span = pl.ds(step * STEP_T, size)
        return pltpu.make_async_copy(captions.at[span], tokens.at[span], load_sem.at[step])

    span = pl.ds(pl.multiple_of(me // 4 * 128, 128), 128)
    load_counts = pltpu.make_async_copy(layout.at[:, span], counts, small_sem.at[0])
    load_images = pltpu.make_async_copy(images, image_rows, small_sem.at[1])
    load_ends = pltpu.make_async_copy(layout.at[:, span], ends, small_sem.at[2])
    weights = {}
    for number, (name, source, target) in enumerate(
        (
            ("query", w_query, query_w),
            ("key", w_keyval.at[:, :WIDTH], key_w),
            ("value", w_keyval.at[:, WIDTH:], value_w),
            ("out", w_out, out_w),
            ("up", w_up, up_w),
            ("down", w_down, down_w),
            ("proj", w_proj, proj_w),
        )
    ):
        weights[name] = pltpu.make_async_copy(source, target, weight_sem.at[number])
    for step in range(LOAD_STEPS):
        load(step).start()
    load_tail = load(LOAD_STEPS, TAIL)
    load_tail.start()
    for copy in (load_counts, load_ends, load_images):
        copy.start()
    for copy in weights.values():
        copy.start(priority=1)

    barrier = pltpu.get_barrier_semaphore()
    friends = [partner]
    for offset in range(1, CHIPS):
        for kind in range(2):
            friends += [place.peer(kind, offset, 0), place.peer(kind, offset, 1)]
    for friend in friends:
        pl.semaphore_signal(barrier, inc=1, device_id=(friend,), device_id_type=MESH)

    normed[:, TOKENS:, :] = jnp.zeros((GROUPS, TOKENS_PAD - TOKENS, WIDTH), BF16)
    tokens[CTX] = jnp.zeros((CAPS, WIDTH), BF16)


    def norm_pair(pair):
        at = pair * TILE if isinstance(pair, int) else pl.multiple_of(pair * TILE, TILE)
        for tile in range(0, CAPS, TILE):
            halves = [
                norm_rows(tokens[2 * pair + side, tile : tile + TILE, :].astype(F32))
                for side in range(2)
            ]
            for first in range(0, TILE, GROUP):
                rows = jnp.concatenate([half[first : first + GROUP] for half in halves], axis=0)
                normed[(tile + first) // GROUP, pl.ds(at, TILE), :] = rows.astype(BF16)

    def norm_step(step, _):
        load(step).wait()
        for inner in range(STEP_T // 2):
            norm_pair(step * (STEP_T // 2) + inner)
        return 0

    lax.fori_loop(0, LOAD_STEPS, norm_step, 0)
    load_tail.wait()
    for pair in range(LOAD_STEPS * STEP_T // 2, PAIRS):
        norm_pair(pair)

    load_ends.wait()
    load_counts.wait()
    weights["query"].wait()
    weights["key"].wait()
    end_values = []
    for first in range(0, CAPS, TILE):
        rows = jnp.zeros((TILE, WIDTH), BF16)
        for inner in range(TILE):
            last = jnp.clip(ends[0, me % 4 * CAPS + first + inner] - 1, 0, CTX - 1)
            found = tokens[last, first : first + TILE, :]
            rows = jnp.where(iota((TILE, WIDTH), 0) == inner, found, rows)
        end_values.append(rows)
    end_values = jnp.concatenate(end_values, axis=0).astype(F32)
    end_normed = norm_rows(end_values).astype(BF16)
    head_of = iota((GROUP, BLOCK), 1) // HEAD_DIM
    groups = [slice(group * GROUP, (group + 1) * GROUP) for group in range(GROUPS)]
    spans = [slice(at, at + BLOCK) for at in range(0, WIDTH, BLOCK)]
    key_query = []
    for span in spans:
        query = dot(end_normed, query_w[:, span]).astype(BF16).astype(F32)
        query = query * (1.0 / math.sqrt(HEAD_DIM))
        spread = [
            jnp.where(head_of == head, query[rows], 0.0)
            for rows in groups
            for head in range(BLOCK_HEADS)
        ]
        spread = jnp.concatenate(spread, axis=0).astype(BF16)
        key_query.append((dot_last(spread, key_w[:, span]) * LOG2_E).astype(BF16))

    picked = iota((CAPS, 128), 1) == iota((CAPS, 128), 0) + me % 4 * CAPS
    lengths = jnp.sum(jnp.where(picked, counts[0:1, :].astype(F32), 0.0), axis=1, keepdims=True)
    lengths = jnp.maximum(lengths, 1.0)

    token = iota((2 * GROUP, TOKENS_PAD), 1)
    own = token % GROUP == iota((2 * GROUP, TOKENS_PAD), 0) % GROUP
    for group in range(GROUPS):
        count = lengths[group * GROUP : (group + 1) * GROUP]
        count = jnp.concatenate([count, count], axis=0)
        inside = own & ((token // GROUP).astype(F32) < count)
        attn_bias[group] = jnp.where(inside, 0.0, -jnp.inf)

    part = BLOCK_HEADS * GROUP
    contexts = []
    for group in range(GROUPS):
        rows = slice(group * part, (group + 1) * part)
        asked = jnp.concatenate([block[rows] for block in key_query], axis=0)
        attn_scores[group] = dot_last(asked, normed[group])
    for group in range(GROUPS):
        totals = []
        for head in range(0, HEADS, 2):
            rows = slice(head * GROUP, (head + 2) * GROUP)
            value = attn_scores[group, rows, :] + attn_bias[group]
            value = jnp.exp2(value - jnp.max(value, axis=1, keepdims=True))
            attn[group, rows, :] = value.astype(BF16)
            totals.append(jnp.sum(value, axis=1, keepdims=True))
        context = dot(attn[group], normed[group]) / jnp.concatenate(totals, axis=0)
        contexts.append(context.astype(BF16))

    load_images.wait()
    image_values = image_rows[...].astype(F32)
    image_unit = (image_values * unit_scale(image_values)).astype(BF16)
    slots = (place.slot(0, 0), place.slot(1, 0))
    units[0, 0, slots[0]] = image_unit

    pl.semaphore_wait(barrier, len(friends))

    def send_units(kind):
        copies = {}
        for offset in range(CHIPS - 1, 0, -1):
            copies[offset] = pltpu.make_async_remote_copy(
                src_ref=units.at[kind, 0, slots[kind]],
                dst_ref=units.at[kind, 0, slots[kind]],
                send_sem=gather_send.at[kind, offset],
                recv_sem=gather_recv.at[kind, offset],
                device_id=(place.peer(kind, offset, core),),
                device_id_type=MESH,
            )
            copies[offset].start()
        return copies

    def hand_on(kind, offset):
        slot = place.slot(kind, offset)
        copy = pltpu.make_async_remote_copy(
            src_ref=units.at[kind, 0, slot],
            dst_ref=units.at[kind, 1, slot],
            send_sem=pass_send.at[kind, offset],
            recv_sem=pass_recv.at[kind, offset],
            device_id=(partner,),
            device_id_type=MESH,
        )
        copy.start()
        return copy

    image_sends = send_units(0)
    passed = {(0, 0): hand_on(0, 0)}

    for name in ("value", "out", "up", "down", "proj"):
        weights[name].wait()
    mixed = []
    for number, span in enumerate(spans):
        rows = slice(number * part, (number + 1) * part)
        by_head = jnp.concatenate([context[rows] for context in contexts], axis=0)
        by_head = dot(by_head, value_w[:, span])
        sums = []
        for group in range(GROUPS):
            total = jnp.zeros((GROUP, BLOCK), F32)
            for head in range(BLOCK_HEADS):
                first = group * part + head * GROUP
                total = total + jnp.where(head_of == head, by_head[first : first + GROUP], 0.0)
            sums.append(total)
        mixed.append(jnp.concatenate(sums, axis=0))
    mixed = jnp.concatenate(mixed, axis=1).astype(BF16)

    residual = (end_values + dot(mixed, out_w[...])).astype(BF16)
    residual = residual.astype(F32)
    inner = norm_rows(residual).astype(BF16)
    final = residual
    for part in range(FF // WIDTH):
        span = slice(part * WIDTH, (part + 1) * WIDTH)
        hidden = dot(inner, up_w[:, span])
        hidden = 0.5 * hidden * (1.0 + lax.erf(hidden * (1.0 / math.sqrt(2.0))))
        final = final + dot(hidden.astype(BF16), down_w[span, :])
    pooled = norm_rows(final).astype(BF16)
    text_values = dot(pooled, proj_w[...]).astype(BF16).astype(F32)
    text_unit = (text_values * unit_scale(text_values)).astype(BF16)
    units[1, 0, slots[1]] = text_unit

    text_sends = send_units(1)
    passed[1, 0] = hand_on(1, 0)

    for offset in range(1, CHIPS):
        image_sends[offset].wait_recv()
        passed[0, offset] = hand_on(0, offset)

    for offset in ARRIVAL:
        text_sends[offset].wait_recv()
        passed[1, offset] = hand_on(1, offset)
    for offset in range(CHIPS):
        passed[0, offset].wait_recv()

    eye = iota((PIECE, PIECE), 0) == iota((PIECE, PIECE), 1)
    half_pieces = HALF // PIECE

    def score(half):
        scores = dot_last(units[1, half].reshape(HALF, WIDTH), units[0].reshape(ROWS, WIDTH))
        scores = scores * (LOGIT_SCALE * LOG2_E)
        for axis, exp, top in ((1, row_exp, row_peak), (0, col_exp, col_peak)):
            peak = jnp.max(scores, axis=axis, keepdims=True)
            value = jnp.exp2(scores - peak)
            exp[half] = value
            top[half] = peak
            if half == 0:
                yield peak + jnp.log(jnp.sum(value, axis=axis, keepdims=True)) * LOG2_E

    row_log, col_log = score(0)
    for piece in range(half_pieces):
        part = row_log[piece * PIECE : (piece + 1) * PIECE]
        part = jnp.sum(jnp.where(eye, part, 0.0), axis=0, keepdims=True)
        text_logs[0, 0, piece] = part
    for piece in range(PIECES):
        image_logs[0, 0, piece] = col_log[:, piece * PIECE : (piece + 1) * PIECE]

    log_sends = []
    for offset in range(CHIPS - 1, -1, -1):
        for kind, logs in enumerate((image_logs, text_logs)):
            for side in range(2):
                if offset == 0 and side == 0:
                    continue
                copy = pltpu.make_async_remote_copy(
                    src_ref=logs.at[0, 0],
                    dst_ref=logs.at[side, offset],
                    send_sem=log_send.at[kind, side, offset],
                    recv_sem=log_recv.at[kind, side, offset],
                    device_id=(place.peer(kind, offset, core + side - 2 * side * core),),
                    device_id_type=MESH,
                )
                copy.start()
                log_sends.append(copy)

    for offset in range(CHIPS):
        passed[1, offset].wait_recv()
    for _ in score(1):
        pass

    for copy in log_sends:
        copy.wait_recv()

    def whole_log(terms):
        top = terms[0]
        for term in terms[1:]:
            top = jnp.maximum(top, term)
        total = sum(jnp.exp2(term - top) for term in terms)
        return top + jnp.log(total) * LOG2_E

    terms = [image_logs[0, offset] for offset in range(CHIPS)]
    for offset in range(CHIPS):
        term = image_logs[1, offset]
        terms.append(jnp.concatenate([term[half_pieces:], term[:half_pieces]], axis=0))
    image_log = whole_log(terms)
    image_log = jnp.concatenate([image_log[piece] for piece in range(PIECES)], axis=1)
    for half in range(2):
        text_log = whole_log([text_logs[half, offset] for offset in range(CHIPS)])
        col_scale = jnp.exp2(col_peak[half] - image_log)
        for piece in range(half_pieces):
            rows = slice(piece * PIECE, (piece + 1) * PIECE)
            first = half * HALF + piece * PIECE
            log = jnp.sum(jnp.where(eye, text_log[piece], 0.0), axis=1, keepdims=True)
            row_scale = jnp.exp2(row_peak[half, rows] - log)
            both = row_exp[half, rows] * row_scale + col_exp[half, rows] * col_scale
            weight[first : first + PIECE, :] = both.astype(BF16)

    duty = 1 - core
    part_sends = []
    for far in (1, 0):
        first = place.slot(duty, 4 * far) // 4 * 4
        spans = [
            pl.ds(pl.multiple_of(side * HALF + first * CAPS, PIECE), PIECE) for side in range(2)
        ]

        def keep(grad):
            blocks[:, pl.ds(first, 4)] = grad.astype(BF16).reshape(2, 4, CAPS, WIDTH)

        @pl.when(duty == 0)
        def _():
            columns = jnp.concatenate([weight[:, span] for span in spans], axis=1)
            keep(dot_first(columns, units[1].reshape(ROWS, WIDTH)))

        @pl.when(duty == 1)
        def _():
            rows = jnp.concatenate([weight[span, :] for span in spans], axis=0)
            keep(dot(rows, units[0].reshape(ROWS, WIDTH)))

        for offset in range(4 * far + 3, 4 * far - 1, -1):
            slot = place.slot(duty, offset)
            for side in range(2):
                if offset == 0 and side == 0:
                    parts[duty, 0] = blocks[0, slot]
                    continue
                copy = pltpu.make_async_remote_copy(
                    src_ref=blocks.at[side, slot],
                    dst_ref=parts.at[duty, offset],
                    send_sem=part_send.at[offset, side],
                    recv_sem=part_recv.at[duty, offset],
                    device_id=(place.peer(duty, offset, core + side - 2 * side * core),),
                    device_id_type=MESH,
                )
                copy.start()
                part_sends.append(copy)

    def arrived(kind, offset):
        pltpu.make_async_remote_copy(
            src_ref=parts.at[kind, offset],
            dst_ref=parts.at[kind, offset],
            send_sem=part_send.at[0, 0],
            recv_sem=part_recv.at[kind, offset],
            device_id=(partner,),
            device_id_type=MESH,
        ).wait_recv()

    arrived(core, 0)
    for offset in range(1, CHIPS):
        for kind in range(2):
            arrived(kind, offset)

    half = 0.5 * LOGIT_SCALE
    sums = []
    for kind in range(2):
        total = parts[kind, 0].astype(F32)
        for offset in range(1, CHIPS):
            total = total + parts[kind, offset].astype(F32)
        sums.append(total)
    image_unit_grad = half * sums[0] - LOGIT_SCALE * text_unit.astype(F32)
    text_unit_grad = half * sums[1] - LOGIT_SCALE * image_unit.astype(F32)
    image_grad[...] = unit_back(image_values, image_unit_grad)
    text_grad[...] = unit_back(text_values, text_unit_grad)

    for copy in [*image_sends.values(), *text_sends.values(), *passed.values()]:
        copy.wait_send()
    for copy in log_sends + part_sends:
        copy.wait_send()


def hand_out(image_from, text_from, image_to, text_to):
    image_to[...] = image_from[...]
    text_to[...] = text_from[...]


def body(captions, caption_layout, images, w_query, w_keyval, w_out, w_up, w_down, w_proj):
    hbm = pl.BlockSpec(memory_space=pl.ANY)
    vmem = pl.BlockSpec(memory_space=pltpu.VMEM)
    dma = pltpu.SemaphoreType.DMA
    grads = (jax.ShapeDtypeStruct((CAPS, WIDTH), F32),) * 2
    made = pl.pallas_call(
        kernel,
        out_shape=(pltpu.VMEM((CAPS, WIDTH), F32),) * 2,
        in_specs=[hbm] * 9,
        out_specs=(vmem, vmem),
        scratch_shapes=[
            pltpu.VMEM((CTX + 1, CAPS, WIDTH), BF16),
            pltpu.VMEM((GROUPS, TOKENS_PAD, WIDTH), BF16),
            pltpu.VMEM((WIDTH, WIDTH), BF16),
            pltpu.VMEM((WIDTH, WIDTH), BF16),
            pltpu.VMEM((WIDTH, WIDTH), BF16),
            pltpu.VMEM((WIDTH, WIDTH), BF16),
            pltpu.VMEM((WIDTH, FF), BF16),
            pltpu.VMEM((FF, WIDTH), BF16),
            pltpu.VMEM((WIDTH, WIDTH), BF16),
            pltpu.VMEM((2, 128), jnp.int32),
            pltpu.SMEM((2, 128), jnp.int32),
            pltpu.VMEM((CAPS, WIDTH), BF16),
            pltpu.VMEM((GROUPS, SPLIT, TOKENS_PAD), F32),
            pltpu.VMEM((GROUPS, 2 * GROUP, TOKENS_PAD), F32),
            pltpu.VMEM((GROUPS, SPLIT, TOKENS_PAD), BF16),
            pltpu.VMEM((2, 2, CHIPS, CAPS, WIDTH), BF16),
            pltpu.VMEM((2, HALF, ROWS), F32),
            pltpu.VMEM((2, HALF, ROWS), F32),
            pltpu.VMEM((2, HALF, 1), F32),
            pltpu.VMEM((2, 1, ROWS), F32),
            pltpu.VMEM((2, CHIPS, PIECES, 1, PIECE), F32),
            pltpu.VMEM((2, CHIPS, HALF // PIECE, 1, PIECE), F32),
            pltpu.VMEM((ROWS, ROWS), BF16),
            pltpu.VMEM((2, CHIPS, CAPS, WIDTH), BF16),
            pltpu.VMEM((2, CHIPS, CAPS, WIDTH), BF16),
            dma((3,)),
            dma((LOAD_STEPS + 1,)),
            dma((7,)),
            dma((2, CHIPS)),
            dma((2, CHIPS)),
            dma((2, CHIPS)),
            dma((2, CHIPS)),
            dma((2, 2, CHIPS)),
            dma((2, 2, CHIPS)),
            dma((CHIPS, 2)),
            dma((2, CHIPS)),
        ],
        compiler_params=pltpu.CompilerParams(
            collective_id=0, has_side_effects=True, vmem_limit_bytes=VMEM_LIMIT
        ),
    )(
        captions.transpose(1, 0, 2),
        caption_layout,
        images,
        w_query,
        w_keyval,
        w_out,
        w_up,
        w_down,
        w_proj,
    )
    return pl.pallas_call(
        hand_out,
        out_shape=grads,
        in_specs=[vmem] * 2,
        out_specs=(vmem, vmem),
        compiler_params=pltpu.CompilerParams(vmem_limit_bytes=4 * 1024 * 1024),
    )(*made)


def solution(mesh):
    return jax.shard_map(
        body,
        mesh=mesh,
        in_specs=(P("dp", None, None), P(), P("dp", None), P(), P(), P(), P(), P(), P()),
        out_specs=(P("dp", None), P("dp", None)),
        check_vma=False,
    )
```

```python
import math

import jax
import jax.numpy as jnp
from jax import lax
from jax.experimental import pallas as pl
from jax.experimental.pallas import tpu as pltpu
from jax.sharding import PartitionSpec as P

HEADS = 12
HEAD_DIM = 64
WIDTH = 768
CTX = 77
CAPS = 32
FF = 3072
TILE = 16
GROUP = 8
GROUPS = CAPS // GROUP
SPLIT = HEADS * GROUP
PAIRS = (CTX + 1) // 2
TOKENS = PAIRS * 2 * GROUP
TOKENS_PAD = -(-TOKENS // 128) * 128
BLOCK = 256
BLOCK_HEADS = BLOCK // HEAD_DIM
BLOCKS = WIDTH // BLOCK
LOAD_STEPS = 6
STEP_T = 12
TAIL = CTX - LOAD_STEPS * STEP_T
CHIPS = 8
ARRIVAL = (7, 1, 6, 3, 2, 5, 4)
ROWS = CHIPS * 2 * CAPS
HALF = ROWS // 2
PIECE = 128
PIECES = ROWS // PIECE

VMEM_LIMIT = 60 * 1024 * 1024
TEXT_OUTER = "y"
LOGIT_SCALE = 100.0
EPS_NORM = 1e-05
EPS_UNIT = 1e-06
LOG2_E = math.log2(math.e)

MESH = pl.DeviceIdType.MESH
F32 = jnp.float32
BF16 = jnp.bfloat16


def norm_rows(values):
    center = values - jnp.mean(values, axis=-1, keepdims=True)
    spread = jnp.mean(center * center, axis=-1, keepdims=True)
    return center * lax.rsqrt(spread + EPS_NORM)


def unit_scale(values):
    return lax.rsqrt(jnp.sum(values * values, axis=-1, keepdims=True) + EPS_UNIT)


def unit_back(values, grad):
    scale = unit_scale(values)
    along = jnp.sum(values * grad, axis=-1, keepdims=True)
    return grad * scale - values * (along * (scale * scale * scale))


def dot(left, right):
    return jnp.dot(left, right, preferred_element_type=F32)


def dot_last(left, right):
    return lax.dot_general(left, right, (((1,), (1,)), ((), ())), preferred_element_type=F32)


def dot_first(left, right):
    return lax.dot_general(left, right, (((0,), (0,)), ((), ())), preferred_element_type=F32)


def iota(shape, dim):
    return lax.broadcasted_iota(jnp.int32, shape, dim)


class Place:
    def __init__(self):
        self.me = lax.axis_index("dp")
        self.core = self.me % 2
        self.at = {"y": (self.me // 2) % 4, "z": (self.me // 8) % 4, "x": self.me // 32}
        self.partner = self.me + 1 - 2 * self.core

    def flip(self, kind, axis):
        value = self.at[axis]
        outer, inner = 3 - value, value + 1 - 2 * (value % 2)
        kind = 1 - kind if axis in TEXT_OUTER else kind
        return outer + kind * (inner - outer)

    def bit(self, kind, axis, value):
        kind = 1 - kind if axis in TEXT_OUTER else kind
        return value // 2 + kind * (value % 2 - value // 2)

    def coords(self, kind, offset):
        return {
            axis: self.flip(kind, axis) if offset >> step & 1 else self.at[axis]
            for step, axis in enumerate("yzx")
        }

    def peer(self, kind, offset, core):
        where = self.coords(kind, offset)
        return ((where["x"] * 4 + where["z"]) * 4 + where["y"]) * 2 + core

    def slot(self, kind, offset):
        where = self.coords(kind, offset)
        bits = {axis: self.bit(kind, axis, where[axis]) for axis in "yzx"}
        return bits["x"] * 4 + bits["z"] * 2 + bits["y"]


def kernel(
    captions,
    layout,
    images,
    w_query,
    w_keyval,
    w_out,
    w_up,
    w_down,
    w_proj,
    image_grad,
    text_grad,
    tokens,
    normed,
    query_w,
    key_w,
    value_w,
    out_w,
    up_w,
    down_w,
    proj_w,
    counts,
    ends,
    image_rows,
    attn_scores,
    attn_bias,
    attn,
    units,
    row_exp,
    col_exp,
    row_peak,
    col_peak,
    image_logs,
    text_logs,
    weight,
    blocks,
    parts,
    small_sem,
    load_sem,
    weight_sem,
    gather_send,
    gather_recv,
    pass_send,
    pass_recv,
    log_send,
    log_recv,
    part_sem,
):
    place = Place()
    me, core, partner = place.me, place.core, place.partner

    def load(step, size=STEP_T):
        span = pl.ds(step * STEP_T, size)
        return pltpu.make_async_copy(captions.at[span], tokens.at[span], load_sem.at[step])

    span = pl.ds(pl.multiple_of(me // 4 * 128, 128), 128)
    load_counts = pltpu.make_async_copy(layout.at[:, span], counts, small_sem.at[0])
    load_images = pltpu.make_async_copy(images, image_rows, small_sem.at[1])
    load_ends = pltpu.make_async_copy(layout.at[:, span], ends, small_sem.at[2])
    weights = {}
    for number, (name, source, target) in enumerate(
        (
            ("query", w_query, query_w),
            ("key", w_keyval.at[:, :WIDTH], key_w),
            ("value", w_keyval.at[:, WIDTH:], value_w),
            ("out", w_out, out_w),
            ("up", w_up, up_w),
            ("down", w_down, down_w),
            ("proj", w_proj, proj_w),
        )
    ):
        weights[name] = pltpu.make_async_copy(source, target, weight_sem.at[number])
    for step in range(LOAD_STEPS):
        load(step).start()
    load_tail = load(LOAD_STEPS, TAIL)
    load_tail.start()
    for copy in (load_counts, load_ends, load_images):
        copy.start()
    for copy in weights.values():
        copy.start(priority=1)

    barrier = pltpu.get_barrier_semaphore()
    friends = [partner]
    for offset in range(1, CHIPS):
        for kind in range(2):
            friends += [place.peer(kind, offset, 0), place.peer(kind, offset, 1)]
    for friend in friends:
        pl.semaphore_signal(barrier, inc=1, device_id=(friend,), device_id_type=MESH)

    normed[:, TOKENS:, :] = jnp.zeros((GROUPS, TOKENS_PAD - TOKENS, WIDTH), BF16)
    tokens[CTX] = jnp.zeros((CAPS, WIDTH), BF16)


    def norm_pair(pair):
        at = pair * TILE if isinstance(pair, int) else pl.multiple_of(pair * TILE, TILE)
        for tile in range(0, CAPS, TILE):
            halves = [
                norm_rows(tokens[2 * pair + side, tile : tile + TILE, :].astype(F32))
                for side in range(2)
            ]
            for first in range(0, TILE, GROUP):
                rows = jnp.concatenate([half[first : first + GROUP] for half in halves], axis=0)
                normed[(tile + first) // GROUP, pl.ds(at, TILE), :] = rows.astype(BF16)

    def norm_step(step, _):
        load(step).wait()
        for inner in range(STEP_T // 2):
            norm_pair(step * (STEP_T // 2) + inner)
        return 0

    lax.fori_loop(0, LOAD_STEPS, norm_step, 0)
    load_tail.wait()
    for pair in range(LOAD_STEPS * STEP_T // 2, PAIRS):
        norm_pair(pair)

    load_ends.wait()
    load_counts.wait()
    weights["query"].wait()
    weights["key"].wait()
    end_values = []
    for first in range(0, CAPS, TILE):
        rows = jnp.zeros((TILE, WIDTH), BF16)
        for inner in range(TILE):
            last = jnp.clip(ends[0, me % 4 * CAPS + first + inner] - 1, 0, CTX - 1)
            found = tokens[last, first : first + TILE, :]
            rows = jnp.where(iota((TILE, WIDTH), 0) == inner, found, rows)
        end_values.append(rows)
    end_values = jnp.concatenate(end_values, axis=0).astype(F32)
    end_normed = norm_rows(end_values).astype(BF16)
    head_of = iota((GROUP, BLOCK), 1) // HEAD_DIM
    groups = [slice(group * GROUP, (group + 1) * GROUP) for group in range(GROUPS)]
    spans = [slice(at, at + BLOCK) for at in range(0, WIDTH, BLOCK)]
    key_query = []
    for span in spans:
        query = dot(end_normed, query_w[:, span]).astype(BF16).astype(F32)
        query = query * (1.0 / math.sqrt(HEAD_DIM))
        spread = [
            jnp.where(head_of == head, query[rows], 0.0)
            for rows in groups
            for head in range(BLOCK_HEADS)
        ]
        spread = jnp.concatenate(spread, axis=0).astype(BF16)
        key_query.append((dot_last(spread, key_w[:, span]) * LOG2_E).astype(BF16))

    picked = iota((CAPS, 128), 1) == iota((CAPS, 128), 0) + me % 4 * CAPS
    lengths = jnp.sum(jnp.where(picked, counts[0:1, :].astype(F32), 0.0), axis=1, keepdims=True)
    lengths = jnp.maximum(lengths, 1.0)

    token = iota((2 * GROUP, TOKENS_PAD), 1)
    own = token % GROUP == iota((2 * GROUP, TOKENS_PAD), 0) % GROUP
    for group in range(GROUPS):
        count = lengths[group * GROUP : (group + 1) * GROUP]
        count = jnp.concatenate([count, count], axis=0)
        inside = own & ((token // GROUP).astype(F32) < count)
        attn_bias[group] = jnp.where(inside, 0.0, -jnp.inf)

    part = BLOCK_HEADS * GROUP
    contexts = []
    for group in range(GROUPS):
        rows = slice(group * part, (group + 1) * part)
        asked = jnp.concatenate([block[rows] for block in key_query], axis=0)
        attn_scores[group] = dot_last(asked, normed[group])
    for group in range(GROUPS):
        totals = []
        for head in range(0, HEADS, 2):
            rows = slice(head * GROUP, (head + 2) * GROUP)
            value = attn_scores[group, rows, :] + attn_bias[group]
            value = jnp.exp2(value - jnp.max(value, axis=1, keepdims=True))
            attn[group, rows, :] = value.astype(BF16)
            totals.append(jnp.sum(value, axis=1, keepdims=True))
        context = dot(attn[group], normed[group]) / jnp.concatenate(totals, axis=0)
        contexts.append(context.astype(BF16))

    load_images.wait()
    image_values = image_rows[...].astype(F32)
    image_unit = (image_values * unit_scale(image_values)).astype(BF16)
    slots = (place.slot(0, 0), place.slot(1, 0))
    units[0, 0, slots[0]] = image_unit

    def all_of(buffer, semaphore):
        return pltpu.make_async_remote_copy(
            src_ref=buffer,
            dst_ref=buffer,
            send_sem=semaphore,
            recv_sem=semaphore,
            device_id=(partner,),
            device_id_type=MESH,
        )

    pl.semaphore_wait(barrier, len(friends))

    def send_units(kind):
        copies = {}
        for offset in range(CHIPS - 1, 0, -1):
            copies[offset] = pltpu.make_async_remote_copy(
                src_ref=units.at[kind, 0, slots[kind]],
                dst_ref=units.at[kind, 0, slots[kind]],
                send_sem=gather_send.at[kind],
                recv_sem=gather_recv.at[offset] if kind else gather_recv.at[0],
                device_id=(place.peer(kind, offset, core),),
                device_id_type=MESH,
            )
            copies[offset].start()
        return copies

    def hand_on(kind, offset):
        slot = place.slot(kind, offset)
        copy = pltpu.make_async_remote_copy(
            src_ref=units.at[kind, 0, slot],
            dst_ref=units.at[kind, 1, slot],
            send_sem=pass_send.at[kind],
            recv_sem=pass_recv.at[kind],
            device_id=(partner,),
            device_id_type=MESH,
        )
        copy.start()

    send_units(0)
    hand_on(0, 0)

    for name in ("value", "out", "up", "down", "proj"):
        weights[name].wait()
    mixed = []
    for number, span in enumerate(spans):
        rows = slice(number * part, (number + 1) * part)
        by_head = jnp.concatenate([context[rows] for context in contexts], axis=0)
        by_head = dot(by_head, value_w[:, span])
        sums = []
        for group in range(GROUPS):
            total = jnp.zeros((GROUP, BLOCK), F32)
            for head in range(BLOCK_HEADS):
                first = group * part + head * GROUP
                total = total + jnp.where(head_of == head, by_head[first : first + GROUP], 0.0)
            sums.append(total)
        mixed.append(jnp.concatenate(sums, axis=0))
    mixed = jnp.concatenate(mixed, axis=1).astype(BF16)

    residual = (end_values + dot(mixed, out_w[...])).astype(BF16)
    residual = residual.astype(F32)
    inner = norm_rows(residual).astype(BF16)
    final = residual
    for part in range(FF // WIDTH):
        span = slice(part * WIDTH, (part + 1) * WIDTH)
        hidden = dot(inner, up_w[:, span])
        hidden = 0.5 * hidden * (1.0 + lax.erf(hidden * (1.0 / math.sqrt(2.0))))
        final = final + dot(hidden.astype(BF16), down_w[span, :])
    pooled = norm_rows(final).astype(BF16)
    text_values = dot(pooled, proj_w[...]).astype(BF16).astype(F32)
    text_unit = (text_values * unit_scale(text_values)).astype(BF16)
    units[1, 0, slots[1]] = text_unit

    text_sends = send_units(1)
    hand_on(1, 0)

    all_of(units.at[0, 0, pl.ds(0, CHIPS - 1)], gather_recv.at[0]).wait_recv()
    for offset in range(1, CHIPS):
        hand_on(0, offset)

    for offset in ARRIVAL:
        text_sends[offset].wait_recv()
        hand_on(1, offset)
    all_of(units.at[0, 1], pass_recv.at[0]).wait_recv()

    eye = iota((PIECE, PIECE), 0) == iota((PIECE, PIECE), 1)
    half_pieces = HALF // PIECE

    def score(half):
        scores = dot_last(units[1, half].reshape(HALF, WIDTH), units[0].reshape(ROWS, WIDTH))
        scores = scores * (LOGIT_SCALE * LOG2_E)
        for axis, exp, top in ((1, row_exp, row_peak), (0, col_exp, col_peak)):
            peak = jnp.max(scores, axis=axis, keepdims=True)
            value = jnp.exp2(scores - peak)
            exp[half] = value
            top[half] = peak
            if half == 0:
                yield peak + jnp.log(jnp.sum(value, axis=axis, keepdims=True)) * LOG2_E

    row_log, col_log = score(0)
    for piece in range(half_pieces):
        part = row_log[piece * PIECE : (piece + 1) * PIECE]
        part = jnp.sum(jnp.where(eye, part, 0.0), axis=0, keepdims=True)
        text_logs[0, piece] = part
    for piece in range(PIECES):
        image_logs[0, piece] = col_log[:, piece * PIECE : (piece + 1) * PIECE]

    for offset in range(CHIPS - 1, -1, -1):
        for kind, logs in enumerate((image_logs, text_logs)):
            for side in range(2):
                if offset == 0 and side == 0:
                    continue
                copy = pltpu.make_async_remote_copy(
                    src_ref=logs.at[0],
                    dst_ref=logs.at[side * CHIPS + offset],
                    send_sem=log_send.at[kind],
                    recv_sem=log_recv.at[kind],
                    device_id=(place.peer(kind, offset, core + side - 2 * side * core),),
                    device_id_type=MESH,
                )
                copy.start()

    all_of(units.at[1, 1], pass_recv.at[1]).wait_recv()
    for _ in score(1):
        pass

    sent_logs = [logs.at[pl.ds(0, 2 * CHIPS - 1)] for logs in (image_logs, text_logs)]
    for kind in range(2):
        all_of(sent_logs[kind], log_recv.at[kind]).wait_recv()

    def whole_log(terms):
        top = terms[0]
        for term in terms[1:]:
            top = jnp.maximum(top, term)
        total = sum(jnp.exp2(term - top) for term in terms)
        return top + jnp.log(total) * LOG2_E

    terms = [image_logs[offset] for offset in range(CHIPS)]
    for offset in range(CHIPS):
        term = image_logs[CHIPS + offset]
        terms.append(jnp.concatenate([term[half_pieces:], term[:half_pieces]], axis=0))
    image_log = whole_log(terms)
    image_log = jnp.concatenate([image_log[piece] for piece in range(PIECES)], axis=1)
    for half in range(2):
        text_log = whole_log([text_logs[half * CHIPS + offset] for offset in range(CHIPS)])
        col_scale = jnp.exp2(col_peak[half] - image_log)
        for piece in range(half_pieces):
            rows = slice(piece * PIECE, (piece + 1) * PIECE)
            first = half * HALF + piece * PIECE
            log = jnp.sum(jnp.where(eye, text_log[piece], 0.0), axis=1, keepdims=True)
            row_scale = jnp.exp2(row_peak[half, rows] - log)
            both = row_exp[half, rows] * row_scale + col_exp[half, rows] * col_scale
            weight[first : first + PIECE, :] = both.astype(BF16)

    duty = 1 - core
    for far in (1, 0):
        first = place.slot(duty, 4 * far) // 4 * 4
        spans = [
            pl.ds(pl.multiple_of(side * HALF + first * CAPS, PIECE), PIECE) for side in range(2)
        ]

        def keep(grad):
            blocks[:, pl.ds(first, 4)] = grad.astype(BF16).reshape(2, 4, CAPS, WIDTH)

        @pl.when(duty == 0)
        def _():
            columns = jnp.concatenate([weight[:, span] for span in spans], axis=1)
            keep(dot_first(columns, units[1].reshape(ROWS, WIDTH)))

        @pl.when(duty == 1)
        def _():
            rows = jnp.concatenate([weight[span, :] for span in spans], axis=0)
            keep(dot(rows, units[0].reshape(ROWS, WIDTH)))

        for offset in range(4 * far + 3, 4 * far - 1, -1):
            slot = place.slot(duty, offset)
            for side in range(2):
                if offset == 0 and side == 0:
                    parts[duty * CHIPS] = blocks[0, slot]
                    continue
                copy = pltpu.make_async_remote_copy(
                    src_ref=blocks.at[side, slot],
                    dst_ref=parts.at[duty * CHIPS + offset],
                    send_sem=part_sem.at[0],
                    recv_sem=part_sem.at[1],
                    device_id=(place.peer(duty, offset, core + side - 2 * side * core),),
                    device_id_type=MESH,
                )
                copy.start()

    sent_parts = parts.at[pl.ds(0, 2 * CHIPS - 1)]
    all_of(sent_parts, part_sem.at[1]).wait_recv()

    half = 0.5 * LOGIT_SCALE
    sums = []
    for kind in range(2):
        total = parts[kind * CHIPS].astype(F32)
        for offset in range(1, CHIPS):
            total = total + parts[kind * CHIPS + offset].astype(F32)
        sums.append(total)
    image_unit_grad = half * sums[0] - LOGIT_SCALE * text_unit.astype(F32)
    text_unit_grad = half * sums[1] - LOGIT_SCALE * image_unit.astype(F32)
    image_grad[...] = unit_back(image_values, image_unit_grad)
    text_grad[...] = unit_back(text_values, text_unit_grad)

    for kind in range(2):
        all_of(units.at[kind, 0, pl.ds(0, CHIPS - 1)], gather_send.at[kind]).wait_send()
        all_of(units.at[kind, 0], pass_send.at[kind]).wait_send()
        all_of(sent_logs[kind], log_send.at[kind]).wait_send()
    all_of(sent_parts, part_sem.at[0]).wait_send()


def hand_out(image_from, text_from, image_to, text_to):
    image_to[...] = image_from[...]
    text_to[...] = text_from[...]


def body(captions, caption_layout, images, w_query, w_keyval, w_out, w_up, w_down, w_proj):
    hbm = pl.BlockSpec(memory_space=pl.ANY)
    vmem = pl.BlockSpec(memory_space=pltpu.VMEM)
    dma = pltpu.SemaphoreType.DMA
    grads = (jax.ShapeDtypeStruct((CAPS, WIDTH), F32),) * 2
    made = pl.pallas_call(
        kernel,
        out_shape=(pltpu.VMEM((CAPS, WIDTH), F32),) * 2,
        in_specs=[hbm] * 9,
        out_specs=(vmem, vmem),
        scratch_shapes=[
            pltpu.VMEM((CTX + 1, CAPS, WIDTH), BF16),
            pltpu.VMEM((GROUPS, TOKENS_PAD, WIDTH), BF16),
            pltpu.VMEM((WIDTH, WIDTH), BF16),
            pltpu.VMEM((WIDTH, WIDTH), BF16),
            pltpu.VMEM((WIDTH, WIDTH), BF16),
            pltpu.VMEM((WIDTH, WIDTH), BF16),
            pltpu.VMEM((WIDTH, FF), BF16),
            pltpu.VMEM((FF, WIDTH), BF16),
            pltpu.VMEM((WIDTH, WIDTH), BF16),
            pltpu.VMEM((2, 128), jnp.int32),
            pltpu.SMEM((2, 128), jnp.int32),
            pltpu.VMEM((CAPS, WIDTH), BF16),
            pltpu.VMEM((GROUPS, SPLIT, TOKENS_PAD), F32),
            pltpu.VMEM((GROUPS, 2 * GROUP, TOKENS_PAD), F32),
            pltpu.VMEM((GROUPS, SPLIT, TOKENS_PAD), BF16),
            pltpu.VMEM((2, 2, CHIPS, CAPS, WIDTH), BF16),
            pltpu.VMEM((2, HALF, ROWS), F32),
            pltpu.VMEM((2, HALF, ROWS), F32),
            pltpu.VMEM((2, HALF, 1), F32),
            pltpu.VMEM((2, 1, ROWS), F32),
            pltpu.VMEM((2 * CHIPS, PIECES, 1, PIECE), F32),
            pltpu.VMEM((2 * CHIPS, HALF // PIECE, 1, PIECE), F32),
            pltpu.VMEM((ROWS, ROWS), BF16),
            pltpu.VMEM((2, CHIPS, CAPS, WIDTH), BF16),
            pltpu.VMEM((2 * CHIPS, CAPS, WIDTH), BF16),
            dma((3,)),
            dma((LOAD_STEPS + 1,)),
            dma((7,)),
            dma((2,)),
            dma((CHIPS,)),
            dma((2,)),
            dma((2,)),
            dma((2,)),
            dma((2,)),
            dma((2,)),
        ],
        compiler_params=pltpu.CompilerParams(
            collective_id=0, has_side_effects=True, vmem_limit_bytes=VMEM_LIMIT
        ),
    )(
        captions.transpose(1, 0, 2),
        caption_layout,
        images,
        w_query,
        w_keyval,
        w_out,
        w_up,
        w_down,
        w_proj,
    )
    return pl.pallas_call(
        hand_out,
        out_shape=grads,
        in_specs=[vmem] * 2,
        out_specs=(vmem, vmem),
        compiler_params=pltpu.CompilerParams(vmem_limit_bytes=4 * 1024 * 1024),
    )(*made)


def solution(mesh):
    return jax.shard_map(
        body,
        mesh=mesh,
        in_specs=(P("dp", None, None), P(), P("dp", None), P(), P(), P(), P(), P(), P()),
        out_specs=(P("dp", None), P("dp", None)),
        check_vma=False,
    )
```

```python
import math

import jax
import jax.numpy as jnp
from jax import lax
from jax.experimental import pallas as pl
from jax.experimental.pallas import tpu as pltpu
from jax.sharding import PartitionSpec as P

HEADS = 12
HEAD_DIM = 64
WIDTH = 768
CTX = 77
CAPS = 32
FF = 3072
TILE = 16
GROUP = 8
GROUPS = CAPS // GROUP
SPLIT = HEADS * GROUP
PAIRS = (CTX + 1) // 2
TOKENS = PAIRS * 2 * GROUP
TOKENS_PAD = -(-TOKENS // 128) * 128
BLOCK = 256
BLOCK_HEADS = BLOCK // HEAD_DIM
BLOCKS = WIDTH // BLOCK
LOAD_STEPS = 6
STEP_T = 12
TAIL = CTX - LOAD_STEPS * STEP_T
CHIPS = 8
ROWS = CHIPS * 2 * CAPS
HALF = ROWS // 2
PIECE = 128
PIECES = ROWS // PIECE

VMEM_LIMIT = 60 * 1024 * 1024
TEXT_OUTER = "y"
LOGIT_SCALE = 100.0
EPS_NORM = 1e-05
EPS_UNIT = 1e-06
LOG2_E = math.log2(math.e)

MESH = pl.DeviceIdType.MESH
F32 = jnp.float32
BF16 = jnp.bfloat16


def norm_rows(values):
    center = values - jnp.mean(values, axis=-1, keepdims=True)
    spread = jnp.mean(center * center, axis=-1, keepdims=True)
    return center * lax.rsqrt(spread + EPS_NORM)


def unit_scale(values):
    return lax.rsqrt(jnp.sum(values * values, axis=-1, keepdims=True) + EPS_UNIT)


def unit_back(values, grad):
    scale = unit_scale(values)
    along = jnp.sum(values * grad, axis=-1, keepdims=True)
    return grad * scale - values * (along * (scale * scale * scale))


def dot(left, right):
    return jnp.dot(left, right, preferred_element_type=F32)


def dot_last(left, right):
    return lax.dot_general(left, right, (((1,), (1,)), ((), ())), preferred_element_type=F32)


def dot_first(left, right):
    return lax.dot_general(left, right, (((0,), (0,)), ((), ())), preferred_element_type=F32)


def iota(shape, dim):
    return lax.broadcasted_iota(jnp.int32, shape, dim)


class Place:
    def __init__(self):
        self.me = lax.axis_index("dp")
        self.core = self.me % 2
        self.at = {"y": (self.me // 2) % 4, "z": (self.me // 8) % 4, "x": self.me // 32}
        self.partner = self.me + 1 - 2 * self.core

    def flip(self, kind, axis):
        value = self.at[axis]
        outer, inner = 3 - value, value + 1 - 2 * (value % 2)
        kind = 1 - kind if axis in TEXT_OUTER else kind
        return outer + kind * (inner - outer)

    def bit(self, kind, axis, value):
        kind = 1 - kind if axis in TEXT_OUTER else kind
        return value // 2 + kind * (value % 2 - value // 2)

    def coords(self, kind, offset):
        return {
            axis: self.flip(kind, axis) if offset >> step & 1 else self.at[axis]
            for step, axis in enumerate("yzx")
        }

    def peer(self, kind, offset, core):
        where = self.coords(kind, offset)
        return ((where["x"] * 4 + where["z"]) * 4 + where["y"]) * 2 + core

    def slot(self, kind, offset):
        where = self.coords(kind, offset)
        bits = {axis: self.bit(kind, axis, where[axis]) for axis in "yzx"}
        return bits["x"] * 4 + bits["z"] * 2 + bits["y"]


def kernel(
    captions,
    layout,
    images,
    w_query,
    w_keyval,
    w_out,
    w_up,
    w_down,
    w_proj,
    image_grad,
    text_grad,
    tokens,
    normed,
    query_w,
    key_w,
    value_w,
    out_w,
    up_w,
    down_w,
    proj_w,
    counts,
    ends,
    image_rows,
    attn_scores,
    attn_bias,
    attn,
    units,
    row_exp,
    col_exp,
    row_peak,
    col_peak,
    image_logs,
    text_logs,
    weight,
    blocks,
    parts,
    small_sem,
    load_sem,
    weight_sem,
    gather_send,
    gather_recv,
    pass_send,
    pass_recv,
    log_send,
    log_recv,
    part_sem,
):
    place = Place()
    me, core, partner = place.me, place.core, place.partner

    def load(step, size=STEP_T):
        span = pl.ds(step * STEP_T, size)
        return pltpu.make_async_copy(captions.at[span], tokens.at[span], load_sem.at[step])

    span = pl.ds(pl.multiple_of(me // 4 * 128, 128), 128)
    load_counts = pltpu.make_async_copy(layout.at[:, span], counts, small_sem.at[0])
    load_images = pltpu.make_async_copy(images, image_rows, small_sem.at[1])
    load_ends = pltpu.make_async_copy(layout.at[:, span], ends, small_sem.at[2])
    weights = {}
    for number, (name, source, target) in enumerate(
        (
            ("query", w_query, query_w),
            ("key", w_keyval.at[:, :WIDTH], key_w),
            ("value", w_keyval.at[:, WIDTH:], value_w),
            ("out", w_out, out_w),
            ("up", w_up, up_w),
            ("down", w_down, down_w),
            ("proj", w_proj, proj_w),
        )
    ):
        weights[name] = pltpu.make_async_copy(source, target, weight_sem.at[number])
    for step in range(LOAD_STEPS):
        load(step).start()
    load_tail = load(LOAD_STEPS, TAIL)
    load_tail.start()
    for copy in (load_counts, load_ends, load_images):
        copy.start()
    for copy in weights.values():
        copy.start(priority=1)

    barrier = pltpu.get_barrier_semaphore()
    friends = [partner]
    for offset in range(1, CHIPS):
        for kind in range(2):
            friends += [place.peer(kind, offset, 0), place.peer(kind, offset, 1)]
    for friend in friends:
        pl.semaphore_signal(barrier, inc=1, device_id=(friend,), device_id_type=MESH)

    normed[:, TOKENS:, :] = jnp.zeros((GROUPS, TOKENS_PAD - TOKENS, WIDTH), BF16)
    tokens[CTX] = jnp.zeros((CAPS, WIDTH), BF16)


    def norm_pair(pair):
        at = pair * TILE if isinstance(pair, int) else pl.multiple_of(pair * TILE, TILE)
        for tile in range(0, CAPS, TILE):
            halves = [
                norm_rows(tokens[2 * pair + side, tile : tile + TILE, :].astype(F32))
                for side in range(2)
            ]
            for first in range(0, TILE, GROUP):
                rows = jnp.concatenate([half[first : first + GROUP] for half in halves], axis=0)
                normed[(tile + first) // GROUP, pl.ds(at, TILE), :] = rows.astype(BF16)

    def norm_step(step, _):
        load(step).wait()
        for inner in range(STEP_T // 2):
            norm_pair(step * (STEP_T // 2) + inner)
        return 0

    lax.fori_loop(0, LOAD_STEPS, norm_step, 0)
    load_tail.wait()
    for pair in range(LOAD_STEPS * STEP_T // 2, PAIRS):
        norm_pair(pair)

    load_ends.wait()
    load_counts.wait()
    weights["query"].wait()
    weights["key"].wait()
    end_values = []
    for first in range(0, CAPS, TILE):
        rows = jnp.zeros((TILE, WIDTH), BF16)
        for inner in range(TILE):
            last = jnp.clip(ends[0, me % 4 * CAPS + first + inner] - 1, 0, CTX - 1)
            found = tokens[last, first : first + TILE, :]
            rows = jnp.where(iota((TILE, WIDTH), 0) == inner, found, rows)
        end_values.append(rows)
    end_values = jnp.concatenate(end_values, axis=0).astype(F32)
    end_normed = norm_rows(end_values).astype(BF16)
    head_of = iota((GROUP, BLOCK), 1) // HEAD_DIM
    groups = [slice(group * GROUP, (group + 1) * GROUP) for group in range(GROUPS)]
    spans = [slice(at, at + BLOCK) for at in range(0, WIDTH, BLOCK)]
    key_query = []
    for span in spans:
        query = dot(end_normed, query_w[:, span]).astype(BF16).astype(F32)
        query = query * (1.0 / math.sqrt(HEAD_DIM))
        spread = [
            jnp.where(head_of == head, query[rows], 0.0)
            for rows in groups
            for head in range(BLOCK_HEADS)
        ]
        spread = jnp.concatenate(spread, axis=0).astype(BF16)
        key_query.append((dot_last(spread, key_w[:, span]) * LOG2_E).astype(BF16))

    picked = iota((CAPS, 128), 1) == iota((CAPS, 128), 0) + me % 4 * CAPS
    lengths = jnp.sum(jnp.where(picked, counts[0:1, :].astype(F32), 0.0), axis=1, keepdims=True)
    lengths = jnp.maximum(lengths, 1.0)

    token = iota((2 * GROUP, TOKENS_PAD), 1)
    own = token % GROUP == iota((2 * GROUP, TOKENS_PAD), 0) % GROUP
    for group in range(GROUPS):
        count = lengths[group * GROUP : (group + 1) * GROUP]
        count = jnp.concatenate([count, count], axis=0)
        inside = own & ((token // GROUP).astype(F32) < count)
        attn_bias[group] = jnp.where(inside, 0.0, -jnp.inf)

    part = BLOCK_HEADS * GROUP
    contexts = []
    for group in range(GROUPS):
        rows = slice(group * part, (group + 1) * part)
        asked = jnp.concatenate([block[rows] for block in key_query], axis=0)
        attn_scores[group] = dot_last(asked, normed[group])
    for group in range(GROUPS):
        totals = []
        for head in range(0, HEADS, 2):
            rows = slice(head * GROUP, (head + 2) * GROUP)
            value = attn_scores[group, rows, :] + attn_bias[group]
            value = jnp.exp2(value - jnp.max(value, axis=1, keepdims=True))
            attn[group, rows, :] = value.astype(BF16)
            totals.append(jnp.sum(value, axis=1, keepdims=True))
        context = dot(attn[group], normed[group]) / jnp.concatenate(totals, axis=0)
        contexts.append(context.astype(BF16))

    load_images.wait()
    image_values = image_rows[...].astype(F32)
    image_unit = (image_values * unit_scale(image_values)).astype(BF16)
    slots = (place.slot(0, 0), place.slot(1, 0))
    units[0, 0, slots[0]] = image_unit

    def all_of(buffer, semaphore):
        return pltpu.make_async_remote_copy(
            src_ref=buffer,
            dst_ref=buffer,
            send_sem=semaphore,
            recv_sem=semaphore,
            device_id=(partner,),
            device_id_type=MESH,
        )

    pl.semaphore_wait(barrier, len(friends))

    def send_units(kind):
        for offset in range(CHIPS - 1, 0, -1):
            copy = pltpu.make_async_remote_copy(
                src_ref=units.at[kind, 0, slots[kind]],
                dst_ref=units.at[kind, 0, slots[kind]],
                send_sem=gather_send.at[kind],
                recv_sem=gather_recv.at[kind],
                device_id=(place.peer(kind, offset, core),),
                device_id_type=MESH,
            )
            copy.start()

    def hand_on(kind, offset):
        slot = place.slot(kind, offset)
        copy = pltpu.make_async_remote_copy(
            src_ref=units.at[kind, 0, slot],
            dst_ref=units.at[kind, 1, slot],
            send_sem=pass_send.at[kind],
            recv_sem=pass_recv.at[kind],
            device_id=(partner,),
            device_id_type=MESH,
        )
        copy.start()

    send_units(0)
    hand_on(0, 0)

    for name in ("value", "out", "up", "down", "proj"):
        weights[name].wait()
    mixed = []
    for number, span in enumerate(spans):
        rows = slice(number * part, (number + 1) * part)
        by_head = jnp.concatenate([context[rows] for context in contexts], axis=0)
        by_head = dot(by_head, value_w[:, span])
        sums = []
        for group in range(GROUPS):
            total = jnp.zeros((GROUP, BLOCK), F32)
            for head in range(BLOCK_HEADS):
                first = group * part + head * GROUP
                total = total + jnp.where(head_of == head, by_head[first : first + GROUP], 0.0)
            sums.append(total)
        mixed.append(jnp.concatenate(sums, axis=0))
    mixed = jnp.concatenate(mixed, axis=1).astype(BF16)

    residual = (end_values + dot(mixed, out_w[...])).astype(BF16)
    residual = residual.astype(F32)
    inner = norm_rows(residual).astype(BF16)
    final = residual
    for part in range(FF // WIDTH):
        span = slice(part * WIDTH, (part + 1) * WIDTH)
        hidden = dot(inner, up_w[:, span])
        hidden = 0.5 * hidden * (1.0 + lax.erf(hidden * (1.0 / math.sqrt(2.0))))
        final = final + dot(hidden.astype(BF16), down_w[span, :])
    pooled = norm_rows(final).astype(BF16)
    text_values = dot(pooled, proj_w[...]).astype(BF16).astype(F32)
    text_unit = (text_values * unit_scale(text_values)).astype(BF16)
    units[1, 0, slots[1]] = text_unit

    send_units(1)
    hand_on(1, 0)

    all_of(units.at[0, 0, pl.ds(0, CHIPS - 1)], gather_recv.at[0]).wait_recv()
    for offset in range(1, CHIPS):
        hand_on(0, offset)

    all_of(units.at[1, 0, pl.ds(0, CHIPS - 1)], gather_recv.at[1]).wait_recv()
    for offset in range(1, CHIPS):
        hand_on(1, offset)
    all_of(units.at[0, 1], pass_recv.at[0]).wait_recv()

    eye = iota((PIECE, PIECE), 0) == iota((PIECE, PIECE), 1)
    half_pieces = HALF // PIECE

    def score(half):
        scores = dot_last(units[1, half].reshape(HALF, WIDTH), units[0].reshape(ROWS, WIDTH))
        scores = scores * (LOGIT_SCALE * LOG2_E)
        for axis, exp, top in ((1, row_exp, row_peak), (0, col_exp, col_peak)):
            peak = jnp.max(scores, axis=axis, keepdims=True)
            value = jnp.exp2(scores - peak)
            exp[half] = value
            top[half] = peak
            if half == 0:
                yield peak + jnp.log(jnp.sum(value, axis=axis, keepdims=True)) * LOG2_E

    row_log, col_log = score(0)
    for piece in range(half_pieces):
        part = row_log[piece * PIECE : (piece + 1) * PIECE]
        part = jnp.sum(jnp.where(eye, part, 0.0), axis=0, keepdims=True)
        text_logs[0, piece] = part
    for piece in range(PIECES):
        image_logs[0, piece] = col_log[:, piece * PIECE : (piece + 1) * PIECE]

    for offset in range(CHIPS - 1, -1, -1):
        for kind, logs in enumerate((image_logs, text_logs)):
            for side in range(2):
                if offset == 0 and side == 0:
                    continue
                copy = pltpu.make_async_remote_copy(
                    src_ref=logs.at[0],
                    dst_ref=logs.at[side * CHIPS + offset],
                    send_sem=log_send.at[kind],
                    recv_sem=log_recv.at[kind],
                    device_id=(place.peer(kind, offset, core + side - 2 * side * core),),
                    device_id_type=MESH,
                )
                copy.start()

    all_of(units.at[1, 1], pass_recv.at[1]).wait_recv()
    for _ in score(1):
        pass

    sent_logs = [logs.at[pl.ds(0, 2 * CHIPS - 1)] for logs in (image_logs, text_logs)]
    for kind in range(2):
        all_of(sent_logs[kind], log_recv.at[kind]).wait_recv()

    def whole_log(terms):
        top = terms[0]
        for term in terms[1:]:
            top = jnp.maximum(top, term)
        total = sum(jnp.exp2(term - top) for term in terms)
        return top + jnp.log(total) * LOG2_E

    terms = [image_logs[offset] for offset in range(CHIPS)]
    for offset in range(CHIPS):
        term = image_logs[CHIPS + offset]
        terms.append(jnp.concatenate([term[half_pieces:], term[:half_pieces]], axis=0))
    image_log = whole_log(terms)
    image_log = jnp.concatenate([image_log[piece] for piece in range(PIECES)], axis=1)
    for half in range(2):
        text_log = whole_log([text_logs[half * CHIPS + offset] for offset in range(CHIPS)])
        col_scale = jnp.exp2(col_peak[half] - image_log)
        for piece in range(half_pieces):
            rows = slice(piece * PIECE, (piece + 1) * PIECE)
            first = half * HALF + piece * PIECE
            log = jnp.sum(jnp.where(eye, text_log[piece], 0.0), axis=1, keepdims=True)
            row_scale = jnp.exp2(row_peak[half, rows] - log)
            both = row_exp[half, rows] * row_scale + col_exp[half, rows] * col_scale
            weight[first : first + PIECE, :] = both.astype(BF16)

    duty = 1 - core
    for far in (1, 0):
        first = place.slot(duty, 4 * far) // 4 * 4
        spans = [
            pl.ds(pl.multiple_of(side * HALF + first * CAPS, PIECE), PIECE) for side in range(2)
        ]

        def keep(grad):
            blocks[:, pl.ds(first, 4)] = grad.astype(BF16).reshape(2, 4, CAPS, WIDTH)

        @pl.when(duty == 0)
        def _():
            columns = jnp.concatenate([weight[:, span] for span in spans], axis=1)
            keep(dot_first(columns, units[1].reshape(ROWS, WIDTH)))

        @pl.when(duty == 1)
        def _():
            rows = jnp.concatenate([weight[span, :] for span in spans], axis=0)
            keep(dot(rows, units[0].reshape(ROWS, WIDTH)))

        for offset in range(4 * far + 3, 4 * far - 1, -1):
            slot = place.slot(duty, offset)
            for side in range(2):
                if offset == 0 and side == 0:
                    parts[duty * CHIPS] = blocks[0, slot]
                    continue
                copy = pltpu.make_async_remote_copy(
                    src_ref=blocks.at[side, slot],
                    dst_ref=parts.at[duty * CHIPS + offset],
                    send_sem=part_sem.at[0],
                    recv_sem=part_sem.at[1],
                    device_id=(place.peer(duty, offset, core + side - 2 * side * core),),
                    device_id_type=MESH,
                )
                copy.start()

    sent_parts = parts.at[pl.ds(0, 2 * CHIPS - 1)]
    all_of(sent_parts, part_sem.at[1]).wait_recv()

    half = 0.5 * LOGIT_SCALE
    sums = []
    for kind in range(2):
        total = parts[kind * CHIPS].astype(F32)
        for offset in range(1, CHIPS):
            total = total + parts[kind * CHIPS + offset].astype(F32)
        sums.append(total)
    image_unit_grad = half * sums[0] - LOGIT_SCALE * text_unit.astype(F32)
    text_unit_grad = half * sums[1] - LOGIT_SCALE * image_unit.astype(F32)
    image_grad[...] = unit_back(image_values, image_unit_grad)
    text_grad[...] = unit_back(text_values, text_unit_grad)

    for kind in range(2):
        all_of(units.at[kind, 0, pl.ds(0, CHIPS - 1)], gather_send.at[kind]).wait_send()
        all_of(units.at[kind, 0], pass_send.at[kind]).wait_send()
        all_of(sent_logs[kind], log_send.at[kind]).wait_send()
    all_of(sent_parts, part_sem.at[0]).wait_send()


def hand_out(image_from, text_from, image_to, text_to):
    image_to[...] = image_from[...]
    text_to[...] = text_from[...]


def body(captions, caption_layout, images, w_query, w_keyval, w_out, w_up, w_down, w_proj):
    hbm = pl.BlockSpec(memory_space=pl.ANY)
    vmem = pl.BlockSpec(memory_space=pltpu.VMEM)
    dma = pltpu.SemaphoreType.DMA
    grads = (jax.ShapeDtypeStruct((CAPS, WIDTH), F32),) * 2
    made = pl.pallas_call(
        kernel,
        out_shape=(pltpu.VMEM((CAPS, WIDTH), F32),) * 2,
        in_specs=[hbm] * 9,
        out_specs=(vmem, vmem),
        scratch_shapes=[
            pltpu.VMEM((CTX + 1, CAPS, WIDTH), BF16),
            pltpu.VMEM((GROUPS, TOKENS_PAD, WIDTH), BF16),
            pltpu.VMEM((WIDTH, WIDTH), BF16),
            pltpu.VMEM((WIDTH, WIDTH), BF16),
            pltpu.VMEM((WIDTH, WIDTH), BF16),
            pltpu.VMEM((WIDTH, WIDTH), BF16),
            pltpu.VMEM((WIDTH, FF), BF16),
            pltpu.VMEM((FF, WIDTH), BF16),
            pltpu.VMEM((WIDTH, WIDTH), BF16),
            pltpu.VMEM((2, 128), jnp.int32),
            pltpu.SMEM((2, 128), jnp.int32),
            pltpu.VMEM((CAPS, WIDTH), BF16),
            pltpu.VMEM((GROUPS, SPLIT, TOKENS_PAD), F32),
            pltpu.VMEM((GROUPS, 2 * GROUP, TOKENS_PAD), F32),
            pltpu.VMEM((GROUPS, SPLIT, TOKENS_PAD), BF16),
            pltpu.VMEM((2, 2, CHIPS, CAPS, WIDTH), BF16),
            pltpu.VMEM((2, HALF, ROWS), F32),
            pltpu.VMEM((2, HALF, ROWS), F32),
            pltpu.VMEM((2, HALF, 1), F32),
            pltpu.VMEM((2, 1, ROWS), F32),
            pltpu.VMEM((2 * CHIPS, PIECES, 1, PIECE), F32),
            pltpu.VMEM((2 * CHIPS, HALF // PIECE, 1, PIECE), F32),
            pltpu.VMEM((ROWS, ROWS), BF16),
            pltpu.VMEM((2, CHIPS, CAPS, WIDTH), BF16),
            pltpu.VMEM((2 * CHIPS, CAPS, WIDTH), BF16),
            dma((3,)),
            dma((LOAD_STEPS + 1,)),
            dma((7,)),
            dma((2,)),
            dma((2,)),
            dma((2,)),
            dma((2,)),
            dma((2,)),
            dma((2,)),
            dma((2,)),
        ],
        compiler_params=pltpu.CompilerParams(
            collective_id=0, has_side_effects=True, vmem_limit_bytes=VMEM_LIMIT
        ),
    )(
        captions.transpose(1, 0, 2),
        caption_layout,
        images,
        w_query,
        w_keyval,
        w_out,
        w_up,
        w_down,
        w_proj,
    )
    return pl.pallas_call(
        hand_out,
        out_shape=grads,
        in_specs=[vmem] * 2,
        out_specs=(vmem, vmem),
        compiler_params=pltpu.CompilerParams(vmem_limit_bytes=4 * 1024 * 1024),
    )(*made)


def solution(mesh):
    return jax.shard_map(
        body,
        mesh=mesh,
        in_specs=(P("dp", None, None), P(), P("dp", None), P(), P(), P(), P(), P(), P()),
        out_specs=(P("dp", None), P("dp", None)),
        check_vma=False,
    )
```

```python
import math

import jax
import jax.numpy as jnp
from jax import lax
from jax.experimental import pallas as pl
from jax.experimental.pallas import tpu as pltpu
from jax.sharding import PartitionSpec as P

HEADS = 12
HEAD_DIM = 64
WIDTH = 768
CTX = 77
CAPS = 32
FF = 3072
TILE = 16
GROUP = 8
GROUPS = CAPS // GROUP
SPLIT = HEADS * GROUP
PAIRS = (CTX + 1) // 2
TOKENS = PAIRS * 2 * GROUP
TOKENS_PAD = -(-TOKENS // 128) * 128
BLOCK = 256
BLOCK_HEADS = BLOCK // HEAD_DIM
BLOCKS = WIDTH // BLOCK
LOAD_STEPS = 6
STEP_T = 12
TAIL = CTX - LOAD_STEPS * STEP_T
CHIPS = 8
ROWS = CHIPS * 2 * CAPS
HALF = ROWS // 2
PIECE = 128
PIECES = ROWS // PIECE

VMEM_LIMIT = 60 * 1024 * 1024
TEXT_OUTER = "y"
LOGIT_SCALE = 100.0
EPS_NORM = 1e-05
EPS_UNIT = 1e-06
LOG2_E = math.log2(math.e)

MESH = pl.DeviceIdType.MESH
F32 = jnp.float32
BF16 = jnp.bfloat16


def norm_rows(values):
    center = values - jnp.mean(values, axis=-1, keepdims=True)
    spread = jnp.mean(center * center, axis=-1, keepdims=True)
    return center * lax.rsqrt(spread + EPS_NORM)


def unit_scale(values):
    return lax.rsqrt(jnp.sum(values * values, axis=-1, keepdims=True) + EPS_UNIT)


def unit_back(values, grad):
    scale = unit_scale(values)
    along = jnp.sum(values * grad, axis=-1, keepdims=True)
    return grad * scale - values * (along * (scale * scale * scale))


def dot(left, right):
    return jnp.dot(left, right, preferred_element_type=F32)


def dot_last(left, right):
    return lax.dot_general(left, right, (((1,), (1,)), ((), ())), preferred_element_type=F32)


def dot_first(left, right):
    return lax.dot_general(left, right, (((0,), (0,)), ((), ())), preferred_element_type=F32)


def iota(shape, dim):
    return lax.broadcasted_iota(jnp.int32, shape, dim)


class Place:
    def __init__(self):
        self.me = lax.axis_index("dp")
        self.core = self.me % 2
        self.at = {"y": (self.me // 2) % 4, "z": (self.me // 8) % 4, "x": self.me // 32}
        self.partner = self.me + 1 - 2 * self.core

    def flip(self, kind, axis):
        value = self.at[axis]
        outer, inner = 3 - value, value + 1 - 2 * (value % 2)
        kind = 1 - kind if axis in TEXT_OUTER else kind
        return outer + kind * (inner - outer)

    def bit(self, kind, axis, value):
        kind = 1 - kind if axis in TEXT_OUTER else kind
        return value // 2 + kind * (value % 2 - value // 2)

    def coords(self, kind, offset):
        return {
            axis: self.flip(kind, axis) if offset >> step & 1 else self.at[axis]
            for step, axis in enumerate("yzx")
        }

    def peer(self, kind, offset, core):
        where = self.coords(kind, offset)
        return ((where["x"] * 4 + where["z"]) * 4 + where["y"]) * 2 + core

    def slot(self, kind, offset):
        where = self.coords(kind, offset)
        bits = {axis: self.bit(kind, axis, where[axis]) for axis in "yzx"}
        return bits["x"] * 4 + bits["z"] * 2 + bits["y"]


def kernel(
    captions,
    layout,
    images,
    w_query,
    w_keyval,
    w_out,
    w_up,
    w_down,
    w_proj,
    image_grad,
    text_grad,
    tokens,
    normed,
    query_w,
    key_w,
    value_w,
    out_w,
    up_w,
    down_w,
    proj_w,
    counts,
    ends,
    image_rows,
    attn_scores,
    attn_bias,
    attn,
    units,
    row_exp,
    col_exp,
    row_peak,
    col_peak,
    image_logs,
    text_logs,
    weight,
    blocks,
    parts,
    small_sem,
    load_sem,
    weight_sem,
    gather_send,
    gather_recv,
    pass_send,
    pass_recv,
    log_send,
    log_recv,
    part_sem,
):
    place = Place()
    me, core, partner = place.me, place.core, place.partner

    def load(step, size=STEP_T):
        span = pl.ds(step * STEP_T, size)
        return pltpu.make_async_copy(captions.at[span], tokens.at[span], load_sem.at[step])

    span = pl.ds(pl.multiple_of(me // 4 * 128, 128), 128)
    load_counts = pltpu.make_async_copy(layout.at[:, span], counts, small_sem.at[0])
    load_images = pltpu.make_async_copy(images, image_rows, small_sem.at[1])
    load_ends = pltpu.make_async_copy(layout.at[:, span], ends, small_sem.at[2])
    weights = {}
    for number, (name, source, target) in enumerate(
        (
            ("query", w_query, query_w),
            ("key", w_keyval.at[:, :WIDTH], key_w),
            ("value", w_keyval.at[:, WIDTH:], value_w),
            ("out", w_out, out_w),
            ("up", w_up, up_w),
            ("down", w_down, down_w),
            ("proj", w_proj, proj_w),
        )
    ):
        weights[name] = pltpu.make_async_copy(source, target, weight_sem.at[number])
    for step in range(LOAD_STEPS):
        load(step).start()
    load_tail = load(LOAD_STEPS, TAIL)
    load_tail.start()
    for copy in (load_counts, load_ends, load_images):
        copy.start()
    for copy in weights.values():
        copy.start(priority=1)

    barrier = pltpu.get_barrier_semaphore()
    friends = [partner]
    for offset in range(1, CHIPS):
        for kind in range(2):
            friends += [place.peer(kind, offset, 0), place.peer(kind, offset, 1)]
    for friend in friends:
        pl.semaphore_signal(barrier, inc=1, device_id=(friend,), device_id_type=MESH)

    normed[:, TOKENS:, :] = jnp.zeros((GROUPS, TOKENS_PAD - TOKENS, WIDTH), BF16)
    tokens[CTX] = jnp.zeros((CAPS, WIDTH), BF16)


    def norm_pair(pair):
        at = pair * TILE if isinstance(pair, int) else pl.multiple_of(pair * TILE, TILE)
        for tile in range(0, CAPS, TILE):
            halves = [
                norm_rows(tokens[2 * pair + side, tile : tile + TILE, :].astype(F32))
                for side in range(2)
            ]
            for first in range(0, TILE, GROUP):
                rows = jnp.concatenate([half[first : first + GROUP] for half in halves], axis=0)
                normed[(tile + first) // GROUP, pl.ds(at, TILE), :] = rows.astype(BF16)

    def norm_step(step, _):
        load(step).wait()
        for inner in range(STEP_T // 2):
            norm_pair(step * (STEP_T // 2) + inner)
        return 0

    lax.fori_loop(0, LOAD_STEPS, norm_step, 0)
    load_tail.wait()
    for pair in range(LOAD_STEPS * STEP_T // 2, PAIRS):
        norm_pair(pair)

    load_ends.wait()
    load_counts.wait()
    weights["query"].wait()
    weights["key"].wait()
    end_values = []
    for first in range(0, CAPS, TILE):
        rows = jnp.zeros((TILE, WIDTH), BF16)
        for inner in range(TILE):
            last = jnp.clip(ends[0, me % 4 * CAPS + first + inner] - 1, 0, CTX - 1)
            found = tokens[last, first : first + TILE, :]
            rows = jnp.where(iota((TILE, WIDTH), 0) == inner, found, rows)
        end_values.append(rows)
    end_values = jnp.concatenate(end_values, axis=0).astype(F32)
    end_normed = norm_rows(end_values).astype(BF16)
    head_of = iota((GROUP, BLOCK), 1) // HEAD_DIM
    groups = [slice(group * GROUP, (group + 1) * GROUP) for group in range(GROUPS)]
    spans = [slice(at, at + BLOCK) for at in range(0, WIDTH, BLOCK)]
    key_query = []
    for span in spans:
        query = dot(end_normed, query_w[:, span]).astype(BF16).astype(F32)
        query = query * (1.0 / math.sqrt(HEAD_DIM))
        spread = [
            jnp.where(head_of == head, query[rows], 0.0)
            for rows in groups
            for head in range(BLOCK_HEADS)
        ]
        spread = jnp.concatenate(spread, axis=0).astype(BF16)
        key_query.append((dot_last(spread, key_w[:, span]) * LOG2_E).astype(BF16))

    picked = iota((CAPS, 128), 1) == iota((CAPS, 128), 0) + me % 4 * CAPS
    lengths = jnp.sum(jnp.where(picked, counts[0:1, :].astype(F32), 0.0), axis=1, keepdims=True)
    lengths = jnp.maximum(lengths, 1.0)

    token = iota((2 * GROUP, TOKENS_PAD), 1)
    own = token % GROUP == iota((2 * GROUP, TOKENS_PAD), 0) % GROUP
    for group in range(GROUPS):
        count = lengths[group * GROUP : (group + 1) * GROUP]
        count = jnp.concatenate([count, count], axis=0)
        inside = own & ((token // GROUP).astype(F32) < count)
        attn_bias[group] = jnp.where(inside, 0.0, -jnp.inf)

    part = BLOCK_HEADS * GROUP
    contexts = []
    for group in range(GROUPS):
        rows = slice(group * part, (group + 1) * part)
        asked = jnp.concatenate([block[rows] for block in key_query], axis=0)
        attn_scores[group] = dot_last(asked, normed[group])
    for group in range(GROUPS):
        totals = []
        for head in range(0, HEADS, 2):
            rows = slice(head * GROUP, (head + 2) * GROUP)
            value = attn_scores[group, rows, :] + attn_bias[group]
            value = jnp.exp2(value - jnp.max(value, axis=1, keepdims=True))
            attn[group, rows, :] = value.astype(BF16)
            totals.append(jnp.sum(value, axis=1, keepdims=True))
        context = dot(attn[group], normed[group]) * (1.0 / jnp.concatenate(totals, axis=0))
        contexts.append(context.astype(BF16))

    load_images.wait()
    image_values = image_rows[...].astype(F32)
    image_unit = (image_values * unit_scale(image_values)).astype(BF16)
    slots = (place.slot(0, 0), place.slot(1, 0))
    units[0, 0, slots[0]] = image_unit

    def all_of(buffer, semaphore):
        return pltpu.make_async_remote_copy(
            src_ref=buffer,
            dst_ref=buffer,
            send_sem=semaphore,
            recv_sem=semaphore,
            device_id=(partner,),
            device_id_type=MESH,
        )

    pl.semaphore_wait(barrier, len(friends))

    def send_units(kind):
        for offset in range(CHIPS - 1, 0, -1):
            copy = pltpu.make_async_remote_copy(
                src_ref=units.at[kind, 0, slots[kind]],
                dst_ref=units.at[kind, 0, slots[kind]],
                send_sem=gather_send.at[kind],
                recv_sem=gather_recv.at[kind],
                device_id=(place.peer(kind, offset, core),),
                device_id_type=MESH,
            )
            copy.start()

    def hand_on(kind, offset):
        slot = place.slot(kind, offset)
        copy = pltpu.make_async_remote_copy(
            src_ref=units.at[kind, 0, slot],
            dst_ref=units.at[kind, 1, slot],
            send_sem=pass_send.at[kind],
            recv_sem=pass_recv.at[kind],
            device_id=(partner,),
            device_id_type=MESH,
        )
        copy.start()

    send_units(0)
    hand_on(0, 0)

    for name in ("value", "out", "up", "down", "proj"):
        weights[name].wait()
    mixed = []
    for number, span in enumerate(spans):
        rows = slice(number * part, (number + 1) * part)
        by_head = jnp.concatenate([context[rows] for context in contexts], axis=0)
        by_head = dot(by_head, value_w[:, span])
        sums = []
        for group in range(GROUPS):
            total = jnp.zeros((GROUP, BLOCK), F32)
            for head in range(BLOCK_HEADS):
                first = group * part + head * GROUP
                total = total + jnp.where(head_of == head, by_head[first : first + GROUP], 0.0)
            sums.append(total)
        mixed.append(jnp.concatenate(sums, axis=0))
    mixed = jnp.concatenate(mixed, axis=1).astype(BF16)

    residual = (end_values + dot(mixed, out_w[...])).astype(BF16)
    residual = residual.astype(F32)
    inner = norm_rows(residual).astype(BF16)
    final = residual
    for part in range(FF // WIDTH):
        span = slice(part * WIDTH, (part + 1) * WIDTH)
        hidden = dot(inner, up_w[:, span])
        hidden = 0.5 * hidden * (1.0 + lax.erf(hidden * (1.0 / math.sqrt(2.0))))
        final = final + dot(hidden.astype(BF16), down_w[span, :])
    pooled = norm_rows(final).astype(BF16)
    text_values = dot(pooled, proj_w[...]).astype(BF16).astype(F32)
    text_unit = (text_values * unit_scale(text_values)).astype(BF16)
    units[1, 0, slots[1]] = text_unit

    send_units(1)
    hand_on(1, 0)

    all_of(units.at[0, 0, pl.ds(0, CHIPS - 1)], gather_recv.at[0]).wait_recv()
    for offset in range(1, CHIPS):
        hand_on(0, offset)

    all_of(units.at[1, 0, pl.ds(0, CHIPS - 1)], gather_recv.at[1]).wait_recv()
    for offset in range(1, CHIPS):
        hand_on(1, offset)
    all_of(units.at[0, 1], pass_recv.at[0]).wait_recv()

    eye = iota((PIECE, PIECE), 0) == iota((PIECE, PIECE), 1)
    half_pieces = HALF // PIECE

    def score(half):
        scores = dot_last(units[1, half].reshape(HALF, WIDTH), units[0].reshape(ROWS, WIDTH))
        scores = scores * (LOGIT_SCALE * LOG2_E)
        for axis, exp, top in ((1, row_exp, row_peak), (0, col_exp, col_peak)):
            peak = jnp.max(scores, axis=axis, keepdims=True)
            value = jnp.exp2(scores - peak)
            exp[half] = value
            top[half] = peak
            if half == 0:
                yield peak + jnp.log(jnp.sum(value, axis=axis, keepdims=True)) * LOG2_E

    row_log, col_log = score(0)
    for piece in range(half_pieces):
        part = row_log[piece * PIECE : (piece + 1) * PIECE]
        part = jnp.sum(jnp.where(eye, part, 0.0), axis=0, keepdims=True)
        text_logs[0, piece] = part
    for piece in range(PIECES):
        image_logs[0, piece] = col_log[:, piece * PIECE : (piece + 1) * PIECE]

    for offset in range(CHIPS - 1, -1, -1):
        for kind, logs in enumerate((image_logs, text_logs)):
            for side in range(2):
                if offset == 0 and side == 0:
                    continue
                copy = pltpu.make_async_remote_copy(
                    src_ref=logs.at[0],
                    dst_ref=logs.at[side * CHIPS + offset],
                    send_sem=log_send.at[kind],
                    recv_sem=log_recv.at[kind],
                    device_id=(place.peer(kind, offset, core + side - 2 * side * core),),
                    device_id_type=MESH,
                )
                copy.start()

    all_of(units.at[1, 1], pass_recv.at[1]).wait_recv()
    for _ in score(1):
        pass

    sent_logs = [logs.at[pl.ds(0, 2 * CHIPS - 1)] for logs in (image_logs, text_logs)]
    for kind in range(2):
        all_of(sent_logs[kind], log_recv.at[kind]).wait_recv()

    def whole_log(terms):
        top = terms[0]
        for term in terms[1:]:
            top = jnp.maximum(top, term)
        total = sum(jnp.exp2(term - top) for term in terms)
        return top + jnp.log(total) * LOG2_E

    terms = [image_logs[offset] for offset in range(CHIPS)]
    for offset in range(CHIPS):
        term = image_logs[CHIPS + offset]
        terms.append(jnp.concatenate([term[half_pieces:], term[:half_pieces]], axis=0))
    image_log = whole_log(terms)
    image_log = jnp.concatenate([image_log[piece] for piece in range(PIECES)], axis=1)
    for half in range(2):
        text_log = whole_log([text_logs[half * CHIPS + offset] for offset in range(CHIPS)])
        col_scale = jnp.exp2(col_peak[half] - image_log)
        for piece in range(half_pieces):
            rows = slice(piece * PIECE, (piece + 1) * PIECE)
            first = half * HALF + piece * PIECE
            log = jnp.sum(jnp.where(eye, text_log[piece], 0.0), axis=1, keepdims=True)
            row_scale = jnp.exp2(row_peak[half, rows] - log)
            both = row_exp[half, rows] * row_scale + col_exp[half, rows] * col_scale
            weight[first : first + PIECE, :] = both.astype(BF16)

    duty = 1 - core
    for far in (1, 0):
        first = place.slot(duty, 4 * far) // 4 * 4
        spans = [
            pl.ds(pl.multiple_of(side * HALF + first * CAPS, PIECE), PIECE) for side in range(2)
        ]

        def keep(grad):
            blocks[:, pl.ds(first, 4)] = grad.astype(BF16).reshape(2, 4, CAPS, WIDTH)

        @pl.when(duty == 0)
        def _():
            columns = jnp.concatenate([weight[:, span] for span in spans], axis=1)
            keep(dot_first(columns, units[1].reshape(ROWS, WIDTH)))

        @pl.when(duty == 1)
        def _():
            rows = jnp.concatenate([weight[span, :] for span in spans], axis=0)
            keep(dot(rows, units[0].reshape(ROWS, WIDTH)))

        for offset in range(4 * far + 3, 4 * far - 1, -1):
            slot = place.slot(duty, offset)
            for side in range(2):
                if offset == 0 and side == 0:
                    parts[duty * CHIPS] = blocks[0, slot]
                    continue
                copy = pltpu.make_async_remote_copy(
                    src_ref=blocks.at[side, slot],
                    dst_ref=parts.at[duty * CHIPS + offset],
                    send_sem=part_sem.at[0],
                    recv_sem=part_sem.at[1],
                    device_id=(place.peer(duty, offset, core + side - 2 * side * core),),
                    device_id_type=MESH,
                )
                copy.start()

    sent_parts = parts.at[pl.ds(0, 2 * CHIPS - 1)]
    all_of(sent_parts, part_sem.at[1]).wait_recv()

    half = 0.5 * LOGIT_SCALE
    sums = []
    for kind in range(2):
        total = parts[kind * CHIPS].astype(F32)
        for offset in range(1, CHIPS):
            total = total + parts[kind * CHIPS + offset].astype(F32)
        sums.append(total)
    image_unit_grad = half * sums[0] - LOGIT_SCALE * text_unit.astype(F32)
    text_unit_grad = half * sums[1] - LOGIT_SCALE * image_unit.astype(F32)
    image_grad[...] = unit_back(image_values, image_unit_grad)
    text_grad[...] = unit_back(text_values, text_unit_grad)

    for kind in range(2):
        all_of(units.at[kind, 0, pl.ds(0, CHIPS - 1)], gather_send.at[kind]).wait_send()
        all_of(units.at[kind, 0], pass_send.at[kind]).wait_send()
        all_of(sent_logs[kind], log_send.at[kind]).wait_send()
    all_of(sent_parts, part_sem.at[0]).wait_send()


def hand_out(image_from, text_from, image_to, text_to):
    image_to[...] = image_from[...]
    text_to[...] = text_from[...]


def body(captions, caption_layout, images, w_query, w_keyval, w_out, w_up, w_down, w_proj):
    hbm = pl.BlockSpec(memory_space=pl.ANY)
    vmem = pl.BlockSpec(memory_space=pltpu.VMEM)
    dma = pltpu.SemaphoreType.DMA
    grads = (jax.ShapeDtypeStruct((CAPS, WIDTH), F32),) * 2
    made = pl.pallas_call(
        kernel,
        out_shape=(pltpu.VMEM((CAPS, WIDTH), F32),) * 2,
        in_specs=[hbm] * 9,
        out_specs=(vmem, vmem),
        scratch_shapes=[
            pltpu.VMEM((CTX + 1, CAPS, WIDTH), BF16),
            pltpu.VMEM((GROUPS, TOKENS_PAD, WIDTH), BF16),
            pltpu.VMEM((WIDTH, WIDTH), BF16),
            pltpu.VMEM((WIDTH, WIDTH), BF16),
            pltpu.VMEM((WIDTH, WIDTH), BF16),
            pltpu.VMEM((WIDTH, WIDTH), BF16),
            pltpu.VMEM((WIDTH, FF), BF16),
            pltpu.VMEM((FF, WIDTH), BF16),
            pltpu.VMEM((WIDTH, WIDTH), BF16),
            pltpu.VMEM((2, 128), jnp.int32),
            pltpu.SMEM((2, 128), jnp.int32),
            pltpu.VMEM((CAPS, WIDTH), BF16),
            pltpu.VMEM((GROUPS, SPLIT, TOKENS_PAD), F32),
            pltpu.VMEM((GROUPS, 2 * GROUP, TOKENS_PAD), F32),
            pltpu.VMEM((GROUPS, SPLIT, TOKENS_PAD), BF16),
            pltpu.VMEM((2, 2, CHIPS, CAPS, WIDTH), BF16),
            pltpu.VMEM((2, HALF, ROWS), F32),
            pltpu.VMEM((2, HALF, ROWS), F32),
            pltpu.VMEM((2, HALF, 1), F32),
            pltpu.VMEM((2, 1, ROWS), F32),
            pltpu.VMEM((2 * CHIPS, PIECES, 1, PIECE), F32),
            pltpu.VMEM((2 * CHIPS, HALF // PIECE, 1, PIECE), F32),
            pltpu.VMEM((ROWS, ROWS), BF16),
            pltpu.VMEM((2, CHIPS, CAPS, WIDTH), BF16),
            pltpu.VMEM((2 * CHIPS, CAPS, WIDTH), BF16),
            dma((3,)),
            dma((LOAD_STEPS + 1,)),
            dma((7,)),
            dma((2,)),
            dma((2,)),
            dma((2,)),
            dma((2,)),
            dma((2,)),
            dma((2,)),
            dma((2,)),
        ],
        compiler_params=pltpu.CompilerParams(
            collective_id=0, has_side_effects=True, vmem_limit_bytes=VMEM_LIMIT
        ),
    )(
        captions.transpose(1, 0, 2),
        caption_layout,
        images,
        w_query,
        w_keyval,
        w_out,
        w_up,
        w_down,
        w_proj,
    )
    return pl.pallas_call(
        hand_out,
        out_shape=grads,
        in_specs=[vmem] * 2,
        out_specs=(vmem, vmem),
        compiler_params=pltpu.CompilerParams(vmem_limit_bytes=4 * 1024 * 1024),
    )(*made)


def solution(mesh):
    return jax.shard_map(
        body,
        mesh=mesh,
        in_specs=(P("dp", None, None), P(), P("dp", None), P(), P(), P(), P(), P(), P()),
        out_specs=(P("dp", None), P("dp", None)),
        check_vma=False,
    )
```
